32 devices in a mesh: gx: 4 (over y, x), gy: 2 (over core), gz: 4 (over z).
Axes of the slice: x: 2, y: 2, z: 4, core: 2. Of those that a mesh axis runs over, the one named last changes fastest.
Arguments:
- populations: float32 [2, 19, 16, 32, 512], P(None, None, 'gx', 'gy', 'gz'), may hold values from 0.01 to 0.2
- solid: int32 [16, 32, 512], P('gx', 'gy', 'gz'), may hold values 0 or 1
Outputs:
- read: float32 [2, 19, 16, 32, 512], P(None, None, 'gx', 'gy', 'gz')
The draws below stay inside these ranges and needn't reach their ends.
All inputs are finite; a program needn't handle non-finite values. No bound on the sum of `solid` on one device may be relied on, other than what follows from the above.
Results may differ from the reference program's by a relative error of at most 0.0001.
Values sent between devices are 32-bit elements; how exact they have to be, the bound alone decides.
A program may use at most 64 MiB of HBM per device.

```python
import math
import jax
import jax.numpy as jnp
import numpy as np
from jax import lax

NX = 16
NY = 32
NZ = 512


def touch_ends(values, own_key, smallest, high):
    extent = values.shape
    index_at = [jax.random.randint(jax.random.fold_in(own_key, axis), (), 0, extent[axis]) for axis in range(len(extent))]
    values = values.at[tuple(index_at)].set(smallest)
    longest = extent.index(max(extent))
    index_at[longest] = (index_at[longest] + 1) % extent[longest]
    return values.at[tuple(index_at)].set(high)


def steps_of(own_key, extent, shards, least, top_value):
    factor_of, own = 1.0, jax.random.fold_in(own_key, 6)
    for dim, blocks in shards:
        steps = jnp.exp(jax.random.uniform(jax.random.fold_in(own, dim), (blocks,), jnp.float32, least / len(shards), top_value / len(shards)))
        factor_of = factor_of * jnp.repeat(steps, extent[dim] // blocks).reshape([-1 if axis == dim else 1 for axis in range(len(extent))])
    return factor_of


def setup_inputs(seed: int = 0) -> dict:
    key_of = jax.random.split(jax.random.key(seed), 3)
    return {
        "populations": jnp.clip(jnp.exp(math.log(0.2) - 2.9957323 * jax.random.uniform(key_of[0], (2, 19, NX, NY, NZ), jnp.float32) ** steps_of(key_of[0], (2, 19, NX, NY, NZ), ((2, 4), (3, 2), (4, 4)), -0.2, 0.2)), 0.01, 0.2),
        "solid": touch_ends((jax.random.randint(key_of[1], (NX, NY, NZ), 0, 8) < 1).astype(jnp.int32), jax.random.fold_in(key_of[1], 1), 0, 1),
    }


VELOCITIES = [(0, 0, 0), (1, 0, 0), (-1, 0, 0), (0, 1, 0), (0, -1, 0), (0, 0, 1), (0, 0, -1),
              (1, 1, 0), (-1, -1, 0), (1, -1, 0), (-1, 1, 0), (1, 0, 1), (-1, 0, -1), (1, 0, -1),
              (-1, 0, 1), (0, 1, 1), (0, -1, -1), (0, 1, -1), (0, -1, 1)]
WEIGHTS = [1.0 / 3.0] + [1.0 / 18.0] * 6 + [1.0 / 36.0] * 12
OPPOSITE = [0, 2, 1, 4, 3, 6, 5, 8, 7, 10, 9, 12, 11, 14, 13, 16, 15, 18, 17]
coupling = 0.9
relax_times = (1.0, 0.8)
wall_values = (0.3, 1.5)


def collide(populations, fluid, psi, gradient):
    vel = jnp.asarray(np.array(VELOCITIES, np.float32))
    weights = jnp.asarray(np.array(WEIGHTS, np.float32))
    rho = jnp.sum(populations, axis=1)
    moment = jnp.einsum("ia,kixyz->kaxyz", vel, populations, precision=lax.Precision.HIGHEST)
    inv_first = 1.0 / relax_times[0]
    inv_second = 1.0 / relax_times[1]
    weight_sum = rho[0] * inv_first + rho[1] * inv_second
    common = (moment[0] * inv_first + moment[1] * inv_second) / weight_sum[None]
    forces = (-coupling * psi[0][None] * gradient[1], -coupling * psi[1][None] * gradient[0])
    results = []
    for comp in range(2):
        velocity = common + relax_times[comp] * forces[comp] / rho[comp][None]
        along = jnp.einsum("ia,axyz->ixyz", vel, velocity, precision=lax.Precision.HIGHEST)
        speed_sq = jnp.sum(velocity * velocity, axis=0)
        equil = weights[:, None, None, None] * rho[comp][None] * (
            1.0 + 3.0 * along + 4.5 * along * along - 1.5 * speed_sq[None])
        current = populations[comp]
        results.append(current - (current - equil) / relax_times[comp])
    post = jnp.stack(results, axis=0)
    return jnp.where(fluid[None, None], post, populations)


def reference(populations, solid):
    fluid = solid == 0
    rho = jnp.sum(populations, axis=1)
    wall = jnp.asarray(np.array(wall_values, np.float32)).reshape(2, 1, 1, 1)
    psi = jnp.where(fluid[None], rho, wall)
    parts = [jnp.zeros_like(psi) for axis_idx in range(3)]
    for i in range(1, 19):
        move = VELOCITIES[i]
        shifted = jnp.roll(psi, (-move[0], -move[1], -move[2]), axis=(1, 2, 3))
        for axis_idx in range(3):
            if move[axis_idx] != 0:
                parts[axis_idx] = parts[axis_idx] + (WEIGHTS[i] * move[axis_idx]) * shifted
    gradient = jnp.stack(parts, axis=1)
    post = collide(populations, fluid, psi, gradient)
    moved = []
    for i in range(19):
        move = VELOCITIES[i]
        pulled = jnp.roll(post[:, i], move, axis=(1, 2, 3))
        source_fluid = jnp.roll(fluid, move, axis=(0, 1, 2))
        moved.append(jnp.where(source_fluid[None], pulled, post[:, OPPOSITE[i]]))
    result = jnp.stack(moved, axis=1)
    return jnp.where(fluid[None, None], result, populations)
```

```python
import jax
import jax.numpy as jnp
from jax import lax
from jax.experimental import pallas as pl
from jax.experimental.pallas import tpu as pltpu
from jax.sharding import PartitionSpec as P

VELOCITIES = [
    (0, 0, 0),
    (1, 0, 0),
    (-1, 0, 0),
    (0, 1, 0),
    (0, -1, 0),
    (0, 0, 1),
    (0, 0, -1),
    (1, 1, 0),
    (-1, -1, 0),
    (1, -1, 0),
    (-1, 1, 0),
    (1, 0, 1),
    (-1, 0, -1),
    (1, 0, -1),
    (-1, 0, 1),
    (0, 1, 1),
    (0, -1, -1),
    (0, 1, -1),
    (0, -1, 1),
]
WEIGHTS = [1.0 / 3.0] + [1.0 / 18.0] * 6 + [1.0 / 36.0] * 12
OPPOSITE = [0, 2, 1, 4, 3, 6, 5, 8, 7, 10, 9, 12, 11, 14, 13, 16, 15, 18, 17]
INDEX = {v: i for i, v in enumerate(VELOCITIES)}
COUPLING = 0.9
RELAX = (1.0, 0.8)
WALL = (0.3, 1.5)
INV = [1.0 / t for t in RELAX]
KEEP = [1.0 - v for v in INV]
AXES = ("gx", "gy", "gz")
MESH = pl.DeviceIdType.MESH

X_UP = [i for i in range(19) if VELOCITIES[i][0] == 1]
Y_UP = [i for i in range(19) if VELOCITIES[i][1] == 1]
Z_UP = [(0, 0, 1), (1, 0, 1), (-1, 0, 1), (0, 1, 1), (0, -1, 1)]
Z_UP = [INDEX[v] for v in Z_UP]
Z_PAIR = {}
for _g, _i in enumerate(Z_UP):
    Z_PAIR[_i] = _g
    Z_PAIR[OPPOSITE[_i]] = _g
Z_FROM = [(dx, dz) for dz in (-1, 1) for dx in (0, -1, 1)]
T = 8
LANES = 128
HALF = LANES // 2


def along_of(i, u):
    total = None
    for d in range(3):
        c = VELOCITIES[i][d]
        if c:
            term = u[d] if c > 0 else -u[d]
            total = term if total is None else total + term
    return total


def step_kernel(pop_hbm, solid_hbm, out, pop, solid, S, SU, SD, psi, H, O, A, V, post, zpost,
                YS, YV, YP, WP, XP, XW, XWR, XPW, ZS, XA, ZR, load_sem, send_sem, recv_sem,
                near_sem, far_sem):
    X, Y, Z = solid.shape
    YT = Y // T
    inner = slice(T, T + Y)
    low, high = slice(0, T), slice(Y + T, Y + 2 * T)
    XX = X + 4
    assert Z == LANES and (YT + 2) * XX * 2 <= HALF and X >= 2
    stride_t = HALF // (YT + 2)
    assert stride_t >= 2 * XX and 2 * X <= XX

    loads = [pltpu.make_async_copy(solid_hbm, solid, load_sem.at[X])]
    loads += [
        pltpu.make_async_copy(pop_hbm.at[:, :, x], pop.at[:, :, x], load_sem.at[x])
        for x in range(X)
    ]

    me = [lax.axis_index(a) for a in AXES]
    count = [lax.axis_size(a) for a in AXES]
    assert count[1] % 2 == 0
    parity = lax.rem(me[1], 2)
    is_near, is_far = parity == 0, parity == 1

    def device(offset):
        return tuple(lax.rem(me[d] + offset[d] + count[d], count[d]) for d in range(3))

    def member(offset, odd):
        place = device(offset)
        return (place[0], me[1] - parity + odd, place[2])

    barrier = pltpu.get_barrier_semaphore()

    def arrive(place):
        pl.semaphore_signal(barrier, inc=1, device_id=place, device_id_type=MESH)

    for dx, dz in sorted(Z_FROM, key=lambda v: -abs(v[0])):
        arrive(member((dx, 0, dz), 1))
    for dx in (1, -1):
        arrive(member((dx, 0, 0), 0))
    arrive((me[0], me[1] + 1 - 2 * parity, me[2]))
    near_count, far_count = 5, 13
    if count[1] > 2:
        near_count += 2
        arrive((me[0], lax.rem(me[1] + 3 * parity - 2 + count[1], count[1]), me[2]))
    partner = (me[0], me[1] + 1 - 2 * parity, me[2])
    for copy in loads:
        copy.start()

    lane = lax.broadcasted_iota(jnp.int32, (T, LANES), 1)
    row = lax.broadcasted_iota(jnp.int32, (T, LANES), 0)
    pair = lane // 2
    even = lane % 2 == 0
    half = lane // HALF
    slot = (lane % stride_t) // 2
    tile_t = (lane % HALF) // stride_t
    first, last = lane == 0, lane == Z - 1
    lane_y = lax.broadcasted_iota(jnp.int32, (Y, LANES), 1)
    first_y, last_y = lane_y == 0, lane_y == Z - 1
    upper = row < T // 2

    def roll(v, n):
        n = n % LANES
        return pltpu.roll(v, n, 1) if n else v

    def roll_rows(v, n):
        n = n % T
        return pltpu.roll(v, n, 0) if n else v

    copies = {}

    def send(name, src, dst, offset):
        n = len(copies)
        copy = pltpu.make_async_remote_copy(
            src_ref=src,
            dst_ref=dst,
            send_sem=send_sem.at[n],
            recv_sem=recv_sem.at[n],
            device_id=device(offset),
            device_id_type=MESH,
        )
        copy.start()
        assert name not in copies
        copies[name] = copy

    def await_(kind):
        for name, copy in copies.items():
            if name[0] == kind:
                copy.wait_recv()

    loads[0].wait()
    for x in range(X):
        loads[1 + x].wait()
        fluid = solid[x] == 0
        total, mom = [], []
        for k in range(2):
            f = [pop[k, i, x] for i in range(19)]
            rho = f[0]
            m = [None, None, None]
            for i in range(1, 19, 2):
                rho = rho + (f[i] + f[i + 1])
                diff = f[i] - f[i + 1]
                for d in range(3):
                    c = VELOCITIES[i][d]
                    if c:
                        m[d] = (
                            (diff if c > 0 else -diff)
                            if m[d] is None
                            else (m[d] + diff if c > 0 else m[d] - diff)
                        )
            total.append(rho)
            S[k, 2 + x, inner] = jnp.where(fluid, rho, -WALL[k])
            mom.append([v * INV[k] if INV[k] != 1.0 else v for v in m])
        scale = 1.0 / (total[0] * INV[0] + total[1] * INV[1])
        for d in range(3):
            V[d, 1 + x, 0:Y] = (mom[0][d] + mom[1][d]) * scale

    @pl.when(is_near)
    def _():
        pl.semaphore_wait(barrier, near_count)
        pl.semaphore_signal(near_sem, inc=1, device_id=partner, device_id_type=MESH)

    @pl.when(is_far)
    def _():
        pl.semaphore_wait(near_sem, 1)

    for n, side in enumerate((1, -1)):
        tile = slice(Y - T, Y) if side > 0 else slice(0, T)
        wide = slice(Y, Y + T) if side > 0 else slice(T, 2 * T)
        to = (0, side, 0)
        send(("yS", side), S.at[:, 2:2 + X, wide], YS.at[n], to)
        send(("yV", side), V.at[:, 1:1 + X, tile], YV.at[n], to)
        for m, i in enumerate(Y_UP):
            i = i if side > 0 else OPPOSITE[i]
            send(("yP", side, m), pop.at[1, i, :, tile], YP.at[n, m], to)
    for n, side in enumerate((1, -1)):
        to = (side, 0, 0)
        src = slice(X, X + 2) if side > 0 else slice(2, 4)
        dst = slice(0, 2) if side > 0 else slice(X + 2, X + 4)
        send(("xS", side), S.at[:, src, inner], S.at[:, dst, inner], to)
    for n, side in enumerate((1, -1)):
        to = (side, 0, 0)
        src, dst = (X, 0) if side > 0 else (1, X + 1)
        send(("xV", side), V.at[:, src, 0:Y], V.at[:, dst, 0:Y], to)
    for m, i in enumerate(X_UP):
        for n, side in enumerate((1, -1)):
            i_s, x_s = (i, X - 1) if side > 0 else (OPPOSITE[i], 0)
            send(("xP", side, m), pop.at[1, i_s, x_s], XP.at[n, m], (side, 0, 0))

    def place_of(h, b, t, x):
        return (h * HALF + t * stride_t + (b * X + x) * 2) // 2

    blank = jnp.zeros((T, LANES), jnp.float32)
    packs = [blank, blank, blank, blank]

    def put(p, h, b, t, x, value):
        j = place_of(h, b, t, x)
        packs[p] = jnp.where(pair == j, roll(value, 2 * j + 1), packs[p])

    POP_PLACE = [(2, 0, 0), (2, 0, 1), (2, 1, 0), (2, 1, 1), (3, 1, 0)]
    V_PLACE = [(1, 0, 0), (1, 0, 1), (1, 1, 0)]

    def second(value):
        return jnp.where(lane < HALF, roll(value, -1), roll(value, 1))

    def pack(x, t):
        rows = low if t == 0 else slice(T * t, T * t + T)
        rows_v = slice(Y, Y + T) if t == 0 else slice(T * (t - 1), T * t)
        for k in range(2):
            value = S[k, 2 + x, rows]
            put(0, k, 0, t, x, value)
            put(0, k, 1, t, x, second(value))
        for d in range(3):
            put(*V_PLACE[d], t, x, V[d, 1 + x, rows_v])
        for g, i in enumerate(Z_UP):
            if t == 0:
                c = VELOCITIES[i]
                if c[1] == 0:
                    continue
                y_dir = i if c[1] > 0 else OPPOSITE[i]
                value = WP[Y_UP.index(y_dir), x]
            else:
                rows_p = slice(T * (t - 1), T * t)
                value = jnp.where(lane < HALF, pop[1, OPPOSITE[i], x, rows_p], pop[1, i, x, rows_p])
            put(*POP_PLACE[g], t, x, value)

    for x in range(X):
        for t in range(1, YT + 1):
            pack(x, t)

    await_("yS")
    await_("yV")
    await_("yP")
    for x in range(X):
        for k in range(2):
            value = jnp.where(upper, YS[1, k, x], YS[0, k, x])
            S[k, 2 + x, low] = value
            S[k, 2 + x, high] = value
        for d in range(3):
            V[d, 1 + x, Y:Y + T] = jnp.where(upper, YV[1, d, x], YV[0, d, x])
        for m in range(5):
            WP[m, x] = jnp.where(upper, YP[1, m, x], YP[0, m, x])
    for x in range(X):
        pack(x, 0)
    diag = jnp.where(((slot % X) == X - 1) == even, roll(packs[2], HALF), roll(packs[2], 2 * X))
    packs[1] = jnp.where((half == 1) & (slot >= X) & (slot < 2 * X), diag, packs[1])
    for p in range(4):
        ZS[p] = jnp.where(tile_t == YT + 1, roll(packs[p], stride_t * (YT + 1)), packs[p])

    pairs_y = [Y_UP.index(INDEX[(1, 1, 0)]), Y_UP.index(INDEX[(-1, 1, 0)])]
    keep_rows = (row < 2) | (row >= T - 2)
    for n, side in enumerate((1, -1)):
        planes = (X, X + 1) if side > 0 else (2, 3)
        for m, p in enumerate(planes):
            XW[n, m] = jnp.where(keep_rows, S[0, p, low], roll_rows(S[1, p, low], 4))
        x = X - 1 if side > 0 else 0
        up, down = (pairs_y[0], pairs_y[1]) if side > 0 else (pairs_y[1], pairs_y[0])
        fields = [V[d, 1 + x, Y:Y + T] for d in range(3)]
        fields.append(jnp.where(upper, WP[down, x], WP[up, x]))
        merged = fields[0]
        for f in range(1, 4):
            at = (row == 2 * f - 1) | (row == 2 * f)
            merged = jnp.where(at, roll_rows(fields[f], 2 * f), merged)
        XW[n, 2] = merged
    for n, side in enumerate((1, -1)):
        send(("xA", side), ZS.at[0], XA.at[n], (side, 0, 0))
        send(("xW", side), XW.at[n], XWR.at[n], (side, 0, 0))

    @pl.when(is_far)
    def _():
        pl.semaphore_wait(barrier, far_count)
        pl.semaphore_signal(far_sem, inc=1, device_id=partner, device_id_type=MESH)

    @pl.when(is_near)
    def _():
        pl.semaphore_wait(far_sem, 1)

    for dx, dz in sorted(Z_FROM, key=lambda v: -abs(v[0])):
        size = slice(0, 2) if dx else slice(0, 4)
        send(("z", dx, dz), ZS.at[size], ZR.at[Z_FROM.index((-dx, -dz)), size], (dx, 0, dz))

    await_("xS")
    await_("xA")
    await_("xW")
    for n in range(2):
        planes = (0, 1) if n == 0 else (X + 2, X + 3)
        for m, p in enumerate(planes):
            value = XWR[n, m]
            other = roll_rows(value, 4)
            for k, w in ((0, value), (1, other)):
                S[k, p, low] = w
                S[k, p, high] = w
    await_("z")

    def gather(b, middle, left, right):
        center = roll(middle, 2 * (2 - b * X))
        before = roll(left, -2 * (b * X + X - 2))
        after = roll(right, 2 * (X + 2 - b * X))
        return jnp.where(slot < 2, before, jnp.where(slot >= X + 2, after, center))

    def merged_z(dx, p):
        return jnp.where(even, ZR[Z_FROM.index((dx, -1)), p], ZR[Z_FROM.index((dx, 1)), p])

    def gather_z(p):
        m = [merged_z(dx, p) for dx in (0, -1, 1)]
        return gather(0, *m), gather(1, *m)

    s1, s2 = gather_z(0)
    s0 = gather(0, ZS[0], XA[0], XA[1])
    s0 = jnp.where(even, roll(s0, -1), roll(s0, 1))

    def spread(tile, k, t, xx):
        return roll(tile, LANES - 1 - (k * HALF + t * stride_t + 2 * xx))

    for p in range(XX):
        for k in range(2):
            for t in range(YT + 1):
                rows = low if t == 0 else slice(T * t, T * t + T)
                value = S[k, p, rows]
                edge = spread(s1, k, t, p)
                above = roll(jnp.where(first, edge, value), -1)
                below = roll(jnp.where(last, edge, value), 1)
                size = jnp.abs(value)
                a_above, a_below = jnp.abs(above), jnp.abs(below)
                for r in (rows,) if t else (low, high):
                    psi[k, p, r] = size
                    H[k, p, r] = 2.0 * size + (a_above + a_below)
                    O[k, p, r] = a_above - a_below
                    if k == 0:
                        SU[p, r] = above
                        SD[p, r] = below

    def window(w, dy):
        if w == 0:
            return slice(T + dy, T + dy + Y)
        return slice(Y + T - 1, Y + 2 * T - 1) if dy < 0 else slice(dy, T + dy)

    def rows_of(w):
        return slice(0, Y) if w == 0 else slice(Y, Y + T)

    for p in range(XX):
        for k in range(2):
            for w in range(2):
                A[k, p, rows_of(w)] = (
                    H[k, p, window(w, 0)] + psi[k, p, window(w, 1)] + psi[k, p, window(w, -1)]
                ) * (1.0 / 36.0)

    def gradient(k, p, w):
        gx = A[k, p + 1, rows_of(w)] - A[k, p - 1, rows_of(w)]
        ends = []
        for dy in (1, -1):
            r = window(w, dy)
            ends.append(H[k, p, r] + (psi[k, p + 1, r] + psi[k, p - 1, r]))
        gy = (ends[0] - ends[1]) * (1.0 / 36.0)
        r = window(w, 0)
        gz = 2.0 * O[k, p, r] + (O[k, p + 1, r] + O[k, p - 1, r])
        gz = (gz + (O[k, p, window(w, 1)] + O[k, p, window(w, -1)])) * (1.0 / 36.0)
        return gx, gy, gz

    def velocities(x, w):
        grads = [gradient(k, x + 2, w) for k in range(2)]
        common = [V[d, 1 + x, rows_of(w)] for d in range(3)]
        return [
            [common[d] - (COUPLING * RELAX[k]) * grads[1 - k][d] for d in range(3)]
            for k in range(2)
        ]

    def flat_of(u):
        return 1.0 - 1.5 * (u[0] * u[0] + u[1] * u[1] + u[2] * u[2])

    def one_way(w, flat, along, sign):
        even_part = w * (flat + 4.5 * (along * along))
        return even_part + w * ((3.0 * sign) * along)

    def collide_own(x):
        us = velocities(x, 0)
        for k in range(2):
            u = us[k]
            rho = psi[k, 2 + x, inner] * INV[k]
            flat = flat_of(u)
            scaled = {w: rho * w for w in sorted(set(WEIGHTS))}
            values = {0: scaled[WEIGHTS[0]] * flat}
            for i in range(1, 19, 2):
                along = along_of(i, u)
                w = scaled[WEIGHTS[i]]
                even_part = w * (flat + 4.5 * (along * along))
                odd_part = w * (3.0 * along)
                values[i] = even_part + odd_part
                values[i + 1] = even_part - odd_part
            for i in range(19):
                if abs(KEEP[k]) > 1e-9:
                    values[i] = values[i] + KEEP[k] * pop[k, i, x]
                post[k, i, 1 + x, inner] = values[i]

    row_sign = jnp.where(upper, -1.0, 1.0)

    def collide_rows(x):
        us = velocities(x, 1)
        for k in range(2):
            u = us[k]
            rho = psi[k, 2 + x, low] * INV[k]
            flat = flat_of(u)
            for m, i in enumerate(Y_UP):
                w = rho * WEIGHTS[i]
                value = one_way(w, flat, along_of(i, u), row_sign)
                if abs(KEEP[k]) > 1e-9:
                    value = value + KEEP[k] * WP[m, x]
                post[k, i, 1 + x, low] = value
                post[k, OPPOSITE[i], 1 + x, high] = value

    def collide_plane(n):
        x = -1 if n == 0 else X
        sign = 1.0 if n == 0 else -1.0
        us = velocities(x, 0)
        for k in range(2):
            u = us[k]
            rho = psi[k, 2 + x, inner] * INV[k]
            flat = flat_of(u)
            for m, i in enumerate(X_UP):
                value = one_way(rho * WEIGHTS[i], flat, along_of(i, u), sign)
                if abs(KEEP[k]) > 1e-9:
                    value = value + KEEP[k] * XP[n, m]
                post[k, i if n == 0 else OPPOSITE[i], 1 + x, inner] = value
        us = velocities(x, 1)
        cx = 1 if n == 0 else -1
        up, down = INDEX[(cx, 1, 0)], INDEX[(cx, -1, 0)]
        for k in range(2):
            u = us[k]
            rho = psi[k, 2 + x, low] * INV[k]
            value = one_way(rho * WEIGHTS[up], flat_of(u), sign * u[0] + row_sign * u[1], 1.0)
            if abs(KEEP[k]) > 1e-9:
                value = value + KEEP[k] * XPW[n]
            post[k, up, 1 + x, low] = value
            post[k, down, 1 + x, high] = value

    def collide_z():
        t1, t2 = gather_z(1)
        other1, other2 = roll(t1, HALF), roll(t2, HALF)
        lower = half == 0
        common = [
            jnp.where(lower, t1, other1),
            jnp.where(lower, t2, other2),
            jnp.where(lower, other1, t1),
        ]
        p0, p1, p2 = jnp.abs(s0), jnp.abs(s1), jnp.abs(s2)

        def x_up(v):
            return roll(v, -2)

        def x_down(v):
            return roll(v, 2)

        def y_up(v):
            r = roll_rows(v, -1)
            return jnp.where(row == T - 1, roll(r, -stride_t), r)

        def y_down(v):
            r = roll_rows(v, 1)
            return jnp.where(row == 0, roll(r, stride_t), r)

        xs = [x_up(v) + x_down(v) for v in (p0, p1, p2)]
        ys = [y_up(v) + y_down(v) for v in (p0, p1, p2)]
        g = 2.0 * p1 + (p0 + p2)
        a = g + ys[1]
        b = g + xs[1]
        c0 = 2.0 * p0 + (xs[0] + ys[0])
        c2 = 2.0 * p2 + (xs[2] + ys[2])
        sign = jnp.where(even, 1.0, -1.0)
        grads = [
            (x_up(a) - x_down(a)) * (1.0 / 36.0),
            (y_up(b) - y_down(b)) * (1.0 / 36.0),
            (c0 - c2) * (sign * (1.0 / 36.0)),
        ]
        factor = jnp.where(lower, COUPLING * RELAX[0], COUPLING * RELAX[1])
        u = [common[d] - factor * roll(grads[d], HALF) for d in range(3)]
        rho = p1 * jnp.where(lower, INV[0], INV[1])
        keep = jnp.where(lower, KEEP[0], KEEP[1])
        flat = flat_of(u)
        beyond = (slot < 2) | (slot >= X + 2)
        results = []
        for g, i in enumerate(Z_UP):
            p, h, b = POP_PLACE[g]
            old = roll(merged_z(0, p), 2 * (2 - b * X) + HALF * (1 - h))
            if VELOCITIES[i][0]:
                old = jnp.where(beyond, t2, old)
            value = one_way(rho * WEIGHTS[i], flat, along_of(i, u), sign)
            results.append(value + keep * jnp.where(lower, 0.0, old))
        for k in range(2):
            for g, i in enumerate(Z_UP):
                c = VELOCITIES[i]
                xs_needed = range(-1, X + 1) if c[0] else range(X)
                ts = range(YT + 2) if c[1] else range(1, YT + 1)
                for x in xs_needed:
                    for t in ts:
                        zpost[k, g, 1 + x, T * t:T * t + T] = spread(results[g], k, t, x + 2)

    def stream(x):
        fluid = solid[x] == 0
        for k in range(2):
            for i in range(19):
                c = VELOCITIES[i]
                rows = slice(T - c[1], T - c[1] + Y)
                read = post[k, i, 1 + x - c[0], rows]
                if i:
                    if c[2]:
                        edge = zpost[k, Z_PAIR[i], 1 + x - c[0], rows]
                        read = jnp.where(last_y if c[2] > 0 else first_y, edge, read)
                        read = roll(read, c[2])
                    p = 2 + x - c[0]
                    source = (SD if c[2] > 0 else SU)[p, rows] if c[2] else S[0, p, rows]
                    bounced = post[k, OPPOSITE[i], 1 + x, inner]
                    read = jnp.where(source > 0.0, read, bounced)
                out[k, i, x] = jnp.where(fluid, read, pop[k, i, x])

    for x in range(X):
        collide_own(x)
    for x in range(X):
        collide_rows(x)
    collide_z()
    for x in range(1, X - 1):
        stream(x)
    await_("xV")
    await_("xP")
    for n in range(2):
        plane = 0 if n == 0 else X + 1
        tile = XWR[n, 2]
        for d in range(3):
            V[d, plane, Y:Y + T] = roll_rows(tile, -2 * d)
        XPW[n] = roll_rows(tile, -6)
    for n in range(2):
        collide_plane(n)
    for x in (0, X - 1):
        stream(x)
    for copy in copies.values():
        copy.wait_send()


def body(populations, solid):
    X, Y, Z = solid.shape
    f32 = jnp.float32
    dma = pltpu.SemaphoreType.DMA
    R = Y + 2 * T

    def vmem(*shape):
        return pltpu.VMEM(shape, f32)

    return pl.pallas_call(
        step_kernel,
        out_shape=pltpu.VMEM(populations.shape, f32),
        in_specs=[pl.BlockSpec(memory_space=pl.ANY)] * 2,
        out_specs=pl.BlockSpec(memory_space=pltpu.VMEM),
        scratch_shapes=[
            vmem(*populations.shape),
            pltpu.VMEM(solid.shape, jnp.int32),
            vmem(2, X + 4, R, Z),
            vmem(X + 4, R, Z),
            vmem(X + 4, R, Z),
            vmem(2, X + 4, R, Z),
            vmem(2, X + 4, R, Z),
            vmem(2, X + 4, R, Z),
            vmem(2, X + 4, Y + T, Z),
            vmem(3, X + 2, Y + T, Z),
            vmem(2, 19, X + 2, R, Z),
            vmem(2, 5, X + 2, R, Z),
            vmem(2, 2, X, T, Z),
            vmem(2, 3, X, T, Z),
            vmem(2, 5, X, T, Z),
            vmem(5, X, T, Z),
            vmem(2, 5, Y, Z),
            vmem(2, 3, T, Z),
            vmem(2, 3, T, Z),
            vmem(2, T, Z),
            vmem(4, T, LANES),
            vmem(2, T, LANES),
            vmem(6, 4, T, LANES),
            dma((X + 1,)),
            dma((38,)),
            dma((38,)),
            pltpu.SemaphoreType.REGULAR,
            pltpu.SemaphoreType.REGULAR,
        ],
        compiler_params=pltpu.CompilerParams(collective_id=0, has_side_effects=True),
    )(populations, solid)


def solution(mesh):
    in_specs = (P(None, None, "gx", "gy", "gz"), P("gx", "gy", "gz"))
    out_specs = P(None, None, "gx", "gy", "gz")
    return jax.shard_map(body, mesh=mesh, in_specs=in_specs, out_specs=out_specs, check_vma=False)
```

```python
import jax
import jax.numpy as jnp
from jax import lax
from jax.experimental import pallas as pl
from jax.experimental.pallas import tpu as pltpu
from jax.sharding import PartitionSpec as P

VELOCITIES = [
    (0, 0, 0),
    (1, 0, 0),
    (-1, 0, 0),
    (0, 1, 0),
    (0, -1, 0),
    (0, 0, 1),
    (0, 0, -1),
    (1, 1, 0),
    (-1, -1, 0),
    (1, -1, 0),
    (-1, 1, 0),
    (1, 0, 1),
    (-1, 0, -1),
    (1, 0, -1),
    (-1, 0, 1),
    (0, 1, 1),
    (0, -1, -1),
    (0, 1, -1),
    (0, -1, 1),
]
WEIGHTS = [1.0 / 3.0] + [1.0 / 18.0] * 6 + [1.0 / 36.0] * 12
OPPOSITE = [0, 2, 1, 4, 3, 6, 5, 8, 7, 10, 9, 12, 11, 14, 13, 16, 15, 18, 17]
INDEX = {v: i for i, v in enumerate(VELOCITIES)}
COUPLING = 0.9
RELAX = (1.0, 0.8)
WALL = (0.3, 1.5)
INV = [1.0 / t for t in RELAX]
KEEP = [1.0 - v for v in INV]
AXES = ("gx", "gy", "gz")
MESH = pl.DeviceIdType.MESH

X_UP = [i for i in range(19) if VELOCITIES[i][0] == 1]
Y_UP = [i for i in range(19) if VELOCITIES[i][1] == 1]
Z_UP = [(0, 0, 1), (1, 0, 1), (-1, 0, 1), (0, 1, 1), (0, -1, 1)]
Z_UP = [INDEX[v] for v in Z_UP]
Z_PAIR = {}
for _g, _i in enumerate(Z_UP):
    Z_PAIR[_i] = _g
    Z_PAIR[OPPOSITE[_i]] = _g
Z_FROM = [(dx, dz) for dz in (-1, 1) for dx in (0, -1, 1)]
T = 8
LANES = 128
HALF = LANES // 2


def along_of(i, u):
    total = None
    for d in range(3):
        c = VELOCITIES[i][d]
        if c:
            term = u[d] if c > 0 else -u[d]
            total = term if total is None else total + term
    return total


def step_kernel(pop_hbm, solid_hbm, out, pop, solid, S, SU, SD, psi, H, O, A, V, post, zpost,
                YR, WP, XB, XWP, XSND, XE, ZS, YW, ZF, ZD, tally, load_sem, send_sem, recv_sem,
                near_sem, far_sem):
    X, Y, Z = solid.shape
    YT = Y // T
    inner = slice(T, T + Y)
    low, high = slice(0, T), slice(Y + T, Y + 2 * T)
    XX = X + 4
    stride_t = HALF // (YT + 2)
    assert Z == LANES and YT == 2 and X >= 3
    assert stride_t >= 2 * XX and 2 * X <= XX

    me = [lax.axis_index(a) for a in AXES]
    count = [lax.axis_size(a) for a in AXES]
    assert count[1] % 2 == 0
    y_sides = (1,) if count[1] == 2 else (1, -1)
    NY = len(y_sides)
    y_slot = {1: 0, -1: NY - 1}

    loads = [pltpu.make_async_copy(solid_hbm, solid, load_sem.at[0])]
    cuts = [0, X // 2, X]
    for n in range(2):
        part = slice(cuts[n], cuts[n + 1])
        loads.append(
            pltpu.make_async_copy(pop_hbm.at[:, :, part], pop.at[:, :, part], load_sem.at[1 + n])
        )
    for copy in loads:
        copy.start()

    parity = lax.rem(me[1], 2)
    is_near, is_far = parity == 0, parity == 1

    def device(offset):
        return tuple(lax.rem(me[d] + offset[d] + count[d], count[d]) for d in range(3))

    barrier = pltpu.get_barrier_semaphore()
    partner = (me[0], me[1] + 1 - 2 * parity, me[2])
    pairs = [me[1] - parity]
    if count[1] > 2:
        pairs.append(lax.rem(me[1] + 3 * parity - 2 + count[1], count[1]))

    def arrive(place):
        pl.semaphore_signal(barrier, inc=1, device_id=place, device_id_type=MESH)

    for dx in (1, -1, 0):
        for dz in (1, -1):
            place = device((dx, 0, dz))
            for base in pairs:
                arrive((place[0], base + 1, place[2]))
    for dx in (1, -1):
        place = device((dx, 0, 0))
        for base in pairs:
            arrive((place[0], base, place[2]))
    for base in pairs[1:]:
        arrive((me[0], base, me[2]))
    arrive(partner)
    near_count, far_count = 4 + 1, 12 + 1
    if count[1] > 2:
        near_count, far_count = near_count + 6, far_count + 12

    lane = lax.broadcasted_iota(jnp.int32, (T, LANES), 1)
    row = lax.broadcasted_iota(jnp.int32, (T, LANES), 0)
    pair = lane // 2
    even = lane % 2 == 0
    half = lane // HALF
    lower = half == 0
    slot = (lane % stride_t) // 2
    tile_t = (lane % HALF) // stride_t
    own_t = (tile_t > 0) & (tile_t <= YT)
    first, last = lane == 0, lane == Z - 1
    lane_y = lax.broadcasted_iota(jnp.int32, (Y, LANES), 1)
    first_y, last_y = lane_y == 0, lane_y == Z - 1
    upper = row < T // 2

    def roll(v, n):
        n = n % LANES
        return pltpu.roll(v, n, 1) if n else v

    def roll_rows(v, n):
        n = n % T
        return pltpu.roll(v, n, 0) if n else v

    def swap(v):
        return jnp.where(even, roll(v, -1), roll(v, 1))

    GROUPS = {"y": 0, "yW": 1, "xS": 2, "xE": 3, "zF": 4, "zD": 5, "xB": 6}
    sent = [0]

    def send(group, src, dst, offset, tiles):
        pltpu.make_async_remote_copy(
            src_ref=src,
            dst_ref=dst,
            send_sem=send_sem,
            recv_sem=recv_sem.at[GROUPS[group]],
            device_id=device(offset),
            device_id_type=MESH,
        ).start()
        sent[0] += tiles

    def await_(group, ref):
        pltpu.make_async_copy(ref, ref, recv_sem.at[GROUPS[group]]).wait()

    @pl.when(is_near)
    def _():
        pl.semaphore_wait(barrier, near_count)
        pl.semaphore_signal(near_sem, inc=1, device_id=partner, device_id_type=MESH)

    def moments(x):
        fluid = solid[x] == 0
        total, mom = [], []
        for k in range(2):
            f = [pop[k, i, x] for i in range(19)]
            rho = f[0]
            m = [None, None, None]
            for i in range(1, 19, 2):
                rho = rho + (f[i] + f[i + 1])
                diff = f[i] - f[i + 1]
                for d in range(3):
                    c = VELOCITIES[i][d]
                    if c:
                        m[d] = (
                            (diff if c > 0 else -diff)
                            if m[d] is None
                            else (m[d] + diff if c > 0 else m[d] - diff)
                        )
            total.append(rho)
            S[k, 2 + x, inner] = jnp.where(fluid, rho, -WALL[k])
            mom.append([v * INV[k] if INV[k] != 1.0 else v for v in m])
        scale = 1.0 / (total[0] * INV[0] + total[1] * INV[1])
        for d in range(3):
            V[d, 1 + x, 0:Y] = (mom[0][d] + mom[1][d]) * scale

    loads[0].wait()
    for n in range(2):
        loads[1 + n].wait()
        for x in range(cuts[n], cuts[n + 1]):
            moments(x)

    @pl.when(is_far)
    def _():
        pl.semaphore_wait(near_sem, 1)

    first_up = lax.rem(me[0], 4) != 1
    sides = [jnp.where(first_up, 1, -1), jnp.where(first_up, -1, 1)]

    def send_x_signs(side):
        up = side > 0
        src = jnp.where(up, X, 2)
        dst = jnp.where(up, 0, X + 2)
        send("xS", S.at[:, pl.ds(src, 2), inner], S.at[:, pl.ds(dst, 2), inner],
             (side, 0, 0), 4 * YT)

    def send_x_bulk(side):
        up = side > 0
        n = jnp.where(up, 0, 1)
        to = (side, 0, 0)
        send("xB", V.at[:, jnp.where(up, X, 1), 0:Y], XB.at[n, 0:3], to, 3 * YT)
        for m, i in enumerate(X_UP):
            send("xB", pop.at[1, jnp.where(up, i, OPPOSITE[i]), jnp.where(up, X - 1, 0)],
                 XB.at[n, 3 + m], to, YT)

    send_x_signs(sides[0])
    for n, side in enumerate((1, -1)):
        tile = slice(Y - T, Y) if side > 0 else slice(0, T)
        wide = slice(Y, Y + T) if side > 0 else slice(T, 2 * T)
        to = (0, side, 0)
        send("y", S.at[:, 2:2 + X, wide], YR.at[n, 0:2], to, 2 * X)
        send("y", V.at[:, 1:1 + X, tile], YR.at[n, 2:5], to, 3 * X)
        for m, i in enumerate(Y_UP):
            i = i if side > 0 else OPPOSITE[i]
            send("y", pop.at[1, i, :, tile], YR.at[n, 5 + m], to, X)

    blank = jnp.zeros((T, LANES), jnp.float32)
    packs = [blank, blank, blank, blank]
    POP_PLACE = [(2, 0, 0), (2, 0, 1), (2, 1, 0), (2, 1, 1), (3, 1, 0)]
    V_PLACE = [(1, 0, 0), (1, 0, 1), (1, 1, 0)]

    def put(p, h, b, t, x, value):
        j = (h * HALF + t * stride_t + (b * X + x) * 2) // 2
        packs[p] = jnp.where(pair == j, roll(value, 2 * j + 1), packs[p])

    for x in range(X):
        for t in range(1, YT + 1):
            rows = slice(T * t, T * t + T)
            rows_v = slice(T * (t - 1), T * t)
            for k in range(2):
                value = S[k, 2 + x, rows]
                put(0, k, 0, t, x, value)
                put(0, k, 1, t, x, jnp.where(lane < HALF, roll(value, -1), roll(value, 1)))
            for d in range(3):
                put(*V_PLACE[d], t, x, V[d, 1 + x, rows_v])
            for g, i in enumerate(Z_UP):
                value = jnp.where(lane < HALF, pop[1, OPPOSITE[i], x, rows_v], pop[1, i, x, rows_v])
                put(*POP_PLACE[g], t, x, value)
    place = slot % X
    diag = jnp.where((place == X - 1) == even, roll(packs[2], HALF), roll(packs[2], 2 * X))
    packs[1] = jnp.where((half == 1) & (slot >= X) & (slot < 2 * X), diag, packs[1])

    def edges(v, q):
        return jnp.where(upper, roll(v, (q - 1) * stride_t), roll(v, (q - YT) * stride_t))

    merged = edges(packs[0], 0)
    for p in range(1, 4):
        merged = jnp.where(tile_t == p, edges(packs[p], p), merged)
    for p in range(4):
        ZS[p] = packs[p]
    ZS[4] = merged
    for n in range(2):
        if n == 0:
            tile = jnp.where(place >= X - 2, packs[0], roll(packs[1], -2 * (X - 1)))
        else:
            tile = jnp.where(place < 2, packs[0], roll(packs[1], 2 * (X - 1)))
        XSND[n, 0] = jnp.where(tile_t == 0, edges(tile, 0), tile)

    def ends(a, b):
        return jnp.where(upper, a, b)

    t_first, t_last = slice(0, T), slice(Y - T, Y)
    s_first, s_last = slice(T, 2 * T), slice(Y, Y + T)
    keep_rows = (row < 2) | (row >= T - 2)
    for n, side in enumerate((1, -1)):
        planes = (X, X + 1) if side > 0 else (2, 3)
        for m, p in enumerate(planes):
            both = [ends(S[k, p, s_first], S[k, p, s_last]) for k in range(2)]
            XSND[n, 1 + m] = jnp.where(keep_rows, both[0], roll_rows(both[1], 4))
        x = X - 1 if side > 0 else 0
        up, down = INDEX[(side, 1, 0)], INDEX[(side, -1, 0)]
        fields = [ends(V[d, 1 + x, t_first], V[d, 1 + x, t_last]) for d in range(3)]
        fields.append(ends(pop[1, down, x, t_first], pop[1, up, x, t_last]))
        packed = fields[0]
        for f in range(1, 4):
            at = (row == 2 * f - 1) | (row == 2 * f)
            packed = jnp.where(at, roll_rows(fields[f], 2 * f), packed)
        XSND[n, 3] = packed

    for n, side in enumerate((1, -1)):
        send("xE", XSND.at[n, 0:1], XE.at[n, 0:1], (side, 0, 0), 1)
        for sy in y_sides:
            m = 1 + 4 * y_slot[-sy]
            send("xE", XSND.at[n], XE.at[n, m:m + 4], (side, sy, 0), 4)
    for sy in y_sides:
        send("yW", ZS.at[4], YW.at[y_slot[-sy]], (0, sy, 0), 1)
    send_x_bulk(sides[0])
    send_x_signs(sides[1])
    send_x_bulk(sides[1])

    @pl.when(is_far)
    def _():
        pl.semaphore_wait(barrier, far_count)
        pl.semaphore_signal(far_sem, inc=1, device_id=partner, device_id_type=MESH)

    @pl.when(is_near)
    def _():
        pl.semaphore_wait(far_sem, 1)

    for n, side in enumerate((1, -1)):
        for m, dz in enumerate((1, -1)):
            send("zD", XSND.at[n, 0], ZD.at[m, n, 0], (side, 0, dz), 1)
            for sy in y_sides:
                send("zD", XSND.at[n, 0], ZD.at[m, n, 1 + y_slot[-sy]], (side, sy, dz), 1)
    for m, dz in enumerate((1, -1)):
        send("zF", ZS.at[0:4], ZF.at[m, 0:4], (0, 0, dz), 4)
        for sy in y_sides:
            send("zF", ZS.at[4], ZF.at[m, 4 + y_slot[-sy]], (0, sy, dz), 1)

    await_("y", YR)
    for x in range(X):
        for k in range(2):
            value = ends(YR[1, k, x], YR[0, k, x])
            S[k, 2 + x, low] = value
            S[k, 2 + x, high] = value
        for d in range(3):
            V[d, 1 + x, Y:Y + T] = ends(YR[1, 2 + d, x], YR[0, 2 + d, x])
        for m in range(5):
            WP[m, x] = ends(YR[1, 5 + m, x], YR[0, 5 + m, x])

    def window(w, dy):
        if w == 0:
            return slice(T + dy, T + dy + Y)
        return slice(Y + T - 1, Y + 2 * T - 1) if dy < 0 else slice(dy, T + dy)

    def rows_of(w):
        return slice(0, Y) if w == 0 else slice(Y, Y + T)

    def prepare(p):
        for k in range(2):
            for t in range(YT + 1):
                rows = slice(T * t, T * t + T)
                value = S[k, p, rows]
                SU[k, p, rows] = roll(value, -1)
                SD[k, p, rows] = roll(value, 1)

    def spread(tile, k, t, xx):
        return roll(tile, LANES - 1 - (k * HALF + t * stride_t + 2 * xx))

    def complete(p, signs):
        for k in range(2):
            for t in range(YT + 1):
                rows = slice(T * t, T * t + T)
                edge = spread(signs, k, t, p)
                above = jnp.where(last, edge, SU[k, p, rows])
                below = jnp.where(first, edge, SD[k, p, rows])
                size = jnp.abs(S[k, p, rows])
                a_above, a_below = jnp.abs(above), jnp.abs(below)
                for r in (rows,) if t else (low, high):
                    psi[k, p, r] = size
                    H[k, p, r] = 2.0 * size + (a_above + a_below)
                    O[k, p, r] = a_above - a_below
                    if k == 0:
                        SU[k, p, r] = above
                        SD[k, p, r] = below

    def sums(p):
        for k in range(2):
            for w in range(2):
                A[k, p, rows_of(w)] = (
                    H[k, p, window(w, 0)] + (psi[k, p, window(w, 1)] + psi[k, p, window(w, -1)])
                ) * (1.0 / 36.0)

    def gradient(k, p, w):
        gx = A[k, p + 1, rows_of(w)] - A[k, p - 1, rows_of(w)]
        sides_y = []
        for dy in (1, -1):
            r = window(w, dy)
            sides_y.append(H[k, p, r] + (psi[k, p + 1, r] + psi[k, p - 1, r]))
        gy = (sides_y[0] - sides_y[1]) * (1.0 / 36.0)
        r = window(w, 0)
        gz = 2.0 * O[k, p, r] + (O[k, p + 1, r] + O[k, p - 1, r])
        gz = (gz + (O[k, p, window(w, 1)] + O[k, p, window(w, -1)])) * (1.0 / 36.0)
        return gx, gy, gz

    def velocities(common, x, w):
        grads = [gradient(k, x + 2, w) for k in range(2)]
        return [
            [common[d] - (COUPLING * RELAX[k]) * grads[1 - k][d] for d in range(3)]
            for k in range(2)
        ]

    def common_of(x, w):
        return [V[d, 1 + x, rows_of(w)] for d in range(3)]

    def flat_of(u):
        return 1.0 - 1.5 * (u[0] * u[0] + u[1] * u[1] + u[2] * u[2])

    def one_way(w, flat, along, sign):
        even_part = w * (flat + 4.5 * (along * along))
        return even_part + w * ((3.0 * sign) * along)

    def collide_own(x):
        us = velocities(common_of(x, 0), x, 0)
        for k in range(2):
            u = us[k]
            rho = psi[k, 2 + x, inner] * INV[k]
            flat = flat_of(u)
            scaled = {w: rho * w for w in sorted(set(WEIGHTS))}
            values = {0: scaled[WEIGHTS[0]] * flat}
            for i in range(1, 19, 2):
                along = along_of(i, u)
                w = scaled[WEIGHTS[i]]
                even_part = w * (flat + 4.5 * (along * along))
                odd_part = w * (3.0 * along)
                values[i] = even_part + odd_part
                values[i + 1] = even_part - odd_part
            for i in range(19):
                if abs(KEEP[k]) > 1e-9:
                    values[i] = values[i] + KEEP[k] * pop[k, i, x]
                post[k, i, 1 + x, inner] = values[i]

    row_sign = jnp.where(upper, -1.0, 1.0)

    def collide_rows(x):
        us = velocities(common_of(x, 1), x, 1)
        for k in range(2):
            u = us[k]
            rho = psi[k, 2 + x, low] * INV[k]
            flat = flat_of(u)
            for m, i in enumerate(Y_UP):
                w = rho * WEIGHTS[i]
                value = one_way(w, flat, along_of(i, u), row_sign)
                if abs(KEEP[k]) > 1e-9:
                    value = value + KEEP[k] * WP[m, x]
                post[k, i, 1 + x, low] = value
                post[k, OPPOSITE[i], 1 + x, high] = value

    def collide_plane(n):
        x = -1 if n == 0 else X
        sign = 1.0 if n == 0 else -1.0
        us = velocities([XB[n, d] for d in range(3)], x, 0)
        for k in range(2):
            u = us[k]
            rho = psi[k, 2 + x, inner] * INV[k]
            flat = flat_of(u)
            for m, i in enumerate(X_UP):
                value = one_way(rho * WEIGHTS[i], flat, along_of(i, u), sign)
                if abs(KEEP[k]) > 1e-9:
                    value = value + KEEP[k] * XB[n, 3 + m]
                post[k, i if n == 0 else OPPOSITE[i], 1 + x, inner] = value

    def collide_corner(n):
        x = -1 if n == 0 else X
        sign = 1.0 if n == 0 else -1.0
        us = velocities(common_of(x, 1), x, 1)
        cx = 1 if n == 0 else -1
        up, down = INDEX[(cx, 1, 0)], INDEX[(cx, -1, 0)]
        for k in range(2):
            u = us[k]
            rho = psi[k, 2 + x, low] * INV[k]
            value = one_way(rho * WEIGHTS[up], flat_of(u), sign * u[0] + row_sign * u[1], 1.0)
            if abs(KEEP[k]) > 1e-9:
                value = value + KEEP[k] * XWP[n]
            post[k, up, 1 + x, low] = value
            post[k, down, 1 + x, high] = value

    def x_up(v):
        return roll(v, -2)

    def x_down(v):
        return roll(v, 2)

    def y_up(v):
        r = roll_rows(v, -1)
        return jnp.where(row == T - 1, roll(r, -stride_t), r)

    def y_down(v):
        r = roll_rows(v, 1)
        return jnp.where(row == 0, roll(r, stride_t), r)

    def collide_z(s0, s1, s2, t1, t2, olds):
        other1, other2 = roll(t1, HALF), roll(t2, HALF)
        common = [
            jnp.where(lower, t1, other1),
            jnp.where(lower, t2, other2),
            jnp.where(lower, other1, t1),
        ]
        p0, p1, p2 = jnp.abs(s0), jnp.abs(s1), jnp.abs(s2)
        xs = [x_up(v) + x_down(v) for v in (p0, p1, p2)]
        ys = [y_up(v) + y_down(v) for v in (p0, p1, p2)]
        g = 2.0 * p1 + (p0 + p2)
        a = g + ys[1]
        b = g + xs[1]
        c0 = 2.0 * p0 + (xs[0] + ys[0])
        c2 = 2.0 * p2 + (xs[2] + ys[2])
        sign = jnp.where(even, 1.0, -1.0)
        grads = [
            (x_up(a) - x_down(a)) * (1.0 / 36.0),
            (y_up(b) - y_down(b)) * (1.0 / 36.0),
            (c0 - c2) * (sign * (1.0 / 36.0)),
        ]
        factor = jnp.where(lower, COUPLING * RELAX[0], COUPLING * RELAX[1])
        u = [common[d] - factor * roll(grads[d], HALF) for d in range(3)]
        rho = p1 * jnp.where(lower, INV[0], INV[1])
        keep = jnp.where(lower, KEEP[0], KEEP[1])
        flat = flat_of(u)
        beyond = (slot < 2) | (slot >= X + 2)
        for g, i in enumerate(Z_UP):
            c = VELOCITIES[i]
            old = jnp.where(beyond, t2, olds[g]) if c[0] else olds[g]
            value = one_way(rho * WEIGHTS[i], flat, along_of(i, u), sign)
            value = value + keep * jnp.where(lower, 0.0, old)
            if c[0]:
                value = jnp.where(even, roll(value, 2 * c[0]), roll(value, -2 * c[0]))
            if c[1]:
                a, b = (y_down, y_up) if c[1] > 0 else (y_up, y_down)
                value = jnp.where(even, a(value), b(value))
            value = swap(value)
            for k in range(2):
                for x in range(X):
                    for t in range(1, YT + 1):
                        zpost[k, g, x, T * (t - 1):T * t] = spread(value, k, t, x + 2)

    def stream(x):
        fluid = solid[x] == 0
        for k in range(2):
            for i in range(19):
                c = VELOCITIES[i]
                rows = slice(T - c[1], T - c[1] + Y)
                read = post[k, i, 1 + x - c[0], rows]
                if i:
                    if c[2]:
                        at = first_y if c[2] > 0 else last_y
                        read = jnp.where(at, zpost[k, Z_PAIR[i], x], roll(read, c[2]))
                    p = 2 + x - c[0]
                    signs = SD if c[2] > 0 else (SU if c[2] else S)
                    bounced = post[k, OPPOSITE[i], 1 + x, inner]
                    read = jnp.where(signs[0, p, rows] > 0.0, read, bounced)
                out[k, i, x] = jnp.where(fluid, read, pop[k, i, x])

    for x in range(X):
        prepare(2 + x)

    def with_rows(tile, w_low, w_high):
        return jnp.where(own_t, tile, jnp.where(tile_t == 0, w_low, w_high))

    def by_row(low_part, high_part):
        return low_part if NY == 1 else ends(low_part, high_part)

    top = stride_t * (YT + 1)

    await_("zF", ZF)
    faces = [jnp.where(even, ZF[0, p], ZF[1, p]) for p in range(4 + NY)]
    z_rows = by_row(faces[4 + y_slot[1]], faces[4 + y_slot[-1]])
    full = [
        with_rows(faces[p], roll(z_rows, -stride_t * p), roll(z_rows, top - stride_t * p))
        for p in range(4)
    ]
    center = [[roll(full[p], 2 * (2 - b * X)) for b in range(2)] for p in range(2)]
    olds = []
    for p, h, b in POP_PLACE:
        olds.append(roll(full[p], 2 * (2 - b * X) + HALF * (1 - h)))
    near_signs = swap(center[0][0])
    for x in range(X):
        complete(2 + x, near_signs)
    for x in range(X):
        sums(2 + x)
    for x in range(1, X - 1):
        collide_own(x)
        collide_rows(x)

    await_("yW", YW)
    await_("xS", S.at[:, 0:4, inner])
    await_("xE", XE)
    for n in range(2):
        planes = (0, 1) if n == 0 else (X + 2, X + 3)
        ups, downs = 1 + 4 * y_slot[1], 1 + 4 * y_slot[-1]
        for m, p in enumerate(planes):
            value = XE[n, ups + 1 + m]
            if NY > 1:
                value = jnp.where(row % 4 < 2, value, XE[n, downs + 1 + m])
            other = roll_rows(value, 4)
            for k, w in ((0, value), (1, other)):
                S[k, p, low] = w
                S[k, p, high] = w
        value = XE[n, ups + 3]
        if NY > 1:
            value = jnp.where(row % 2 == 0, value, XE[n, downs + 3])
        plane = 0 if n == 0 else X + 1
        for d in range(3):
            V[d, plane, Y:Y + T] = roll_rows(value, -2 * d)
        XWP[n] = roll_rows(value, -6)
    outer = [0, 1, X + 2, X + 3]
    for p in outer:
        prepare(p)

    def assemble(middle, left, right, shift_left, shift_right):
        return jnp.where(
            slot < 2,
            roll(left, 2 * shift_left),
            jnp.where(slot >= X + 2, roll(right, 2 * shift_right), middle),
        )

    y_rows = by_row(YW[y_slot[1]], YW[y_slot[-1]])
    own = with_rows(ZS[0], y_rows, roll(y_rows, top))
    beside = []
    for n in range(2):
        w = by_row(XE[n, 1 + 4 * y_slot[1]], XE[n, 1 + 4 * y_slot[-1]])
        beside.append(with_rows(XE[n, 0], w, roll(w, top)))
    s0 = swap(assemble(roll(own, 4), beside[0], beside[1], 2 - X, X + 2))

    await_("zD", ZD)
    diags = []
    for n in range(2):
        merged = [jnp.where(even, ZD[0, n, q], ZD[1, n, q]) for q in range(1 + NY)]
        w = by_row(merged[1 + y_slot[1]], merged[1 + y_slot[-1]])
        diags.append(with_rows(merged[0], w, roll(w, top)))
    s1, s2 = [
        assemble(center[0][b], *diags, -(b * X + X - 2), X + 2 - b * X) for b in range(2)
    ]
    t1, t2 = [assemble(center[1][b], *diags, 1 - b * X, 3 - b * X) for b in range(2)]
    signs = swap(s1)
    for p in outer:
        complete(p, signs)
    for p in outer:
        sums(p)
    for x in (0, X - 1):
        collide_own(x)
        collide_rows(x)
    collide_z(s0, s1, s2, t1, t2, olds)
    for n in range(2):
        collide_corner(n)
    for x in range(1, X - 1):
        stream(x)
    await_("xB", XB)
    for n in range(2):
        collide_plane(n)
    for x in (0, X - 1):
        stream(x)
    assert sent[0] == tally.shape[0]
    pltpu.make_async_copy(tally, tally, send_sem).wait()


def body(populations, solid):
    X, Y, Z = solid.shape
    f32 = jnp.float32
    dma = pltpu.SemaphoreType.DMA
    R = Y + 2 * T
    XX = X + 4
    NY = 1 if lax.axis_size("gy") == 2 else 2
    YT = Y // T
    tiles = 20 * X + 24 * YT + 14 + 15 * NY

    def vmem(*shape):
        return pltpu.VMEM(shape, f32)

    return pl.pallas_call(
        step_kernel,
        out_shape=pltpu.VMEM(populations.shape, f32),
        in_specs=[pl.BlockSpec(memory_space=pl.ANY)] * 2,
        out_specs=pl.BlockSpec(memory_space=pltpu.VMEM),
        scratch_shapes=[
            vmem(*populations.shape),
            pltpu.VMEM(solid.shape, jnp.int32),
            vmem(2, XX, R, Z),
            vmem(2, XX, R, Z),
            vmem(2, XX, R, Z),
            vmem(2, XX, R, Z),
            vmem(2, XX, R, Z),
            vmem(2, XX, R, Z),
            vmem(2, XX, Y + T, Z),
            vmem(3, X + 2, Y + T, Z),
            vmem(2, 19, X + 2, R, Z),
            vmem(2, 5, X, Y, Z),
            vmem(2, 10, X, T, Z),
            vmem(5, X, T, Z),
            vmem(2, 8, Y, Z),
            vmem(2, T, Z),
            vmem(2, 4, T, LANES),
            vmem(2, 1 + 4 * NY, T, LANES),
            vmem(5, T, LANES),
            vmem(NY, T, LANES),
            vmem(2, 4 + NY, T, LANES),
            vmem(2, 2, 1 + NY, T, LANES),
            vmem(tiles, T, LANES),
            dma((3,)),
            dma,
            dma((7,)),
            pltpu.SemaphoreType.REGULAR,
            pltpu.SemaphoreType.REGULAR,
        ],
        compiler_params=pltpu.CompilerParams(collective_id=0, has_side_effects=True),
    )(populations, solid)


def solution(mesh):
    in_specs = (P(None, None, "gx", "gy", "gz"), P("gx", "gy", "gz"))
    out_specs = P(None, None, "gx", "gy", "gz")
    return jax.shard_map(body, mesh=mesh, in_specs=in_specs, out_specs=out_specs, check_vma=False)
```

```python
import jax
import jax.numpy as jnp
from jax import lax
from jax.experimental import pallas as pl
from jax.experimental.pallas import tpu as pltpu
from jax.sharding import PartitionSpec as P

VELOCITIES = [
    (0, 0, 0),
    (1, 0, 0),
    (-1, 0, 0),
    (0, 1, 0),
    (0, -1, 0),
    (0, 0, 1),
    (0, 0, -1),
    (1, 1, 0),
    (-1, -1, 0),
    (1, -1, 0),
    (-1, 1, 0),
    (1, 0, 1),
    (-1, 0, -1),
    (1, 0, -1),
    (-1, 0, 1),
    (0, 1, 1),
    (0, -1, -1),
    (0, 1, -1),
    (0, -1, 1),
]
WEIGHTS = [1.0 / 3.0] + [1.0 / 18.0] * 6 + [1.0 / 36.0] * 12
OPPOSITE = [0, 2, 1, 4, 3, 6, 5, 8, 7, 10, 9, 12, 11, 14, 13, 16, 15, 18, 17]
INDEX = {v: i for i, v in enumerate(VELOCITIES)}
COUPLING = 0.9
RELAX = (1.0, 0.8)
WALL = (0.3, 1.5)
INV = [1.0 / t for t in RELAX]
KEEP = [1.0 - v for v in INV]
AXES = ("gx", "gy", "gz")
MESH = pl.DeviceIdType.MESH

X_UP = [i for i in range(19) if VELOCITIES[i][0] == 1]
Y_UP = [i for i in range(19) if VELOCITIES[i][1] == 1]
Z_UP = [(0, 0, 1), (1, 0, 1), (-1, 0, 1), (0, 1, 1), (0, -1, 1)]
Z_UP = [INDEX[v] for v in Z_UP]
Z_PAIR = {}
for _g, _i in enumerate(Z_UP):
    Z_PAIR[_i] = _g
    Z_PAIR[OPPOSITE[_i]] = _g
Z_FROM = [(dx, dz) for dz in (-1, 1) for dx in (0, -1, 1)]
T = 8
LANES = 128
HALF = LANES // 2


def along_of(i, u):
    total = None
    for d in range(3):
        c = VELOCITIES[i][d]
        if c:
            term = u[d] if c > 0 else -u[d]
            total = term if total is None else total + term
    return total


def step_kernel(pop_hbm, solid_hbm, out, pop, solid, S, SU, SD, psi, H, O, A, V, post, zpost,
                YR, WP, XB, XWP, XSND, XE, ZS, YW, ZF, ZD, tally, load_sem, send_sem, recv_sem,
                near_sem, far_sem):
    X, Y, Z = solid.shape
    YT = Y // T
    inner = slice(T, T + Y)
    low, high = slice(0, T), slice(Y + T, Y + 2 * T)
    XX = X + 4
    stride_t = HALF // (YT + 2)
    assert Z == LANES and YT == 2 and X >= 3
    assert stride_t >= 2 * XX and 2 * X <= XX

    me = [lax.axis_index(a) for a in AXES]
    count = [lax.axis_size(a) for a in AXES]
    assert count[1] % 2 == 0
    y_sides = (1,) if count[1] == 2 else (1, -1)
    NY = len(y_sides)
    y_slot = {1: 0, -1: NY - 1}

    loads = [pltpu.make_async_copy(solid_hbm, solid, load_sem.at[0])]
    cuts = [0, X // 2, X]
    for n in range(2):
        part = slice(cuts[n], cuts[n + 1])
        loads.append(
            pltpu.make_async_copy(pop_hbm.at[:, :, part], pop.at[:, :, part], load_sem.at[1 + n])
        )
    for copy in loads:
        copy.start()

    parity = lax.rem(me[1], 2)
    is_near, is_far = parity == 0, parity == 1

    def device(offset):
        return tuple(lax.rem(me[d] + offset[d] + count[d], count[d]) for d in range(3))

    barrier = pltpu.get_barrier_semaphore()
    partner = (me[0], me[1] + 1 - 2 * parity, me[2])
    pairs = [me[1] - parity]
    if count[1] > 2:
        pairs.append(lax.rem(me[1] + 3 * parity - 2 + count[1], count[1]))

    def arrive(place):
        pl.semaphore_signal(barrier, inc=1, device_id=place, device_id_type=MESH)

    for dx in (1, -1, 0):
        for dz in (1, -1):
            place = device((dx, 0, dz))
            for base in pairs:
                arrive((place[0], base + 1, place[2]))
    for dx in (1, -1):
        place = device((dx, 0, 0))
        for base in pairs:
            arrive((place[0], base, place[2]))
    for base in pairs[1:]:
        arrive((me[0], base, me[2]))
    arrive(partner)
    near_count, far_count = 4 + 1, 12 + 1
    if count[1] > 2:
        near_count, far_count = near_count + 6, far_count + 12

    lane = lax.broadcasted_iota(jnp.int32, (T, LANES), 1)
    row = lax.broadcasted_iota(jnp.int32, (T, LANES), 0)
    pair = lane // 2
    even = lane % 2 == 0
    half = lane // HALF
    lower = half == 0
    slot = (lane % stride_t) // 2
    tile_t = (lane % HALF) // stride_t
    own_t = (tile_t > 0) & (tile_t <= YT)
    first, last = lane == 0, lane == Z - 1
    lane_y = lax.broadcasted_iota(jnp.int32, (Y, LANES), 1)
    first_y, last_y = lane_y == 0, lane_y == Z - 1
    upper = row < T // 2

    def roll(v, n):
        n = n % LANES
        return pltpu.roll(v, n, 1) if n else v

    def roll_rows(v, n):
        n = n % T
        return pltpu.roll(v, n, 0) if n else v

    def swap(v):
        return jnp.where(even, roll(v, -1), roll(v, 1))

    GROUPS = {"y": 0, "yW": 1, "xS": 2, "xE": 3, "zF": 4, "zD": 5, "xB": 6}
    sent = [0]

    def send(group, src, dst, offset, tiles):
        pltpu.make_async_remote_copy(
            src_ref=src,
            dst_ref=dst,
            send_sem=send_sem,
            recv_sem=recv_sem.at[GROUPS[group]],
            device_id=device(offset),
            device_id_type=MESH,
        ).start()
        sent[0] += tiles

    def await_(group, ref):
        pltpu.make_async_copy(ref, ref, recv_sem.at[GROUPS[group]]).wait()

    def moments(x):
        fluid = solid[x] == 0
        total, mom = [], []
        for k in range(2):
            f = [pop[k, i, x] for i in range(19)]
            rho = f[0]
            m = [None, None, None]
            for i in range(1, 19, 2):
                rho = rho + (f[i] + f[i + 1])
                diff = f[i] - f[i + 1]
                for d in range(3):
                    c = VELOCITIES[i][d]
                    if c:
                        m[d] = (
                            (diff if c > 0 else -diff)
                            if m[d] is None
                            else (m[d] + diff if c > 0 else m[d] - diff)
                        )
            total.append(rho)
            S[k, 2 + x, inner] = jnp.where(fluid, rho, -WALL[k])
            mom.append([v * INV[k] if INV[k] != 1.0 else v for v in m])
        scale = 1.0 / (total[0] * INV[0] + total[1] * INV[1])
        for d in range(3):
            V[d, 1 + x, 0:Y] = (mom[0][d] + mom[1][d]) * scale

    blank = jnp.zeros((T, LANES), jnp.float32)
    packs = [blank, blank, blank, blank]
    POP_PLACE = [(2, 0, 0), (2, 0, 1), (2, 1, 0), (2, 1, 1), (3, 1, 0)]
    V_PLACE = [(1, 0, 0), (1, 0, 1), (1, 1, 0)]

    def put(p, h, b, t, x, value, inside=False):
        j = (h * HALF + t * stride_t + (b * X + x) * 2) // 2
        if inside:
            value = jnp.where(even, roll(value, 2 * j + 2), roll(value, 2 * j))
        else:
            value = roll(value, 2 * j + 1)
        packs[p] = jnp.where(pair == j, value, packs[p])

    def z_ends(i, x, t):
        rows = slice(T * (t - 1), T * t)
        return jnp.where(lane < HALF, pop[1, OPPOSITE[i], x, rows], pop[1, i, x, rows])

    def pack_signs(x):
        for t in range(1, YT + 1):
            for k in range(2):
                value = S[k, 2 + x, T * t:T * t + T]
                put(0, k, 0, t, x, value)
                put(0, k, 1, t, x, value, inside=True)
            for d in range(3):
                put(*V_PLACE[d], t, x, V[d, 1 + x, T * (t - 1):T * t])
            if x in (0, X - 1):
                out_i, in_i = (Z_UP[1], Z_UP[2]) if x else (Z_UP[2], Z_UP[1])
                rows = slice(T * (t - 1), T * t)
                value = jnp.where(lane < HALF, pop[1, OPPOSITE[in_i], x, rows], pop[1, out_i, x, rows])
                put(1, 1, 1, t, x, value)

    loads[0].wait()
    for n in range(2):
        loads[1 + n].wait()
        for x in range(cuts[n], cuts[n + 1]):
            moments(x)
        for x in range(cuts[n], cuts[n + 1]):
            pack_signs(x)

    place = slot % X

    def edges(v, q):
        return jnp.where(upper, roll(v, (q - 1) * stride_t), roll(v, (q - YT) * stride_t))

    for n in range(2):
        if n == 0:
            tile = jnp.where(place >= X - 2, packs[0], roll(packs[1], -2 * (X - 1)))
        else:
            tile = jnp.where(place < 2, packs[0], roll(packs[1], 2 * (X - 1)))
        XSND[n, 0] = jnp.where(tile_t == 0, edges(tile, 0), tile)

    def ends(a, b):
        return jnp.where(upper, a, b)

    t_first, t_last = slice(0, T), slice(Y - T, Y)
    s_first, s_last = slice(T, 2 * T), slice(Y, Y + T)
    keep_rows = (row < 2) | (row >= T - 2)
    for n, side in enumerate((1, -1)):
        planes = (X, X + 1) if side > 0 else (2, 3)
        for m, p in enumerate(planes):
            both = [ends(S[k, p, s_first], S[k, p, s_last]) for k in range(2)]
            XSND[n, 1 + m] = jnp.where(keep_rows, both[0], roll_rows(both[1], 4))
        x = X - 1 if side > 0 else 0
        up, down = INDEX[(side, 1, 0)], INDEX[(side, -1, 0)]
        fields = [ends(V[d, 1 + x, t_first], V[d, 1 + x, t_last]) for d in range(3)]
        fields.append(ends(pop[1, down, x, t_first], pop[1, up, x, t_last]))
        packed = fields[0]
        for f in range(1, 4):
            at = (row == 2 * f - 1) | (row == 2 * f)
            packed = jnp.where(at, roll_rows(fields[f], 2 * f), packed)
        XSND[n, 3] = packed

    top_z = me[2] == count[2] - 1
    not_top = jnp.logical_not(top_z)

    def tell(sem):
        pl.semaphore_signal(sem, inc=1, device_id=partner, device_id_type=MESH)

    def learn_far():
        pl.semaphore_wait(barrier, far_count)
        tell(far_sem)

    @pl.when(is_near)
    def _():
        pl.semaphore_wait(barrier, near_count)
        tell(near_sem)

    @pl.when(is_far & top_z)
    def _():
        learn_far()

    @pl.when(is_far)
    def _():
        pl.semaphore_wait(near_sem, 1)

    first_up = lax.rem(me[0], 4) != 1
    sides = [jnp.where(first_up, 1, -1), jnp.where(first_up, -1, 1)]

    def send_x_signs(side):
        up = side > 0
        src = jnp.where(up, X, 2)
        dst = jnp.where(up, 0, X + 2)
        send("xS", S.at[:, pl.ds(src, 2), inner], S.at[:, pl.ds(dst, 2), inner],
             (side, 0, 0), 4 * YT)

    def send_x_bulk(side):
        up = side > 0
        n = jnp.where(up, 0, 1)
        to = (side, 0, 0)
        send("xB", V.at[:, jnp.where(up, X, 1), 0:Y], XB.at[n, 0:3], to, 3 * YT)
        for m, i in enumerate(X_UP):
            send("xB", pop.at[1, jnp.where(up, i, OPPOSITE[i]), jnp.where(up, X - 1, 0)],
                 XB.at[n, 3 + m], to, YT)

    def send_diagonal():
        for n, side in enumerate((1, -1)):
            for m, dz in enumerate((1, -1)):
                send("zD", XSND.at[n, 0], ZD.at[m, n, 0], (side, 0, dz), 1)
                for sy in y_sides:
                    send("zD", XSND.at[n, 0], ZD.at[m, n, 1 + y_slot[-sy]], (side, sy, dz), 1)

    @pl.when(top_z)
    def _():
        @pl.when(is_near)
        def _():
            pl.semaphore_wait(far_sem, 1)

        send_diagonal()

    send_x_signs(sides[0])
    for n, side in enumerate((1, -1)):
        send("xE", XSND.at[n, 0:1], XE.at[n, 0:1], (side, 0, 0), 1)
        for sy in y_sides:
            m = 1 + 4 * y_slot[-sy]
            send("xE", XSND.at[n], XE.at[n, m:m + 4], (side, sy, 0), 4)
    for n, side in enumerate((1, -1)):
        tile = slice(Y - T, Y) if side > 0 else slice(0, T)
        wide = slice(Y, Y + T) if side > 0 else slice(T, 2 * T)
        to = (0, side, 0)
        send("y", S.at[:, 2:2 + X, wide], YR.at[n, 0:2], to, 2 * X)
        send("y", V.at[:, 1:1 + X, tile], YR.at[n, 2:5], to, 3 * X)
        for m, i in enumerate(Y_UP):
            i = i if side > 0 else OPPOSITE[i]
            send("y", pop.at[1, i, :, tile], YR.at[n, 5 + m], to, X)
    send_x_bulk(sides[0])
    send_x_signs(sides[1])
    send_x_bulk(sides[1])

    for x in range(X):
        for t in range(1, YT + 1):
            for g, i in enumerate(Z_UP):
                put(*POP_PLACE[g], t, x, z_ends(i, x, t))
    merged = edges(packs[0], 0)
    for p in range(1, 4):
        merged = jnp.where(tile_t == p, edges(packs[p], p), merged)
    for p in range(4):
        ZS[p] = packs[p]
    ZS[4] = merged
    for sy in y_sides:
        send("yW", ZS.at[4], YW.at[y_slot[-sy]], (0, sy, 0), 1)

    @pl.when(not_top)
    def _():
        @pl.when(is_far)
        def _():
            learn_far()

        @pl.when(is_near)
        def _():
            pl.semaphore_wait(far_sem, 1)

        send_diagonal()

    sent[0] -= 4 * (1 + NY)
    for m, dz in enumerate((1, -1)):
        send("zF", ZS.at[0:4], ZF.at[m, 0:4], (0, 0, dz), 4)
        for sy in y_sides:
            send("zF", ZS.at[4], ZF.at[m, 4 + y_slot[-sy]], (0, sy, dz), 1)

    await_("y", YR)
    for x in range(X):
        for k in range(2):
            value = ends(YR[1, k, x], YR[0, k, x])
            S[k, 2 + x, low] = value
            S[k, 2 + x, high] = value
        for d in range(3):
            V[d, 1 + x, Y:Y + T] = ends(YR[1, 2 + d, x], YR[0, 2 + d, x])
        for m in range(5):
            WP[m, x] = ends(YR[1, 5 + m, x], YR[0, 5 + m, x])

    def window(w, dy):
        if w == 0:
            return slice(T + dy, T + dy + Y)
        return slice(Y + T - 1, Y + 2 * T - 1) if dy < 0 else slice(dy, T + dy)

    def rows_of(w):
        return slice(0, Y) if w == 0 else slice(Y, Y + T)

    def prepare(p):
        for k in range(2):
            for t in range(YT + 1):
                rows = slice(T * t, T * t + T)
                value = S[k, p, rows]
                SU[k, p, rows] = roll(value, -1)
                SD[k, p, rows] = roll(value, 1)

    def spread(tile, k, t, xx):
        return roll(tile, LANES - 1 - (k * HALF + t * stride_t + 2 * xx))

    def complete(p, signs):
        for k in range(2):
            for t in range(YT + 1):
                rows = slice(T * t, T * t + T)
                edge = spread(signs, k, t, p)
                above = jnp.where(last, edge, SU[k, p, rows])
                below = jnp.where(first, edge, SD[k, p, rows])
                size = jnp.abs(S[k, p, rows])
                a_above, a_below = jnp.abs(above), jnp.abs(below)
                for r in (rows,) if t else (low, high):
                    psi[k, p, r] = size
                    H[k, p, r] = 2.0 * size + (a_above + a_below)
                    O[k, p, r] = a_above - a_below
                    if k == 0:
                        SU[k, p, r] = above
                        SD[k, p, r] = below

    def sums(p):
        for k in range(2):
            for w in range(2):
                A[k, p, rows_of(w)] = (
                    H[k, p, window(w, 0)] + (psi[k, p, window(w, 1)] + psi[k, p, window(w, -1)])
                ) * (1.0 / 36.0)

    def gradient(k, p, w):
        gx = A[k, p + 1, rows_of(w)] - A[k, p - 1, rows_of(w)]
        sides_y = []
        for dy in (1, -1):
            r = window(w, dy)
            sides_y.append(H[k, p, r] + (psi[k, p + 1, r] + psi[k, p - 1, r]))
        gy = (sides_y[0] - sides_y[1]) * (1.0 / 36.0)
        r = window(w, 0)
        gz = 2.0 * O[k, p, r] + (O[k, p + 1, r] + O[k, p - 1, r])
        gz = (gz + (O[k, p, window(w, 1)] + O[k, p, window(w, -1)])) * (1.0 / 36.0)
        return gx, gy, gz

    def velocities(common, x, w):
        grads = [gradient(k, x + 2, w) for k in range(2)]
        return [
            [common[d] - (COUPLING * RELAX[k]) * grads[1 - k][d] for d in range(3)]
            for k in range(2)
        ]

    def common_of(x, w):
        return [V[d, 1 + x, rows_of(w)] for d in range(3)]

    def flat_of(u):
        return 1.0 - 1.5 * (u[0] * u[0] + u[1] * u[1] + u[2] * u[2])

    def one_way(w, flat, along, sign):
        even_part = w * (flat + 4.5 * (along * along))
        return even_part + w * ((3.0 * sign) * along)

    def collide_own(x):
        us = velocities(common_of(x, 0), x, 0)
        for k in range(2):
            u = us[k]
            rho = psi[k, 2 + x, inner] * INV[k]
            flat = flat_of(u)
            scaled = {w: rho * w for w in sorted(set(WEIGHTS))}
            values = {0: scaled[WEIGHTS[0]] * flat}
            for i in range(1, 19, 2):
                along = along_of(i, u)
                w = scaled[WEIGHTS[i]]
                even_part = w * (flat + 4.5 * (along * along))
                odd_part = w * (3.0 * along)
                values[i] = even_part + odd_part
                values[i + 1] = even_part - odd_part
            for i in range(19):
                if abs(KEEP[k]) > 1e-9:
                    values[i] = values[i] + KEEP[k] * pop[k, i, x]
                post[k, i, 1 + x, inner] = values[i]

    row_sign = jnp.where(upper, -1.0, 1.0)

    def collide_rows(x):
        us = velocities(common_of(x, 1), x, 1)
        for k in range(2):
            u = us[k]
            rho = psi[k, 2 + x, low] * INV[k]
            flat = flat_of(u)
            for m, i in enumerate(Y_UP):
                w = rho * WEIGHTS[i]
                value = one_way(w, flat, along_of(i, u), row_sign)
                if abs(KEEP[k]) > 1e-9:
                    value = value + KEEP[k] * WP[m, x]
                post[k, i, 1 + x, low] = value
                post[k, OPPOSITE[i], 1 + x, high] = value

    def collide_plane(n):
        x = -1 if n == 0 else X
        sign = 1.0 if n == 0 else -1.0
        us = velocities([XB[n, d] for d in range(3)], x, 0)
        for k in range(2):
            u = us[k]
            rho = psi[k, 2 + x, inner] * INV[k]
            flat = flat_of(u)
            for m, i in enumerate(X_UP):
                value = one_way(rho * WEIGHTS[i], flat, along_of(i, u), sign)
                if abs(KEEP[k]) > 1e-9:
                    value = value + KEEP[k] * XB[n, 3 + m]
                post[k, i if n == 0 else OPPOSITE[i], 1 + x, inner] = value

    def collide_corner(n):
        x = -1 if n == 0 else X
        sign = 1.0 if n == 0 else -1.0
        us = velocities(common_of(x, 1), x, 1)
        cx = 1 if n == 0 else -1
        up, down = INDEX[(cx, 1, 0)], INDEX[(cx, -1, 0)]
        for k in range(2):
            u = us[k]
            rho = psi[k, 2 + x, low] * INV[k]
            value = one_way(rho * WEIGHTS[up], flat_of(u), sign * u[0] + row_sign * u[1], 1.0)
            if abs(KEEP[k]) > 1e-9:
                value = value + KEEP[k] * XWP[n]
            post[k, up, 1 + x, low] = value
            post[k, down, 1 + x, high] = value

    def x_up(v):
        return roll(v, -2)

    def x_down(v):
        return roll(v, 2)

    def y_up(v, n=0):
        r = roll_rows(v, -1)
        return jnp.where(row == T - 1, roll(r, n - stride_t), roll(r, n))

    def y_down(v, n=0):
        r = roll_rows(v, 1)
        return jnp.where(row == 0, roll(r, n + stride_t), roll(r, n))

    def collide_z(s0, s1, s2, t1, t2, olds):
        other1, other2 = roll(t1, HALF), roll(t2, HALF)
        common = [
            jnp.where(lower, t1, other1),
            jnp.where(lower, t2, other2),
            jnp.where(lower, other1, t1),
        ]
        p0, p1, p2 = jnp.abs(s0), jnp.abs(s1), jnp.abs(s2)
        xs = [x_up(v) + x_down(v) for v in (p0, p1, p2)]
        ys = [y_up(v) + y_down(v) for v in (p0, p1, p2)]
        g = 2.0 * p1 + (p0 + p2)
        a = g + ys[1]
        b = g + xs[1]
        c0 = 2.0 * p0 + (xs[0] + ys[0])
        c2 = 2.0 * p2 + (xs[2] + ys[2])
        sign = jnp.where(even, 1.0, -1.0)
        grads = [
            roll(a, HALF - 2) - roll(a, HALF + 2),
            y_up(b, HALF) - y_down(b, HALF),
            roll((c0 - c2) * sign, HALF),
        ]
        factor = jnp.where(lower, COUPLING * RELAX[0] / 36.0, COUPLING * RELAX[1] / 36.0)
        u = [common[d] - factor * grads[d] for d in range(3)]
        rho = p1 * jnp.where(lower, INV[0], INV[1])
        keep = jnp.where(lower, KEEP[0], KEEP[1])
        flat = flat_of(u)
        beyond = (slot < 2) | (slot >= X + 2)
        for g, i in enumerate(Z_UP):
            c = VELOCITIES[i]
            old = jnp.where(beyond, t2, olds[g]) if c[0] else olds[g]
            value = one_way(rho * WEIGHTS[i], flat, along_of(i, u), sign)
            value = value + keep * jnp.where(lower, 0.0, old)
            if c[1]:
                a, b = (y_down, y_up) if c[1] > 0 else (y_up, y_down)
                value = jnp.where(even, b(value, -1), a(value, 1))
            else:
                value = jnp.where(even, roll(value, -1 - 2 * c[0]), roll(value, 1 + 2 * c[0]))
            for k in range(2):
                for x in range(X):
                    for t in range(1, YT + 1):
                        zpost[k, g, x, T * (t - 1):T * t] = spread(value, k, t, x + 2)

    def stream(x):
        fluid = solid[x] == 0
        for k in range(2):
            for i in range(19):
                c = VELOCITIES[i]
                rows = slice(T - c[1], T - c[1] + Y)
                read = post[k, i, 1 + x - c[0], rows]
                if i:
                    if c[2]:
                        at = first_y if c[2] > 0 else last_y
                        read = jnp.where(at, zpost[k, Z_PAIR[i], x], roll(read, c[2]))
                    p = 2 + x - c[0]
                    signs = SD if c[2] > 0 else (SU if c[2] else S)
                    bounced = post[k, OPPOSITE[i], 1 + x, inner]
                    read = jnp.where(signs[0, p, rows] > 0.0, read, bounced)
                out[k, i, x] = jnp.where(fluid, read, pop[k, i, x])

    for x in range(X):
        prepare(2 + x)

    await_("xS", S.at[:, 0:4, inner])
    await_("xE", XE)
    for n in range(2):
        planes = (0, 1) if n == 0 else (X + 2, X + 3)
        ups, downs = 1 + 4 * y_slot[1], 1 + 4 * y_slot[-1]
        for m, p in enumerate(planes):
            value = XE[n, ups + 1 + m]
            if NY > 1:
                value = jnp.where(row % 4 < 2, value, XE[n, downs + 1 + m])
            other = roll_rows(value, 4)
            for k, w in ((0, value), (1, other)):
                S[k, p, low] = w
                S[k, p, high] = w
        value = XE[n, ups + 3]
        if NY > 1:
            value = jnp.where(row % 2 == 0, value, XE[n, downs + 3])
        plane = 0 if n == 0 else X + 1
        for d in range(3):
            V[d, plane, Y:Y + T] = roll_rows(value, -2 * d)
        XWP[n] = roll_rows(value, -6)
    outer = [0, 1, X + 2, X + 3]
    for p in outer:
        prepare(p)

    def with_rows(tile, w_low, w_high):
        return jnp.where(own_t, tile, jnp.where(tile_t == 0, w_low, w_high))

    def by_row(low_part, high_part):
        return low_part if NY == 1 else ends(low_part, high_part)

    top = stride_t * (YT + 1)

    def assemble(middle, left, right, shift_left, shift_right):
        return jnp.where(
            slot < 2,
            roll(left, 2 * shift_left),
            jnp.where(slot >= X + 2, roll(right, 2 * shift_right), middle),
        )

    await_("yW", YW)
    y_rows = by_row(YW[y_slot[1]], YW[y_slot[-1]])
    own = with_rows(ZS[0], y_rows, roll(y_rows, top))
    beside = []
    for n in range(2):
        w = by_row(XE[n, 1 + 4 * y_slot[1]], XE[n, 1 + 4 * y_slot[-1]])
        beside.append(with_rows(XE[n, 0], w, roll(w, top)))
    s0 = swap(assemble(roll(own, 4), beside[0], beside[1], 2 - X, X + 2))

    await_("zF", ZF)
    faces = [jnp.where(even, ZF[0, p], ZF[1, p]) for p in range(4 + NY)]
    z_rows = by_row(faces[4 + y_slot[1]], faces[4 + y_slot[-1]])
    full = [
        with_rows(faces[p], roll(z_rows, -stride_t * p), roll(z_rows, top - stride_t * p))
        for p in range(4)
    ]
    center = [[roll(full[p], 2 * (2 - b * X)) for b in range(2)] for p in range(2)]
    olds = []
    for p, h, b in POP_PLACE:
        olds.append(roll(full[p], 2 * (2 - b * X) + HALF * (1 - h)))
    near_signs = swap(center[0][0])
    for x in range(X):
        complete(2 + x, near_signs)
    for x in range(X):
        sums(2 + x)
    for x in range(1, X - 1):
        collide_own(x)
        collide_rows(x)

    await_("zD", ZD)
    diags = []
    for n in range(2):
        merged = [jnp.where(even, ZD[0, n, q], ZD[1, n, q]) for q in range(1 + NY)]
        w = by_row(merged[1 + y_slot[1]], merged[1 + y_slot[-1]])
        diags.append(with_rows(merged[0], w, roll(w, top)))
    s1, s2 = [
        assemble(center[0][b], *diags, -(b * X + X - 2), X + 2 - b * X) for b in range(2)
    ]
    t1, t2 = [assemble(center[1][b], *diags, 1 - b * X, 3 - b * X) for b in range(2)]
    signs = swap(s1)
    for p in outer:
        complete(p, signs)
    for p in outer:
        sums(p)
    for x in (0, X - 1):
        collide_own(x)
        collide_rows(x)
    collide_z(s0, s1, s2, t1, t2, olds)
    for n in range(2):
        collide_corner(n)
    for x in range(1, X - 1):
        stream(x)
    await_("xB", XB)
    for n in range(2):
        collide_plane(n)
    for x in (0, X - 1):
        stream(x)
    assert sent[0] == tally.shape[0]
    pltpu.make_async_copy(tally, tally, send_sem).wait()


def body(populations, solid):
    X, Y, Z = solid.shape
    f32 = jnp.float32
    dma = pltpu.SemaphoreType.DMA
    R = Y + 2 * T
    XX = X + 4
    NY = 1 if lax.axis_size("gy") == 2 else 2
    YT = Y // T
    tiles = 20 * X + 24 * YT + 14 + 15 * NY

    def vmem(*shape):
        return pltpu.VMEM(shape, f32)

    return pl.pallas_call(
        step_kernel,
        out_shape=pltpu.VMEM(populations.shape, f32),
        in_specs=[pl.BlockSpec(memory_space=pl.ANY)] * 2,
        out_specs=pl.BlockSpec(memory_space=pltpu.VMEM),
        scratch_shapes=[
            vmem(*populations.shape),
            pltpu.VMEM(solid.shape, jnp.int32),
            vmem(2, XX, R, Z),
            vmem(2, XX, R, Z),
            vmem(2, XX, R, Z),
            vmem(2, XX, R, Z),
            vmem(2, XX, R, Z),
            vmem(2, XX, R, Z),
            vmem(2, XX, Y + T, Z),
            vmem(3, X + 2, Y + T, Z),
            vmem(2, 19, X + 2, R, Z),
            vmem(2, 5, X, Y, Z),
            vmem(2, 10, X, T, Z),
            vmem(5, X, T, Z),
            vmem(2, 8, Y, Z),
            vmem(2, T, Z),
            vmem(2, 4, T, LANES),
            vmem(2, 1 + 4 * NY, T, LANES),
            vmem(5, T, LANES),
            vmem(NY, T, LANES),
            vmem(2, 4 + NY, T, LANES),
            vmem(2, 2, 1 + NY, T, LANES),
            vmem(tiles, T, LANES),
            dma((3,)),
            dma,
            dma((7,)),
            pltpu.SemaphoreType.REGULAR,
            pltpu.SemaphoreType.REGULAR,
        ],
        compiler_params=pltpu.CompilerParams(collective_id=0, has_side_effects=True),
    )(populations, solid)


def solution(mesh):
    in_specs = (P(None, None, "gx", "gy", "gz"), P("gx", "gy", "gz"))
    out_specs = P(None, None, "gx", "gy", "gz")
    return jax.shard_map(body, mesh=mesh, in_specs=in_specs, out_specs=out_specs, check_vma=False)
```

```python
import jax
import jax.numpy as jnp
from jax import lax
from jax.experimental import pallas as pl
from jax.experimental.pallas import tpu as pltpu
from jax.sharding import PartitionSpec as P

VELOCITIES = [
    (0, 0, 0),
    (1, 0, 0),
    (-1, 0, 0),
    (0, 1, 0),
    (0, -1, 0),
    (0, 0, 1),
    (0, 0, -1),
    (1, 1, 0),
    (-1, -1, 0),
    (1, -1, 0),
    (-1, 1, 0),
    (1, 0, 1),
    (-1, 0, -1),
    (1, 0, -1),
    (-1, 0, 1),
    (0, 1, 1),
    (0, -1, -1),
    (0, 1, -1),
    (0, -1, 1),
]
WEIGHTS = [1.0 / 3.0] + [1.0 / 18.0] * 6 + [1.0 / 36.0] * 12
OPPOSITE = [0, 2, 1, 4, 3, 6, 5, 8, 7, 10, 9, 12, 11, 14, 13, 16, 15, 18, 17]
INDEX = {v: i for i, v in enumerate(VELOCITIES)}
COUPLING = 0.9
RELAX = (1.0, 0.8)
WALL = (0.3, 1.5)
INV = [1.0 / t for t in RELAX]
KEEP = [1.0 - v for v in INV]
AXES = ("gx", "gy", "gz")
MESH = pl.DeviceIdType.MESH

X_UP = [i for i in range(19) if VELOCITIES[i][0] == 1]
Y_UP = [i for i in range(19) if VELOCITIES[i][1] == 1]
Z_UP = [(0, 0, 1), (1, 0, 1), (-1, 0, 1), (0, 1, 1), (0, -1, 1)]
Z_UP = [INDEX[v] for v in Z_UP]
Z_PAIR = {}
for _g, _i in enumerate(Z_UP):
    Z_PAIR[_i] = _g
    Z_PAIR[OPPOSITE[_i]] = _g
Z_FROM = [(dx, dz) for dz in (-1, 1) for dx in (0, -1, 1)]
T = 8
LANES = 128
HALF = LANES // 2


def along_of(i, u):
    total = None
    for d in range(3):
        c = VELOCITIES[i][d]
        if c:
            term = u[d] if c > 0 else -u[d]
            total = term if total is None else total + term
    return total


def step_kernel(pop_hbm, solid_hbm, out, pop, solid, S, SU, SD, psi, H, O, A, V, post, zpost,
                YR, WP, XB, XWP, XSND, XE, ZS, YW, ZF, ZD, tally, load_sem, send_sem, recv_sem,
                near_sem, far_sem):
    X, Y, Z = solid.shape
    YT = Y // T
    inner = slice(T, T + Y)
    low, high = slice(0, T), slice(Y + T, Y + 2 * T)
    XX = X + 4
    stride_t = HALF // (YT + 2)
    assert Z == LANES and YT == 2 and X >= 3
    assert stride_t >= 2 * XX and 2 * X <= XX

    me = [lax.axis_index(a) for a in AXES]
    count = [lax.axis_size(a) for a in AXES]
    assert count[1] % 2 == 0
    y_sides = (1,) if count[1] == 2 else (1, -1)
    NY = len(y_sides)
    y_slot = {1: 0, -1: NY - 1}

    loads = [pltpu.make_async_copy(solid_hbm, solid, load_sem.at[0])]
    cuts = [0, X // 2, X]
    for n in range(2):
        part = slice(cuts[n], cuts[n + 1])
        loads.append(
            pltpu.make_async_copy(pop_hbm.at[:, :, part], pop.at[:, :, part], load_sem.at[1 + n])
        )
    for copy in loads:
        copy.start()

    parity = lax.rem(me[1], 2)
    is_near, is_far = parity == 0, parity == 1

    def device(offset):
        return tuple(lax.rem(me[d] + offset[d] + count[d], count[d]) for d in range(3))

    barrier = pltpu.get_barrier_semaphore()
    partner = (me[0], me[1] + 1 - 2 * parity, me[2])
    pairs = [me[1] - parity]
    if count[1] > 2:
        pairs.append(lax.rem(me[1] + 3 * parity - 2 + count[1], count[1]))

    def arrive(place):
        pl.semaphore_signal(barrier, inc=1, device_id=place, device_id_type=MESH)

    for dx in (1, -1, 0):
        for dz in (1, -1):
            place = device((dx, 0, dz))
            for base in pairs:
                arrive((place[0], base + 1, place[2]))
    for dx in (1, -1):
        place = device((dx, 0, 0))
        for base in pairs:
            arrive((place[0], base, place[2]))
    for base in pairs[1:]:
        arrive((me[0], base, me[2]))
    arrive(partner)
    near_count, far_count = 4 + 1, 12 + 1
    if count[1] > 2:
        near_count, far_count = near_count + 6, far_count + 12

    lane = lax.broadcasted_iota(jnp.int32, (T, LANES), 1)
    row = lax.broadcasted_iota(jnp.int32, (T, LANES), 0)
    pair = lane // 2
    even = lane % 2 == 0
    half = lane // HALF
    lower = half == 0
    slot = (lane % stride_t) // 2
    tile_t = (lane % HALF) // stride_t
    own_t = (tile_t > 0) & (tile_t <= YT)
    first, last = lane == 0, lane == Z - 1
    lane_y = lax.broadcasted_iota(jnp.int32, (Y, LANES), 1)
    first_y, last_y = lane_y == 0, lane_y == Z - 1
    upper = row < T // 2

    def roll(v, n):
        n = n % LANES
        return pltpu.roll(v, n, 1) if n else v

    def roll_rows(v, n):
        n = n % T
        return pltpu.roll(v, n, 0) if n else v

    def swap(v):
        return jnp.where(even, roll(v, -1), roll(v, 1))

    GROUPS = {"y": 0, "yW": 1, "xS": 2, "xE": 3, "zF": 4, "zD": 5, "xB": 6}
    sent = [0]

    def send(group, src, dst, offset, tiles):
        pltpu.make_async_remote_copy(
            src_ref=src,
            dst_ref=dst,
            send_sem=send_sem,
            recv_sem=recv_sem.at[GROUPS[group]],
            device_id=device(offset),
            device_id_type=MESH,
        ).start()
        sent[0] += tiles

    def await_(group, ref):
        pltpu.make_async_copy(ref, ref, recv_sem.at[GROUPS[group]]).wait()

    def moments(x):
        fluid = solid[x] == 0
        total, mom = [], []
        for k in range(2):
            f = [pop[k, i, x] for i in range(19)]
            rho = f[0]
            m = [None, None, None]
            for i in range(1, 19, 2):
                rho = rho + (f[i] + f[i + 1])
                diff = f[i] - f[i + 1]
                for d in range(3):
                    c = VELOCITIES[i][d]
                    if c:
                        m[d] = (
                            (diff if c > 0 else -diff)
                            if m[d] is None
                            else (m[d] + diff if c > 0 else m[d] - diff)
                        )
            total.append(rho)
            S[k, 2 + x, inner] = jnp.where(fluid, rho, -WALL[k])
            mom.append([v * INV[k] if INV[k] != 1.0 else v for v in m])
        scale = 1.0 / (total[0] * INV[0] + total[1] * INV[1])
        for d in range(3):
            V[d, 1 + x, 0:Y] = (mom[0][d] + mom[1][d]) * scale

    blank = jnp.zeros((T, LANES), jnp.float32)
    packs = [blank, blank, blank, blank]
    POP_PLACE = [(2, 0, 0), (2, 0, 1), (2, 1, 0), (2, 1, 1), (3, 1, 0)]
    V_PLACE = [(1, 0, 0), (1, 0, 1), (1, 1, 0)]

    def put(p, h, b, t, x, value, inside=False):
        j = (h * HALF + t * stride_t + (b * X + x) * 2) // 2
        if inside:
            value = jnp.where(even, roll(value, 2 * j + 2), roll(value, 2 * j))
        else:
            value = roll(value, 2 * j + 1)
        packs[p] = jnp.where(pair == j, value, packs[p])

    def z_ends(i, x, t):
        rows = slice(T * (t - 1), T * t)
        return jnp.where(lane < HALF, pop[1, OPPOSITE[i], x, rows], pop[1, i, x, rows])

    def pack_signs(x):
        for t in range(1, YT + 1):
            for k in range(2):
                value = S[k, 2 + x, T * t:T * t + T]
                put(0, k, 0, t, x, value)
                put(0, k, 1, t, x, value, inside=True)
            for d in range(3):
                put(*V_PLACE[d], t, x, V[d, 1 + x, T * (t - 1):T * t])
            if x in (0, X - 1):
                out_i, in_i = (Z_UP[1], Z_UP[2]) if x else (Z_UP[2], Z_UP[1])
                rows = slice(T * (t - 1), T * t)
                value = jnp.where(lane < HALF, pop[1, OPPOSITE[in_i], x, rows], pop[1, out_i, x, rows])
                put(1, 1, 1, t, x, value)

    loads[0].wait()
    for n in range(2):
        loads[1 + n].wait()
        for x in range(cuts[n], cuts[n + 1]):
            moments(x)
        for x in range(cuts[n], cuts[n + 1]):
            pack_signs(x)

    place = slot % X

    def edges(v, q):
        return jnp.where(upper, roll(v, (q - 1) * stride_t), roll(v, (q - YT) * stride_t))

    for n in range(2):
        if n == 0:
            tile = jnp.where(place >= X - 2, packs[0], roll(packs[1], -2 * (X - 1)))
        else:
            tile = jnp.where(place < 2, packs[0], roll(packs[1], 2 * (X - 1)))
        XSND[n, 0] = jnp.where(tile_t == 0, edges(tile, 0), tile)

    def ends(a, b):
        return jnp.where(upper, a, b)

    t_first, t_last = slice(0, T), slice(Y - T, Y)
    s_first, s_last = slice(T, 2 * T), slice(Y, Y + T)
    keep_rows = (row < 2) | (row >= T - 2)
    for n, side in enumerate((1, -1)):
        planes = (X, X + 1) if side > 0 else (2, 3)
        for m, p in enumerate(planes):
            both = [ends(S[k, p, s_first], S[k, p, s_last]) for k in range(2)]
            XSND[n, 1 + m] = jnp.where(keep_rows, both[0], roll_rows(both[1], 4))
        x = X - 1 if side > 0 else 0
        up, down = INDEX[(side, 1, 0)], INDEX[(side, -1, 0)]
        fields = [ends(V[d, 1 + x, t_first], V[d, 1 + x, t_last]) for d in range(3)]
        fields.append(ends(pop[1, down, x, t_first], pop[1, up, x, t_last]))
        packed = fields[0]
        for f in range(1, 4):
            at = (row == 2 * f - 1) | (row == 2 * f)
            packed = jnp.where(at, roll_rows(fields[f], 2 * f), packed)
        XSND[n, 3] = packed

    top_z = me[2] == count[2] - 1
    not_top = jnp.logical_not(top_z)

    def tell(sem):
        pl.semaphore_signal(sem, inc=1, device_id=partner, device_id_type=MESH)

    def learn_far():
        pl.semaphore_wait(barrier, far_count)
        tell(far_sem)

    first_up = lax.rem(me[0], 4) != 1
    sides = [jnp.where(first_up, 1, -1), jnp.where(first_up, -1, 1)]

    def send_x_signs(side):
        up = side > 0
        src = jnp.where(up, X, 2)
        dst = jnp.where(up, 0, X + 2)
        send("xS", S.at[:, pl.ds(src, 2), inner], S.at[:, pl.ds(dst, 2), inner],
             (side, 0, 0), 4 * YT)

    def send_x_bulk(side):
        up = side > 0
        n = jnp.where(up, 0, 1)
        to = (side, 0, 0)
        send("xB", V.at[:, jnp.where(up, X, 1), 0:Y], XB.at[n, 0:3], to, 3 * YT)
        for m, i in enumerate(X_UP):
            send("xB", pop.at[1, jnp.where(up, i, OPPOSITE[i]), jnp.where(up, X - 1, 0)],
                 XB.at[n, 3 + m], to, YT)

    def send_diagonal():
        for n, side in enumerate((1, -1)):
            for m, dz in enumerate((1, -1)):
                send("zD", XSND.at[n, 0], ZD.at[m, n, 0], (side, 0, dz), 1)
                for sy in y_sides:
                    send("zD", XSND.at[n, 0], ZD.at[m, n, 1 + y_slot[-sy]], (side, sy, dz), 1)

    ZS[5] = packs[0]

    def pack_faces():
        for x in range(X):
            for t in range(1, YT + 1):
                for g, i in enumerate(Z_UP):
                    put(*POP_PLACE[g], t, x, z_ends(i, x, t))
        merged = edges(packs[0], 0)
        for p in range(1, 4):
            merged = jnp.where(tile_t == p, edges(packs[p], p), merged)
        for m in range(2):
            one, two = packs[2 * m], packs[2 * m + 1]
            ZS[m] = jnp.where(even, one, roll(two, 1))
            ZS[2 + m] = jnp.where(even, roll(two, -1), one)
        ZS[4] = merged
        packs[2] = packs[3] = blank

    def send_faces():
        for m, dz in enumerate((1, -1)):
            send("zF", ZS.at[2 * m:2 * m + 2], ZF.at[m, 0:2], (0, 0, dz), 2)
            for sy in y_sides:
                send("zF", ZS.at[4], ZF.at[m, 2 + y_slot[-sy]], (0, sy, dz), 1)

    @pl.when(is_far & top_z)
    def _():
        learn_far()

    @pl.when(is_near & top_z)
    def _():
        pl.semaphore_wait(far_sem, 1)

    counted = sent[0]

    @pl.when(top_z)
    def _():
        send_diagonal()
        pack_faces()
        send_faces()

    sent[0] = counted

    @pl.when(is_near)
    def _():
        pl.semaphore_wait(barrier, near_count)
        tell(near_sem)

    @pl.when(is_far)
    def _():
        pl.semaphore_wait(near_sem, 1)

    send_x_signs(sides[0])
    send_x_signs(sides[1])
    for n, side in enumerate((1, -1)):
        send("xE", XSND.at[n, 0:1], XE.at[n, 0:1], (side, 0, 0), 1)
        for sy in y_sides:
            m = 1 + 4 * y_slot[-sy]
            send("xE", XSND.at[n], XE.at[n, m:m + 4], (side, sy, 0), 4)
    for n, side in enumerate((1, -1)):
        tile = slice(Y - T, Y) if side > 0 else slice(0, T)
        wide = slice(Y, Y + T) if side > 0 else slice(T, 2 * T)
        to = (0, side, 0)
        send("y", S.at[:, 2:2 + X, wide], YR.at[n, 0:2], to, 2 * X)
        send("y", V.at[:, 1:1 + X, tile], YR.at[n, 2:5], to, 3 * X)
        for m, i in enumerate(Y_UP):
            i = i if side > 0 else OPPOSITE[i]
            send("y", pop.at[1, i, :, tile], YR.at[n, 5 + m], to, X)
    send_x_bulk(sides[0])
    send_x_bulk(sides[1])

    @pl.when(not_top)
    def _():
        pack_faces()

    for sy in y_sides:
        send("yW", ZS.at[4], YW.at[y_slot[-sy]], (0, sy, 0), 1)

    @pl.when(is_far & not_top)
    def _():
        learn_far()

    @pl.when(is_near & not_top)
    def _():
        pl.semaphore_wait(far_sem, 1)

    @pl.when(not_top)
    def _():
        send_diagonal()
        send_faces()

    await_("y", YR)
    for x in range(X):
        for k in range(2):
            value = ends(YR[1, k, x], YR[0, k, x])
            S[k, 2 + x, low] = value
            S[k, 2 + x, high] = value
        for d in range(3):
            V[d, 1 + x, Y:Y + T] = ends(YR[1, 2 + d, x], YR[0, 2 + d, x])
        for m in range(5):
            WP[m, x] = ends(YR[1, 5 + m, x], YR[0, 5 + m, x])

    def window(w, dy):
        if w == 0:
            return slice(T + dy, T + dy + Y)
        return slice(Y + T - 1, Y + 2 * T - 1) if dy < 0 else slice(dy, T + dy)

    def rows_of(w):
        return slice(0, Y) if w == 0 else slice(Y, Y + T)

    def prepare(p):
        for k in range(2):
            for t in range(YT + 1):
                rows = slice(T * t, T * t + T)
                value = S[k, p, rows]
                SU[k, p, rows] = roll(value, -1)
                SD[k, p, rows] = roll(value, 1)

    def spread(tile, k, t, xx):
        return roll(tile, LANES - 1 - (k * HALF + t * stride_t + 2 * xx))

    def complete(p, signs, at):
        for k in range(2):
            for t in range(YT + 1):
                rows = slice(T * t, T * t + T)
                edge = spread(signs, k, t, at)
                above = jnp.where(last, edge, SU[k, p, rows])
                below = jnp.where(first, edge, SD[k, p, rows])
                size = jnp.abs(S[k, p, rows])
                a_above, a_below = jnp.abs(above), jnp.abs(below)
                for r in (rows,) if t else (low, high):
                    psi[k, p, r] = size
                    H[k, p, r] = 2.0 * size + (a_above + a_below)
                    O[k, p, r] = a_above - a_below
                    if k == 0:
                        SU[k, p, r] = above
                        SD[k, p, r] = below

    def sums(p):
        for k in range(2):
            for w in range(2):
                A[k, p, rows_of(w)] = (
                    H[k, p, window(w, 0)] + (psi[k, p, window(w, 1)] + psi[k, p, window(w, -1)])
                ) * (1.0 / 36.0)

    def gradient(k, p, w):
        gx = A[k, p + 1, rows_of(w)] - A[k, p - 1, rows_of(w)]
        sides_y = []
        for dy in (1, -1):
            r = window(w, dy)
            sides_y.append(H[k, p, r] + (psi[k, p + 1, r] + psi[k, p - 1, r]))
        gy = (sides_y[0] - sides_y[1]) * (1.0 / 36.0)
        r = window(w, 0)
        gz = 2.0 * O[k, p, r] + (O[k, p + 1, r] + O[k, p - 1, r])
        gz = (gz + (O[k, p, window(w, 1)] + O[k, p, window(w, -1)])) * (1.0 / 36.0)
        return gx, gy, gz

    def velocities(common, x, w):
        grads = [gradient(k, x + 2, w) for k in range(2)]
        return [
            [common[d] - (COUPLING * RELAX[k]) * grads[1 - k][d] for d in range(3)]
            for k in range(2)
        ]

    def common_of(x, w):
        return [V[d, 1 + x, rows_of(w)] for d in range(3)]

    def flat_of(u):
        return 1.0 - 1.5 * (u[0] * u[0] + u[1] * u[1] + u[2] * u[2])

    def one_way(w, flat, along, sign):
        even_part = w * (flat + 4.5 * (along * along))
        return even_part + w * ((3.0 * sign) * along)

    def collide_own(x):
        us = velocities(common_of(x, 0), x, 0)
        for k in range(2):
            u = us[k]
            rho = psi[k, 2 + x, inner] * INV[k]
            flat = flat_of(u)
            scaled = {w: rho * w for w in sorted(set(WEIGHTS))}
            values = {0: scaled[WEIGHTS[0]] * flat}
            for i in range(1, 19, 2):
                along = along_of(i, u)
                w = scaled[WEIGHTS[i]]
                even_part = w * (flat + 4.5 * (along * along))
                odd_part = w * (3.0 * along)
                values[i] = even_part + odd_part
                values[i + 1] = even_part - odd_part
            for i in range(19):
                if abs(KEEP[k]) > 1e-9:
                    values[i] = values[i] + KEEP[k] * pop[k, i, x]
                post[k, i, 1 + x, inner] = values[i]

    row_sign = jnp.where(upper, -1.0, 1.0)

    def collide_rows(x):
        us = velocities(common_of(x, 1), x, 1)
        for k in range(2):
            u = us[k]
            rho = psi[k, 2 + x, low] * INV[k]
            flat = flat_of(u)
            for m, i in enumerate(Y_UP):
                w = rho * WEIGHTS[i]
                value = one_way(w, flat, along_of(i, u), row_sign)
                if abs(KEEP[k]) > 1e-9:
                    value = value + KEEP[k] * WP[m, x]
                post[k, i, 1 + x, low] = value
                post[k, OPPOSITE[i], 1 + x, high] = value

    def collide_plane(n):
        x = -1 if n == 0 else X
        sign = 1.0 if n == 0 else -1.0
        us = velocities([XB[n, d] for d in range(3)], x, 0)
        for k in range(2):
            u = us[k]
            rho = psi[k, 2 + x, inner] * INV[k]
            flat = flat_of(u)
            for m, i in enumerate(X_UP):
                value = one_way(rho * WEIGHTS[i], flat, along_of(i, u), sign)
                if abs(KEEP[k]) > 1e-9:
                    value = value + KEEP[k] * XB[n, 3 + m]
                post[k, i if n == 0 else OPPOSITE[i], 1 + x, inner] = value

    def collide_corner(n):
        x = -1 if n == 0 else X
        sign = 1.0 if n == 0 else -1.0
        us = velocities(common_of(x, 1), x, 1)
        cx = 1 if n == 0 else -1
        up, down = INDEX[(cx, 1, 0)], INDEX[(cx, -1, 0)]
        for k in range(2):
            u = us[k]
            rho = psi[k, 2 + x, low] * INV[k]
            value = one_way(rho * WEIGHTS[up], flat_of(u), sign * u[0] + row_sign * u[1], 1.0)
            if abs(KEEP[k]) > 1e-9:
                value = value + KEEP[k] * XWP[n]
            post[k, up, 1 + x, low] = value
            post[k, down, 1 + x, high] = value

    def x_up(v):
        return roll(v, -2)

    def x_down(v):
        return roll(v, 2)

    def y_up(v, n=0):
        r = roll_rows(v, -1)
        return jnp.where(row == T - 1, roll(r, n - stride_t), roll(r, n))

    def y_down(v, n=0):
        r = roll_rows(v, 1)
        return jnp.where(row == 0, roll(r, n + stride_t), roll(r, n))

    def collide_z(s0, s1, s2, t1, t2, olds):
        other1, other2 = roll(t1, HALF), roll(t2, HALF)
        common = [
            jnp.where(lower, t1, other1),
            jnp.where(lower, t2, other2),
            jnp.where(lower, other1, t1),
        ]
        p0, p1, p2 = jnp.abs(s0), jnp.abs(s1), jnp.abs(s2)
        xs = [x_up(v) + x_down(v) for v in (p0, p1, p2)]
        ys = [y_up(v) + y_down(v) for v in (p0, p1, p2)]
        g = 2.0 * p1 + (p0 + p2)
        a = g + ys[1]
        b = g + xs[1]
        c0 = 2.0 * p0 + (xs[0] + ys[0])
        c2 = 2.0 * p2 + (xs[2] + ys[2])
        sign = jnp.where(even, 1.0, -1.0)
        grads = [
            roll(a, HALF - 2) - roll(a, HALF + 2),
            y_up(b, HALF) - y_down(b, HALF),
            roll((c0 - c2) * sign, HALF),
        ]
        factor = jnp.where(lower, COUPLING * RELAX[0] / 36.0, COUPLING * RELAX[1] / 36.0)
        u = [common[d] - factor * grads[d] for d in range(3)]
        rho = p1 * jnp.where(lower, INV[0], INV[1])
        keep = jnp.where(lower, KEEP[0], KEEP[1])
        flat = flat_of(u)
        beyond = (slot < 2) | (slot >= X + 2)
        for g, i in enumerate(Z_UP):
            c = VELOCITIES[i]
            old = jnp.where(beyond, t2, olds[g]) if c[0] else olds[g]
            value = one_way(rho * WEIGHTS[i], flat, along_of(i, u), sign)
            value = value + keep * jnp.where(lower, 0.0, old)
            if c[1]:
                a, b = (y_down, y_up) if c[1] > 0 else (y_up, y_down)
                value = jnp.where(even, b(value, -1), a(value, 1))
            else:
                value = jnp.where(even, roll(value, -1 - 2 * c[0]), roll(value, 1 + 2 * c[0]))
            for k in range(2):
                for x in range(X):
                    for t in range(1, YT + 1):
                        zpost[k, g, x, T * (t - 1):T * t] = spread(value, k, t, x + 2)

    def stream(x):
        fluid = solid[x] == 0
        for k in range(2):
            for i in range(19):
                c = VELOCITIES[i]
                rows = slice(T - c[1], T - c[1] + Y)
                read = post[k, i, 1 + x - c[0], rows]
                if i:
                    if c[2]:
                        at = first_y if c[2] > 0 else last_y
                        read = jnp.where(at, zpost[k, Z_PAIR[i], x], roll(read, c[2]))
                    p = 2 + x - c[0]
                    signs = SD if c[2] > 0 else (SU if c[2] else S)
                    bounced = post[k, OPPOSITE[i], 1 + x, inner]
                    read = jnp.where(signs[0, p, rows] > 0.0, read, bounced)
                out[k, i, x] = jnp.where(fluid, read, pop[k, i, x])

    for x in range(X):
        prepare(2 + x)

    await_("xS", S.at[:, 0:4, inner])
    await_("xE", XE)
    for n in range(2):
        planes = (0, 1) if n == 0 else (X + 2, X + 3)
        ups, downs = 1 + 4 * y_slot[1], 1 + 4 * y_slot[-1]
        for m, p in enumerate(planes):
            value = XE[n, ups + 1 + m]
            if NY > 1:
                value = jnp.where(row % 4 < 2, value, XE[n, downs + 1 + m])
            other = roll_rows(value, 4)
            for k, w in ((0, value), (1, other)):
                S[k, p, low] = w
                S[k, p, high] = w
        value = XE[n, ups + 3]
        if NY > 1:
            value = jnp.where(row % 2 == 0, value, XE[n, downs + 3])
        plane = 0 if n == 0 else X + 1
        for d in range(3):
            V[d, plane, Y:Y + T] = roll_rows(value, -2 * d)
        XWP[n] = roll_rows(value, -6)
    outer = [0, 1, X + 2, X + 3]
    for p in outer:
        prepare(p)

    def with_rows(tile, w_low, w_high):
        return jnp.where(own_t, tile, jnp.where(tile_t == 0, w_low, w_high))

    def by_row(low_part, high_part):
        return low_part if NY == 1 else ends(low_part, high_part)

    top = stride_t * (YT + 1)

    def assemble(middle, left, right, shift_left, shift_right):
        return jnp.where(
            slot < 2,
            roll(left, 2 * shift_left),
            jnp.where(slot >= X + 2, roll(right, 2 * shift_right), middle),
        )

    await_("yW", YW)
    y_rows = by_row(YW[y_slot[1]], YW[y_slot[-1]])
    own = with_rows(ZS[5], y_rows, roll(y_rows, top))
    beside = []
    for n in range(2):
        w = by_row(XE[n, 1 + 4 * y_slot[1]], XE[n, 1 + 4 * y_slot[-1]])
        beside.append(with_rows(XE[n, 0], w, roll(w, top)))
    s0 = swap(assemble(roll(own, 4), beside[0], beside[1], 2 - X, X + 2))

    await_("zF", ZF)
    one, two = ZF[0, 0], ZF[1, 0]
    rows_z = [jnp.where(even, ZF[0, 2 + m], ZF[1, 2 + m]) for m in range(NY)]
    z_rows = by_row(rows_z[y_slot[1]], rows_z[y_slot[-1]])
    near_signs = jnp.where(even, roll(two, -1), roll(one, 1))
    near_signs = jnp.where(tile_t == 0, swap(z_rows), near_signs)
    faces = []
    for m in range(2):
        one, two = ZF[0, m], ZF[1, m]
        faces.append(jnp.where(even, one, two))
        faces.append(jnp.where(even, roll(one, -1), roll(two, 1)))
    full = [
        with_rows(faces[p], roll(z_rows, -stride_t * p), roll(z_rows, top - stride_t * p))
        for p in range(4)
    ]
    center = [[roll(full[p], 2 * (2 - b * X)) for b in range(2)] for p in range(2)]
    olds = []
    for p, h, b in POP_PLACE:
        olds.append(roll(full[p], 2 * (2 - b * X) + HALF * (1 - h)))
    for x in range(X):
        complete(2 + x, near_signs, x)
    for x in range(X):
        sums(2 + x)
    for x in range(1, X - 1):
        collide_own(x)
        collide_rows(x)

    await_("zD", ZD)
    diags, far_signs = [], []
    for n in range(2):
        merged = [jnp.where(even, ZD[0, n, q], ZD[1, n, q]) for q in range(1 + NY)]
        w = by_row(merged[1 + y_slot[1]], merged[1 + y_slot[-1]])
        far_signs.append(swap(jnp.where(tile_t == 0, w, merged[0])))
        diags.append(with_rows(merged[0], w, roll(w, top)))
    for m in range(2):
        complete(m, far_signs[0], X - 2 + m)
        complete(X + 2 + m, far_signs[1], m)
    s1, s2 = [
        assemble(center[0][b], *diags, -(b * X + X - 2), X + 2 - b * X) for b in range(2)
    ]
    t1, t2 = [assemble(center[1][b], *diags, 1 - b * X, 3 - b * X) for b in range(2)]
    for p in outer:
        sums(p)
    for x in (0, X - 1):
        collide_own(x)
        collide_rows(x)
    collide_z(s0, s1, s2, t1, t2, olds)
    for n in range(2):
        collide_corner(n)
    for x in range(1, X - 1):
        stream(x)
    await_("xB", XB)
    for n in range(2):
        collide_plane(n)
    for x in (0, X - 1):
        stream(x)
    assert sent[0] == tally.shape[0]
    pltpu.make_async_copy(tally, tally, send_sem).wait()


def body(populations, solid):
    X, Y, Z = solid.shape
    f32 = jnp.float32
    dma = pltpu.SemaphoreType.DMA
    R = Y + 2 * T
    XX = X + 4
    NY = 1 if lax.axis_size("gy") == 2 else 2
    YT = Y // T
    tiles = 20 * X + 24 * YT + 10 + 15 * NY

    def vmem(*shape):
        return pltpu.VMEM(shape, f32)

    return pl.pallas_call(
        step_kernel,
        out_shape=pltpu.VMEM(populations.shape, f32),
        in_specs=[pl.BlockSpec(memory_space=pl.ANY)] * 2,
        out_specs=pl.BlockSpec(memory_space=pltpu.VMEM),
        scratch_shapes=[
            vmem(*populations.shape),
            pltpu.VMEM(solid.shape, jnp.int32),
            vmem(2, XX, R, Z),
            vmem(2, XX, R, Z),
            vmem(2, XX, R, Z),
            vmem(2, XX, R, Z),
            vmem(2, XX, R, Z),
            vmem(2, XX, R, Z),
            vmem(2, XX, Y + T, Z),
            vmem(3, X + 2, Y + T, Z),
            vmem(2, 19, X + 2, R, Z),
            vmem(2, 5, X, Y, Z),
            vmem(2, 10, X, T, Z),
            vmem(5, X, T, Z),
            vmem(2, 8, Y, Z),
            vmem(2, T, Z),
            vmem(2, 4, T, LANES),
            vmem(2, 1 + 4 * NY, T, LANES),
            vmem(6, T, LANES),
            vmem(NY, T, LANES),
            vmem(2, 2 + NY, T, LANES),
            vmem(2, 2, 1 + NY, T, LANES),
            vmem(tiles, T, LANES),
            dma((3,)),
            dma,
            dma((7,)),
            pltpu.SemaphoreType.REGULAR,
            pltpu.SemaphoreType.REGULAR,
        ],
        compiler_params=pltpu.CompilerParams(collective_id=0, has_side_effects=True),
    )(populations, solid)


def solution(mesh):
    in_specs = (P(None, None, "gx", "gy", "gz"), P("gx", "gy", "gz"))
    out_specs = P(None, None, "gx", "gy", "gz")
    return jax.shard_map(body, mesh=mesh, in_specs=in_specs, out_specs=out_specs, check_vma=False)
```

```python
import jax
import jax.numpy as jnp
from jax import lax
from jax.experimental import pallas as pl
from jax.experimental.pallas import tpu as pltpu
from jax.sharding import PartitionSpec as P

VELOCITIES = [
    (0, 0, 0),
    (1, 0, 0),
    (-1, 0, 0),
    (0, 1, 0),
    (0, -1, 0),
    (0, 0, 1),
    (0, 0, -1),
    (1, 1, 0),
    (-1, -1, 0),
    (1, -1, 0),
    (-1, 1, 0),
    (1, 0, 1),
    (-1, 0, -1),
    (1, 0, -1),
    (-1, 0, 1),
    (0, 1, 1),
    (0, -1, -1),
    (0, 1, -1),
    (0, -1, 1),
]
WEIGHTS = [1.0 / 3.0] + [1.0 / 18.0] * 6 + [1.0 / 36.0] * 12
OPPOSITE = [0, 2, 1, 4, 3, 6, 5, 8, 7, 10, 9, 12, 11, 14, 13, 16, 15, 18, 17]
INDEX = {v: i for i, v in enumerate(VELOCITIES)}
COUPLING = 0.9
RELAX = (1.0, 0.8)
WALL = (0.3, 1.5)
INV = [1.0 / t for t in RELAX]
KEEP = [1.0 - v for v in INV]
AXES = ("gx", "gy", "gz")
MESH = pl.DeviceIdType.MESH

X_UP = [i for i in range(19) if VELOCITIES[i][0] == 1]
Y_UP = [i for i in range(19) if VELOCITIES[i][1] == 1]
Z_UP = [(0, 0, 1), (1, 0, 1), (-1, 0, 1), (0, 1, 1), (0, -1, 1)]
Z_UP = [INDEX[v] for v in Z_UP]
Z_PAIR = {}
for _g, _i in enumerate(Z_UP):
    Z_PAIR[_i] = _g
    Z_PAIR[OPPOSITE[_i]] = _g
Z_FROM = [(dx, dz) for dz in (-1, 1) for dx in (0, -1, 1)]
T = 8
LANES = 128
HALF = LANES // 2


def along_of(i, u):
    total = None
    for d in range(3):
        c = VELOCITIES[i][d]
        if c:
            term = u[d] if c > 0 else -u[d]
            total = term if total is None else total + term
    return total


def step_kernel(pop_hbm, solid_hbm, out, pop, solid, S, SU, SD, psi, H, O, A, V, post, zpost,
                YR, WP, XB, XWP, XSND, XE, ZS, YX, ZF, ZD, tally, load_sem, send_sem, recv_sem,
                near_sem, far_sem):
    X, Y, Z = solid.shape
    YT = Y // T
    inner = slice(T, T + Y)
    low, high = slice(0, T), slice(Y + T, Y + 2 * T)
    XX = X + 4
    stride_t = HALF // (YT + 2)
    assert Z == LANES and YT == 2 and X >= 3
    assert stride_t >= 2 * XX and 2 * X <= XX

    me = [lax.axis_index(a) for a in AXES]
    count = [lax.axis_size(a) for a in AXES]
    assert count[1] % 2 == 0
    y_sides = (1,) if count[1] == 2 else (1, -1)
    NY = len(y_sides)
    y_slot = {1: 0, -1: NY - 1}

    loads = [pltpu.make_async_copy(solid_hbm, solid, load_sem.at[0])]
    cuts = [0, X // 2, X]
    for n in range(2):
        part = slice(cuts[n], cuts[n + 1])
        loads.append(
            pltpu.make_async_copy(pop_hbm.at[:, :, part], pop.at[:, :, part], load_sem.at[1 + n])
        )
    for copy in loads:
        copy.start()

    parity = lax.rem(me[1], 2)
    is_near, is_far = parity == 0, parity == 1

    def device(offset):
        return tuple(lax.rem(me[d] + offset[d] + count[d], count[d]) for d in range(3))

    barrier = pltpu.get_barrier_semaphore()
    partner = (me[0], me[1] + 1 - 2 * parity, me[2])
    pairs = [me[1] - parity]
    if count[1] > 2:
        pairs.append(lax.rem(me[1] + 3 * parity - 2 + count[1], count[1]))

    def arrive(place):
        pl.semaphore_signal(barrier, inc=1, device_id=place, device_id_type=MESH)

    for dx in (1, -1, 0):
        for dz in (1, -1):
            place = device((dx, 0, dz))
            for base in pairs:
                arrive((place[0], base + 1, place[2]))
    for dx in (1, -1):
        place = device((dx, 0, 0))
        for base in pairs:
            arrive((place[0], base, place[2]))
    for base in pairs[1:]:
        arrive((me[0], base, me[2]))
    arrive(partner)
    near_count, far_count = 4 + 1, 12 + 1
    if count[1] > 2:
        near_count, far_count = near_count + 6, far_count + 12

    lane = lax.broadcasted_iota(jnp.int32, (T, LANES), 1)
    row = lax.broadcasted_iota(jnp.int32, (T, LANES), 0)
    pair = lane // 2
    even = lane % 2 == 0
    half = lane // HALF
    lower = half == 0
    slot = (lane % stride_t) // 2
    tile_t = (lane % HALF) // stride_t
    own_t = (tile_t > 0) & (tile_t <= YT)
    first, last = lane == 0, lane == Z - 1
    lane_y = lax.broadcasted_iota(jnp.int32, (Y, LANES), 1)
    first_y, last_y = lane_y == 0, lane_y == Z - 1
    upper = row < T // 2

    def roll(v, n):
        n = n % LANES
        return pltpu.roll(v, n, 1) if n else v

    def roll_rows(v, n):
        n = n % T
        return pltpu.roll(v, n, 0) if n else v

    def swap(v):
        return jnp.where(even, roll(v, -1), roll(v, 1))

    GROUPS = {"y": 0, "yX": 1, "xS": 2, "xE": 3, "zF": 4, "zD": 5, "xB": 6}
    sent = [0]

    def send(group, src, dst, offset, tiles):
        pltpu.make_async_remote_copy(
            src_ref=src,
            dst_ref=dst,
            send_sem=send_sem,
            recv_sem=recv_sem.at[GROUPS[group]],
            device_id=device(offset),
            device_id_type=MESH,
        ).start()
        sent[0] += tiles

    def await_(group, ref):
        pltpu.make_async_copy(ref, ref, recv_sem.at[GROUPS[group]]).wait()

    def moments(x):
        fluid = solid[x] == 0
        total, mom = [], []
        for k in range(2):
            f = [pop[k, i, x] for i in range(19)]
            rho = f[0]
            m = [None, None, None]
            for i in range(1, 19, 2):
                rho = rho + (f[i] + f[i + 1])
                diff = f[i] - f[i + 1]
                for d in range(3):
                    c = VELOCITIES[i][d]
                    if c:
                        m[d] = (
                            (diff if c > 0 else -diff)
                            if m[d] is None
                            else (m[d] + diff if c > 0 else m[d] - diff)
                        )
            total.append(rho)
            S[k, 2 + x, inner] = jnp.where(fluid, rho, -WALL[k])
            mom.append([v * INV[k] if INV[k] != 1.0 else v for v in m])
        scale = 1.0 / (total[0] * INV[0] + total[1] * INV[1])
        for d in range(3):
            V[d, 1 + x, 0:Y] = (mom[0][d] + mom[1][d]) * scale

    blank = jnp.zeros((T, LANES), jnp.float32)
    packs = [blank, blank, blank, blank]
    POP_PLACE = [(2, 0, 0), (2, 0, 1), (2, 1, 0), (2, 1, 1), (3, 1, 0)]
    V_PLACE = [(1, 0, 0), (1, 0, 1), (1, 1, 0)]

    def put(p, h, b, t, x, value, inside=False):
        j = (h * HALF + t * stride_t + (b * X + x) * 2) // 2
        if inside:
            value = jnp.where(even, roll(value, 2 * j + 2), roll(value, 2 * j))
        else:
            value = roll(value, 2 * j + 1)
        packs[p] = jnp.where(pair == j, value, packs[p])

    def z_ends(i, x, t):
        rows = slice(T * (t - 1), T * t)
        return jnp.where(lane < HALF, pop[1, OPPOSITE[i], x, rows], pop[1, i, x, rows])

    def pack_signs(x):
        for t in range(1, YT + 1):
            for k in range(2):
                value = S[k, 2 + x, T * t:T * t + T]
                put(0, k, 0, t, x, value)
                put(0, k, 1, t, x, value, inside=True)
            for d in range(3):
                put(*V_PLACE[d], t, x, V[d, 1 + x, T * (t - 1):T * t])
            if x in (0, X - 1):
                out_i, in_i = (Z_UP[1], Z_UP[2]) if x else (Z_UP[2], Z_UP[1])
                rows = slice(T * (t - 1), T * t)
                value = jnp.where(lane < HALF, pop[1, OPPOSITE[in_i], x, rows], pop[1, out_i, x, rows])
                put(1, 1, 1, t, x, value)

    loads[0].wait()
    for n in range(2):
        loads[1 + n].wait()
        for x in range(cuts[n], cuts[n + 1]):
            moments(x)
        for x in range(cuts[n], cuts[n + 1]):
            pack_signs(x)

    place = slot % X

    def edges(v, q):
        return jnp.where(upper, roll(v, (q - 1) * stride_t), roll(v, (q - YT) * stride_t))

    for n in range(2):
        if n == 0:
            tile = jnp.where(place >= X - 2, packs[0], roll(packs[1], -2 * (X - 1)))
        else:
            tile = jnp.where(place < 2, packs[0], roll(packs[1], 2 * (X - 1)))
        XSND[n, 0] = jnp.where(tile_t == 0, edges(tile, 0), tile)

    def ends(a, b):
        return jnp.where(upper, a, b)

    t_first, t_last = slice(0, T), slice(Y - T, Y)
    for n, side in enumerate((1, -1)):
        x = X - 1 if side > 0 else 0
        up, down = INDEX[(side, 1, 0)], INDEX[(side, -1, 0)]
        fields = [ends(V[d, 1 + x, t_first], V[d, 1 + x, t_last]) for d in range(3)]
        fields.append(ends(pop[1, down, x, t_first], pop[1, up, x, t_last]))
        packed = fields[0]
        for f in range(1, 4):
            at = (row == 2 * f - 1) | (row == 2 * f)
            packed = jnp.where(at, roll_rows(fields[f], 2 * f), packed)
        XSND[n, 1] = packed

    top_z = me[2] == count[2] - 1
    not_top = jnp.logical_not(top_z)

    def tell(sem):
        pl.semaphore_signal(sem, inc=1, device_id=partner, device_id_type=MESH)

    def learn_far():
        pl.semaphore_wait(barrier, far_count)
        tell(far_sem)

    first_up = lax.rem(me[0], 4) != 1
    sides = [jnp.where(first_up, 1, -1), jnp.where(first_up, -1, 1)]

    def send_x_signs(side):
        up = side > 0
        src = jnp.where(up, X, 2)
        dst = jnp.where(up, 0, X + 2)
        send("xS", S.at[:, pl.ds(src, 2), inner], S.at[:, pl.ds(dst, 2), inner],
             (side, 0, 0), 4 * YT)

    def send_x_bulk(side):
        up = side > 0
        n = jnp.where(up, 0, 1)
        to = (side, 0, 0)
        send("xB", V.at[:, jnp.where(up, X, 1), 0:Y], XB.at[n, 0:3], to, 3 * YT)
        for m, i in enumerate(X_UP):
            send("xB", pop.at[1, jnp.where(up, i, OPPOSITE[i]), jnp.where(up, X - 1, 0)],
                 XB.at[n, 3 + m], to, YT)

    def send_diagonal():
        for n, side in enumerate((1, -1)):
            for m, dz in enumerate((1, -1)):
                send("zD", XSND.at[n, 0], ZD.at[m, n, 0], (side, 0, dz), 1)
                for sy in y_sides:
                    send("zD", XSND.at[n, 0], ZD.at[m, n, 1 + y_slot[-sy]], (side, sy, dz), 1)

    ZS[5] = packs[0]

    def pack_faces():
        for x in range(X):
            for t in range(1, YT + 1):
                for g, i in enumerate(Z_UP):
                    put(*POP_PLACE[g], t, x, z_ends(i, x, t))
        merged = edges(packs[0], 0)
        for p in range(1, 4):
            merged = jnp.where(tile_t == p, edges(packs[p], p), merged)
        for m in range(2):
            one, two = packs[2 * m], packs[2 * m + 1]
            ZS[m] = jnp.where(even, one, roll(two, 1))
            ZS[2 + m] = jnp.where(even, roll(two, -1), one)
        ZS[4] = merged
        packs[2] = packs[3] = blank

    def send_faces():
        for m, dz in enumerate((1, -1)):
            send("zF", ZS.at[2 * m:2 * m + 2], ZF.at[m, 0:2], (0, 0, dz), 2)
            for sy in y_sides:
                send("zF", ZS.at[4], ZF.at[m, 2 + y_slot[-sy]], (0, sy, dz), 1)

    @pl.when(is_far & top_z)
    def _():
        learn_far()

    @pl.when(is_near & top_z)
    def _():
        pl.semaphore_wait(far_sem, 1)

    counted = sent[0]

    @pl.when(top_z)
    def _():
        send_diagonal()
        pack_faces()
        send_faces()

    sent[0] = counted

    @pl.when(is_near)
    def _():
        pl.semaphore_wait(barrier, near_count)
        tell(near_sem)

    @pl.when(is_far)
    def _():
        pl.semaphore_wait(near_sem, 1)

    send_x_signs(sides[0])
    send_x_signs(sides[1])
    for n, side in enumerate((1, -1)):
        for sy in y_sides:
            send("xE", XSND.at[n, 1], XE.at[n, y_slot[-sy]], (side, sy, 0), 1)
    for n, side in enumerate((1, -1)):
        tile = slice(Y - T, Y) if side > 0 else slice(0, T)
        wide = slice(Y, Y + T) if side > 0 else slice(T, 2 * T)
        to = (0, side, 0)
        send("y", S.at[:, 2:2 + X, wide], YR.at[n, 0:2], to, 2 * X)
        send("y", V.at[:, 1:1 + X, tile], YR.at[n, 2:5], to, 3 * X)
        for m, i in enumerate(Y_UP):
            i = i if side > 0 else OPPOSITE[i]
            send("y", pop.at[1, i, :, tile], YR.at[n, 5 + m], to, X)
    send_x_bulk(sides[0])

    @pl.when(not_top)
    def _():
        pack_faces()

    @pl.when(is_far & not_top)
    def _():
        learn_far()

    @pl.when(is_near & not_top)
    def _():
        pl.semaphore_wait(far_sem, 1)

    @pl.when(not_top)
    def _():
        send_diagonal()
        send_faces()

    send_x_bulk(sides[1])
    await_("y", YR)
    for x in range(X):
        for k in range(2):
            value = ends(YR[1, k, x], YR[0, k, x])
            S[k, 2 + x, low] = value
            S[k, 2 + x, high] = value
        for d in range(3):
            V[d, 1 + x, Y:Y + T] = ends(YR[1, 2 + d, x], YR[0, 2 + d, x])
        for m in range(5):
            WP[m, x] = ends(YR[1, 5 + m, x], YR[0, 5 + m, x])

    def window(w, dy):
        if w == 0:
            return slice(T + dy, T + dy + Y)
        return slice(Y + T - 1, Y + 2 * T - 1) if dy < 0 else slice(dy, T + dy)

    def rows_of(w):
        return slice(0, Y) if w == 0 else slice(Y, Y + T)

    def prepare(p):
        for k in range(2):
            for t in range(YT + 1):
                rows = slice(T * t, T * t + T)
                value = S[k, p, rows]
                SU[k, p, rows] = roll(value, -1)
                SD[k, p, rows] = roll(value, 1)

    def spread(tile, k, t, xx):
        return roll(tile, LANES - 1 - (k * HALF + t * stride_t + 2 * xx))

    def complete(p, signs, at):
        for k in range(2):
            for t in range(YT + 1):
                rows = slice(T * t, T * t + T)
                edge = spread(signs, k, t, at)
                above = jnp.where(last, edge, SU[k, p, rows])
                below = jnp.where(first, edge, SD[k, p, rows])
                size = jnp.abs(S[k, p, rows])
                a_above, a_below = jnp.abs(above), jnp.abs(below)
                for r in (rows,) if t else (low, high):
                    psi[k, p, r] = size
                    H[k, p, r] = 2.0 * size + (a_above + a_below)
                    O[k, p, r] = a_above - a_below
                    if k == 0:
                        SU[k, p, r] = above
                        SD[k, p, r] = below

    def sums(p):
        for k in range(2):
            for w in range(2):
                A[k, p, rows_of(w)] = (
                    H[k, p, window(w, 0)] + (psi[k, p, window(w, 1)] + psi[k, p, window(w, -1)])
                ) * (1.0 / 36.0)

    def gradient(k, p, w):
        gx = A[k, p + 1, rows_of(w)] - A[k, p - 1, rows_of(w)]
        sides_y = []
        for dy in (1, -1):
            r = window(w, dy)
            sides_y.append(H[k, p, r] + (psi[k, p + 1, r] + psi[k, p - 1, r]))
        gy = (sides_y[0] - sides_y[1]) * (1.0 / 36.0)
        r = window(w, 0)
        gz = 2.0 * O[k, p, r] + (O[k, p + 1, r] + O[k, p - 1, r])
        gz = (gz + (O[k, p, window(w, 1)] + O[k, p, window(w, -1)])) * (1.0 / 36.0)
        return gx, gy, gz

    def velocities(common, x, w):
        grads = [gradient(k, x + 2, w) for k in range(2)]
        return [
            [common[d] - (COUPLING * RELAX[k]) * grads[1 - k][d] for d in range(3)]
            for k in range(2)
        ]

    def common_of(x, w):
        return [V[d, 1 + x, rows_of(w)] for d in range(3)]

    def flat_of(u):
        return 1.0 - 1.5 * (u[0] * u[0] + u[1] * u[1] + u[2] * u[2])

    def one_way(w, flat, along, sign):
        even_part = w * (flat + 4.5 * (along * along))
        return even_part + w * ((3.0 * sign) * along)

    def collide_own(x):
        us = velocities(common_of(x, 0), x, 0)
        for k in range(2):
            u = us[k]
            rho = psi[k, 2 + x, inner] * INV[k]
            flat = flat_of(u)
            scaled = {w: rho * w for w in sorted(set(WEIGHTS))}
            values = {0: scaled[WEIGHTS[0]] * flat}
            for i in range(1, 19, 2):
                along = along_of(i, u)
                w = scaled[WEIGHTS[i]]
                even_part = w * (flat + 4.5 * (along * along))
                odd_part = w * (3.0 * along)
                values[i] = even_part + odd_part
                values[i + 1] = even_part - odd_part
            for i in range(19):
                if abs(KEEP[k]) > 1e-9:
                    values[i] = values[i] + KEEP[k] * pop[k, i, x]
                post[k, i, 1 + x, inner] = values[i]

    row_sign = jnp.where(upper, -1.0, 1.0)

    def collide_rows(x):
        us = velocities(common_of(x, 1), x, 1)
        for k in range(2):
            u = us[k]
            rho = psi[k, 2 + x, low] * INV[k]
            flat = flat_of(u)
            for m, i in enumerate(Y_UP):
                w = rho * WEIGHTS[i]
                value = one_way(w, flat, along_of(i, u), row_sign)
                if abs(KEEP[k]) > 1e-9:
                    value = value + KEEP[k] * WP[m, x]
                post[k, i, 1 + x, low] = value
                post[k, OPPOSITE[i], 1 + x, high] = value

    def collide_plane(n):
        x = -1 if n == 0 else X
        sign = 1.0 if n == 0 else -1.0
        us = velocities([XB[n, d] for d in range(3)], x, 0)
        for k in range(2):
            u = us[k]
            rho = psi[k, 2 + x, inner] * INV[k]
            flat = flat_of(u)
            for m, i in enumerate(X_UP):
                value = one_way(rho * WEIGHTS[i], flat, along_of(i, u), sign)
                if abs(KEEP[k]) > 1e-9:
                    value = value + KEEP[k] * XB[n, 3 + m]
                post[k, i if n == 0 else OPPOSITE[i], 1 + x, inner] = value

    def collide_corner(n):
        x = -1 if n == 0 else X
        sign = 1.0 if n == 0 else -1.0
        us = velocities(common_of(x, 1), x, 1)
        cx = 1 if n == 0 else -1
        up, down = INDEX[(cx, 1, 0)], INDEX[(cx, -1, 0)]
        for k in range(2):
            u = us[k]
            rho = psi[k, 2 + x, low] * INV[k]
            value = one_way(rho * WEIGHTS[up], flat_of(u), sign * u[0] + row_sign * u[1], 1.0)
            if abs(KEEP[k]) > 1e-9:
                value = value + KEEP[k] * XWP[n]
            post[k, up, 1 + x, low] = value
            post[k, down, 1 + x, high] = value

    def x_up(v):
        return roll(v, -2)

    def x_down(v):
        return roll(v, 2)

    def y_up(v, n=0):
        r = roll_rows(v, -1)
        return jnp.where(row == T - 1, roll(r, n - stride_t), roll(r, n))

    def y_down(v, n=0):
        r = roll_rows(v, 1)
        return jnp.where(row == 0, roll(r, n + stride_t), roll(r, n))

    def collide_z(s0, s1, s2, t1, t2, olds):
        other1, other2 = roll(t1, HALF), roll(t2, HALF)
        common = [
            jnp.where(lower, t1, other1),
            jnp.where(lower, t2, other2),
            jnp.where(lower, other1, t1),
        ]
        p0, p1, p2 = jnp.abs(s0), jnp.abs(s1), jnp.abs(s2)
        xs = [x_up(v) + x_down(v) for v in (p0, p1, p2)]
        ys = [y_up(v) + y_down(v) for v in (p0, p1, p2)]
        g = 2.0 * p1 + (p0 + p2)
        a = g + ys[1]
        b = g + xs[1]
        c0 = 2.0 * p0 + (xs[0] + ys[0])
        c2 = 2.0 * p2 + (xs[2] + ys[2])
        sign = jnp.where(even, 1.0, -1.0)
        grads = [
            roll(a, HALF - 2) - roll(a, HALF + 2),
            y_up(b, HALF) - y_down(b, HALF),
            roll((c0 - c2) * sign, HALF),
        ]
        factor = jnp.where(lower, COUPLING * RELAX[0] / 36.0, COUPLING * RELAX[1] / 36.0)
        u = [common[d] - factor * grads[d] for d in range(3)]
        rho = p1 * jnp.where(lower, INV[0], INV[1])
        keep = jnp.where(lower, KEEP[0], KEEP[1])
        flat = flat_of(u)
        beyond = (slot < 2) | (slot >= X + 2)
        for g, i in enumerate(Z_UP):
            c = VELOCITIES[i]
            old = jnp.where(beyond, t2, olds[g]) if c[0] else olds[g]
            value = one_way(rho * WEIGHTS[i], flat, along_of(i, u), sign)
            value = value + keep * jnp.where(lower, 0.0, old)
            if c[1]:
                a, b = (y_down, y_up) if c[1] > 0 else (y_up, y_down)
                value = jnp.where(even, b(value, -1), a(value, 1))
            else:
                value = jnp.where(even, roll(value, -1 - 2 * c[0]), roll(value, 1 + 2 * c[0]))
            for k in range(2):
                for x in range(X):
                    for t in range(1, YT + 1):
                        zpost[k, g, x, T * (t - 1):T * t] = spread(value, k, t, x + 2)

    def stream(x):
        fluid = solid[x] == 0
        for k in range(2):
            for i in range(19):
                c = VELOCITIES[i]
                rows = slice(T - c[1], T - c[1] + Y)
                read = post[k, i, 1 + x - c[0], rows]
                if i:
                    if c[2]:
                        at = first_y if c[2] > 0 else last_y
                        read = jnp.where(at, zpost[k, Z_PAIR[i], x], roll(read, c[2]))
                    p = 2 + x - c[0]
                    signs = SD if c[2] > 0 else (SU if c[2] else S)
                    bounced = post[k, OPPOSITE[i], 1 + x, inner]
                    read = jnp.where(signs[0, p, rows] > 0.0, read, bounced)
                out[k, i, x] = jnp.where(fluid, read, pop[k, i, x])

    for x in range(X):
        prepare(2 + x)

    await_("xS", S.at[:, 0:4, inner])
    for n, side in enumerate((1, -1)):
        wide = slice(Y, Y + T) if side > 0 else slice(T, 2 * T)
        for m, p in enumerate((0, X + 2)):
            send("yX", S.at[:, p:p + 2, wide], YX.at[n, m], (0, side, 0), 4)
    await_("xE", XE)
    for n in range(2):
        value = XE[n, y_slot[1]]
        if NY > 1:
            value = jnp.where(row % 2 == 0, value, XE[n, y_slot[-1]])
        plane = 0 if n == 0 else X + 1
        for d in range(3):
            V[d, plane, Y:Y + T] = roll_rows(value, -2 * d)
        XWP[n] = roll_rows(value, -6)
    await_("yX", YX)
    for m, base in enumerate((0, X + 2)):
        for q in range(2):
            for k in range(2):
                value = ends(YX[1, m, k, q], YX[0, m, k, q])
                S[k, base + q, low] = value
                S[k, base + q, high] = value
    outer = [0, 1, X + 2, X + 3]
    for p in outer:
        prepare(p)

    def with_rows(tile, w_low, w_high):
        return jnp.where(own_t, tile, jnp.where(tile_t == 0, w_low, w_high))

    def by_row(low_part, high_part):
        return low_part if NY == 1 else ends(low_part, high_part)

    top = stride_t * (YT + 1)

    def assemble(middle, left, right, shift_left, shift_right):
        return jnp.where(
            slot < 2,
            roll(left, 2 * shift_left),
            jnp.where(slot >= X + 2, roll(right, 2 * shift_right), middle),
        )

    s0 = roll(ZS[5], 4)
    for p in range(XX):
        for k in range(2):
            for t in ([0] if 2 <= p < X + 2 else range(YT + 1)):
                j = (k * HALF + t * stride_t) // 2 + p
                s0 = jnp.where(pair == j, roll(S[k, p, T * t:T * t + T], 2 * j + 1), s0)
    s0 = swap(jnp.where(tile_t == YT + 1, roll(s0, top), s0))

    await_("zF", ZF)
    one, two = ZF[0, 0], ZF[1, 0]
    rows_z = [jnp.where(even, ZF[0, 2 + m], ZF[1, 2 + m]) for m in range(NY)]
    z_rows = by_row(rows_z[y_slot[1]], rows_z[y_slot[-1]])
    near_signs = jnp.where(even, roll(two, -1), roll(one, 1))
    near_signs = jnp.where(tile_t == 0, swap(z_rows), near_signs)
    faces = []
    for m in range(2):
        one, two = ZF[0, m], ZF[1, m]
        faces.append(jnp.where(even, one, two))
        faces.append(jnp.where(even, roll(one, -1), roll(two, 1)))
    full = [
        with_rows(faces[p], roll(z_rows, -stride_t * p), roll(z_rows, top - stride_t * p))
        for p in range(4)
    ]
    center = [[roll(full[p], 2 * (2 - b * X)) for b in range(2)] for p in range(2)]
    olds = []
    for p, h, b in POP_PLACE:
        olds.append(roll(full[p], 2 * (2 - b * X) + HALF * (1 - h)))
    for x in range(X):
        complete(2 + x, near_signs, x)
    for x in range(X):
        sums(2 + x)
    for x in range(1, X - 1):
        collide_own(x)
        collide_rows(x)

    await_("zD", ZD)
    diags, far_signs = [], []
    for n in range(2):
        merged = [jnp.where(even, ZD[0, n, q], ZD[1, n, q]) for q in range(1 + NY)]
        w = by_row(merged[1 + y_slot[1]], merged[1 + y_slot[-1]])
        far_signs.append(swap(jnp.where(tile_t == 0, w, merged[0])))
        diags.append(with_rows(merged[0], w, roll(w, top)))
    for m in range(2):
        complete(m, far_signs[0], X - 2 + m)
        complete(X + 2 + m, far_signs[1], m)
    s1, s2 = [
        assemble(center[0][b], *diags, -(b * X + X - 2), X + 2 - b * X) for b in range(2)
    ]
    t1, t2 = [assemble(center[1][b], *diags, 1 - b * X, 3 - b * X) for b in range(2)]
    for p in outer:
        sums(p)
    for x in (0, X - 1):
        collide_own(x)
        collide_rows(x)
    collide_z(s0, s1, s2, t1, t2, olds)
    for n in range(2):
        collide_corner(n)
    for x in range(1, X - 1):
        stream(x)
    await_("xB", XB)
    for n in range(2):
        collide_plane(n)
    for x in (0, X - 1):
        stream(x)
    assert sent[0] == tally.shape[0]
    pltpu.make_async_copy(tally, tally, send_sem).wait()


def body(populations, solid):
    X, Y, Z = solid.shape
    f32 = jnp.float32
    dma = pltpu.SemaphoreType.DMA
    R = Y + 2 * T
    XX = X + 4
    NY = 1 if lax.axis_size("gy") == 2 else 2
    YT = Y // T
    tiles = 20 * X + 24 * YT + 24 + 8 * NY

    def vmem(*shape):
        return pltpu.VMEM(shape, f32)

    return pl.pallas_call(
        step_kernel,
        out_shape=pltpu.VMEM(populations.shape, f32),
        in_specs=[pl.BlockSpec(memory_space=pl.ANY)] * 2,
        out_specs=pl.BlockSpec(memory_space=pltpu.VMEM),
        scratch_shapes=[
            vmem(*populations.shape),
            pltpu.VMEM(solid.shape, jnp.int32),
            vmem(2, XX, R, Z),
            vmem(2, XX, R, Z),
            vmem(2, XX, R, Z),
            vmem(2, XX, R, Z),
            vmem(2, XX, R, Z),
            vmem(2, XX, R, Z),
            vmem(2, XX, Y + T, Z),
            vmem(3, X + 2, Y + T, Z),
            vmem(2, 19, X + 2, R, Z),
            vmem(2, 5, X, Y, Z),
            vmem(2, 10, X, T, Z),
            vmem(5, X, T, Z),
            vmem(2, 8, Y, Z),
            vmem(2, T, Z),
            vmem(2, 2, T, LANES),
            vmem(2, NY, T, LANES),
            vmem(6, T, LANES),
            vmem(2, 2, 2, 2, T, LANES),
            vmem(2, 2 + NY, T, LANES),
            vmem(2, 2, 1 + NY, T, LANES),
            vmem(tiles, T, LANES),
            dma((3,)),
            dma,
            dma((7,)),
            pltpu.SemaphoreType.REGULAR,
            pltpu.SemaphoreType.REGULAR,
        ],
        compiler_params=pltpu.CompilerParams(collective_id=0, has_side_effects=True),
    )(populations, solid)


def solution(mesh):
    in_specs = (P(None, None, "gx", "gy", "gz"), P("gx", "gy", "gz"))
    out_specs = P(None, None, "gx", "gy", "gz")
    return jax.shard_map(body, mesh=mesh, in_specs=in_specs, out_specs=out_specs, check_vma=False)
```

```python
import jax
import jax.numpy as jnp
from jax import lax
from jax.experimental import pallas as pl
from jax.experimental.pallas import tpu as pltpu
from jax.sharding import PartitionSpec as P

VELOCITIES = [
    (0, 0, 0),
    (1, 0, 0),
    (-1, 0, 0),
    (0, 1, 0),
    (0, -1, 0),
    (0, 0, 1),
    (0, 0, -1),
    (1, 1, 0),
    (-1, -1, 0),
    (1, -1, 0),
    (-1, 1, 0),
    (1, 0, 1),
    (-1, 0, -1),
    (1, 0, -1),
    (-1, 0, 1),
    (0, 1, 1),
    (0, -1, -1),
    (0, 1, -1),
    (0, -1, 1),
]
WEIGHTS = [1.0 / 3.0] + [1.0 / 18.0] * 6 + [1.0 / 36.0] * 12
OPPOSITE = [0, 2, 1, 4, 3, 6, 5, 8, 7, 10, 9, 12, 11, 14, 13, 16, 15, 18, 17]
INDEX = {v: i for i, v in enumerate(VELOCITIES)}
COUPLING = 0.9
RELAX = (1.0, 0.8)
WALL = (0.3, 1.5)
INV = [1.0 / t for t in RELAX]
KEEP = [1.0 - v for v in INV]
AXES = ("gx", "gy", "gz")
MESH = pl.DeviceIdType.MESH

X_UP = [i for i in range(19) if VELOCITIES[i][0] == 1]
Y_UP = [i for i in range(19) if VELOCITIES[i][1] == 1]
Z_UP = [(0, 0, 1), (1, 0, 1), (-1, 0, 1), (0, 1, 1), (0, -1, 1)]
Z_UP = [INDEX[v] for v in Z_UP]
Z_PAIR = {}
for _g, _i in enumerate(Z_UP):
    Z_PAIR[_i] = _g
    Z_PAIR[OPPOSITE[_i]] = _g
Z_FROM = [(dx, dz) for dz in (-1, 1) for dx in (0, -1, 1)]
T = 8
LANES = 128
HALF = LANES // 2


def along_of(i, u):
    total = None
    for d in range(3):
        c = VELOCITIES[i][d]
        if c:
            term = u[d] if c > 0 else -u[d]
            total = term if total is None else total + term
    return total


def stream(x, out_at, refs, dirs=range(19)):
    pop, solid, post, zpost, signs, out = refs
    X, Y, Z = solid.shape
    lane = lax.broadcasted_iota(jnp.int32, (Y, Z), 1)
    first, last = lane == 0, lane == Z - 1
    fluid = solid[x] == 0
    for k in range(2):
        for i in dirs:
            c = VELOCITIES[i]
            rows = slice(T - c[1], T - c[1] + Y)
            read = post[k, i, 1 + x - c[0], rows]
            if i:
                if c[2]:
                    shifted = pltpu.roll(read, c[2] % Z, 1)
                    read = jnp.where(first if c[2] > 0 else last, zpost[k, Z_PAIR[i], x], shifted)
                bounced = post[k, OPPOSITE[i], 1 + x, T:T + Y]
                read = jnp.where(signs[c[2] % 3, 2 + x - c[0], rows] > 0.0, read, bounced)
            out[k, i, out_at] = jnp.where(fluid, read, pop[k, i, x])


def finish_kernel(pop, solid, post, zpost, signs, inside, out, ends, sem):
    X, Y, Z = solid.shape
    copies = [pltpu.make_async_copy(inside, out.at[:, :, 1:X - 1], sem.at[0])]
    copies[0].start()
    for n, x in enumerate((0, X - 1)):
        stream(x, n, (pop, solid, post, zpost, signs, ends))
        copies.append(pltpu.make_async_copy(ends.at[:, :, n], out.at[:, :, x], sem.at[1 + n]))
        copies[-1].start()
    for copy in copies:
        copy.wait()


def step_kernel(pop_hbm, solid_hbm, pop, solid, post, zpost, signs, inside, S, SU, SD, psi, H, O, A, V,
                YR, WP, XB, XWP, XSND, XE, ZS, YX, ZF, ZD, tally, load_sem, send_sem, recv_sem,
                near_sem, far_sem):
    X, Y, Z = solid.shape
    YT = Y // T
    inner = slice(T, T + Y)
    low, high = slice(0, T), slice(Y + T, Y + 2 * T)
    XX = X + 4
    stride_t = HALF // (YT + 2)
    assert Z == LANES and YT == 2 and X >= 3
    assert stride_t >= 2 * XX and 2 * X <= XX

    me = [lax.axis_index(a) for a in AXES]
    count = [lax.axis_size(a) for a in AXES]
    assert count[1] % 2 == 0
    y_sides = (1,) if count[1] == 2 else (1, -1)
    NY = len(y_sides)
    y_slot = {1: 0, -1: NY - 1}

    loads = [pltpu.make_async_copy(solid_hbm, solid, load_sem.at[0])]
    cuts = [0, X // 2, X]
    for n in range(2):
        part = slice(cuts[n], cuts[n + 1])
        loads.append(
            pltpu.make_async_copy(pop_hbm.at[:, :, part], pop.at[:, :, part], load_sem.at[1 + n])
        )
    for copy in loads:
        copy.start()

    parity = lax.rem(me[1], 2)
    is_near, is_far = parity == 0, parity == 1

    def device(offset):
        return tuple(lax.rem(me[d] + offset[d] + count[d], count[d]) for d in range(3))

    barrier = pltpu.get_barrier_semaphore()
    partner = (me[0], me[1] + 1 - 2 * parity, me[2])
    pairs = [me[1] - parity]
    if count[1] > 2:
        pairs.append(lax.rem(me[1] + 3 * parity - 2 + count[1], count[1]))

    def arrive(place):
        pl.semaphore_signal(barrier, inc=1, device_id=place, device_id_type=MESH)

    for dx in (1, -1, 0):
        for dz in (1, -1):
            place = device((dx, 0, dz))
            for base in pairs:
                arrive((place[0], base + 1, place[2]))
    for dx in (1, -1):
        place = device((dx, 0, 0))
        for base in pairs:
            arrive((place[0], base, place[2]))
    for base in pairs[1:]:
        arrive((me[0], base, me[2]))
    arrive(partner)
    near_count, far_count = 4 + 1, 12 + 1
    if count[1] > 2:
        near_count, far_count = near_count + 6, far_count + 12

    lane = lax.broadcasted_iota(jnp.int32, (T, LANES), 1)
    row = lax.broadcasted_iota(jnp.int32, (T, LANES), 0)
    pair = lane // 2
    even = lane % 2 == 0
    half = lane // HALF
    lower = half == 0
    slot = (lane % stride_t) // 2
    tile_t = (lane % HALF) // stride_t
    own_t = (tile_t > 0) & (tile_t <= YT)
    first, last = lane == 0, lane == Z - 1
    lane_y = lax.broadcasted_iota(jnp.int32, (Y, LANES), 1)
    first_y, last_y = lane_y == 0, lane_y == Z - 1
    upper = row < T // 2

    def roll(v, n):
        n = n % LANES
        return pltpu.roll(v, n, 1) if n else v

    def roll_rows(v, n):
        n = n % T
        return pltpu.roll(v, n, 0) if n else v

    def swap(v):
        return jnp.where(even, roll(v, -1), roll(v, 1))

    GROUPS = {"y": 0, "yX": 1, "xS": 2, "xE": 3, "zF": 4, "zD": 5, "xB": 6}
    sent = [0]

    def send(group, src, dst, offset, tiles):
        pltpu.make_async_remote_copy(
            src_ref=src,
            dst_ref=dst,
            send_sem=send_sem,
            recv_sem=recv_sem.at[GROUPS[group]],
            device_id=device(offset),
            device_id_type=MESH,
        ).start()
        sent[0] += tiles

    def await_(group, ref):
        pltpu.make_async_copy(ref, ref, recv_sem.at[GROUPS[group]]).wait()

    def moments(x):
        fluid = solid[x] == 0
        total, mom = [], []
        for k in range(2):
            f = [pop[k, i, x] for i in range(19)]
            rho = f[0]
            m = [None, None, None]
            for i in range(1, 19, 2):
                rho = rho + (f[i] + f[i + 1])
                diff = f[i] - f[i + 1]
                for d in range(3):
                    c = VELOCITIES[i][d]
                    if c:
                        m[d] = (
                            (diff if c > 0 else -diff)
                            if m[d] is None
                            else (m[d] + diff if c > 0 else m[d] - diff)
                        )
            total.append(rho)
            S[k, 2 + x, inner] = jnp.where(fluid, rho, -WALL[k])
            mom.append([v * INV[k] if INV[k] != 1.0 else v for v in m])
        scale = 1.0 / (total[0] * INV[0] + total[1] * INV[1])
        for d in range(3):
            V[d, 1 + x, 0:Y] = (mom[0][d] + mom[1][d]) * scale

    blank = jnp.zeros((T, LANES), jnp.float32)
    packs = [blank, blank, blank, blank]
    POP_PLACE = [(2, 0, 0), (2, 0, 1), (2, 1, 0), (2, 1, 1), (3, 1, 0)]
    V_PLACE = [(1, 0, 0), (1, 0, 1), (1, 1, 0)]

    def put(p, h, b, t, x, value, inside=False):
        j = (h * HALF + t * stride_t + (b * X + x) * 2) // 2
        if inside:
            value = jnp.where(even, roll(value, 2 * j + 2), roll(value, 2 * j))
        else:
            value = roll(value, 2 * j + 1)
        packs[p] = jnp.where(pair == j, value, packs[p])

    def z_ends(i, x, t):
        rows = slice(T * (t - 1), T * t)
        return jnp.where(lane < HALF, pop[1, OPPOSITE[i], x, rows], pop[1, i, x, rows])

    def pack_signs(x):
        for t in range(1, YT + 1):
            for k in range(2):
                value = S[k, 2 + x, T * t:T * t + T]
                put(0, k, 0, t, x, value)
                put(0, k, 1, t, x, value, inside=True)
            for d in range(3):
                put(*V_PLACE[d], t, x, V[d, 1 + x, T * (t - 1):T * t])
            if x in (0, X - 1):
                out_i, in_i = (Z_UP[1], Z_UP[2]) if x else (Z_UP[2], Z_UP[1])
                rows = slice(T * (t - 1), T * t)
                value = jnp.where(lane < HALF, pop[1, OPPOSITE[in_i], x, rows], pop[1, out_i, x, rows])
                put(1, 1, 1, t, x, value)

    loads[0].wait()
    for n in range(2):
        loads[1 + n].wait()
        for x in range(cuts[n], cuts[n + 1]):
            moments(x)
        for x in range(cuts[n], cuts[n + 1]):
            pack_signs(x)

    place = slot % X

    def edges(v, q):
        return jnp.where(upper, roll(v, (q - 1) * stride_t), roll(v, (q - YT) * stride_t))

    for n in range(2):
        if n == 0:
            tile = jnp.where(place >= X - 2, packs[0], roll(packs[1], -2 * (X - 1)))
        else:
            tile = jnp.where(place < 2, packs[0], roll(packs[1], 2 * (X - 1)))
        XSND[n, 0] = jnp.where(tile_t == 0, edges(tile, 0), tile)

    def ends(a, b):
        return jnp.where(upper, a, b)

    t_first, t_last = slice(0, T), slice(Y - T, Y)
    for n, side in enumerate((1, -1)):
        x = X - 1 if side > 0 else 0
        up, down = INDEX[(side, 1, 0)], INDEX[(side, -1, 0)]
        fields = [ends(V[d, 1 + x, t_first], V[d, 1 + x, t_last]) for d in range(3)]
        fields.append(ends(pop[1, down, x, t_first], pop[1, up, x, t_last]))
        packed = fields[0]
        for f in range(1, 4):
            at = (row == 2 * f - 1) | (row == 2 * f)
            packed = jnp.where(at, roll_rows(fields[f], 2 * f), packed)
        XSND[n, 1] = packed

    top_z = me[2] == count[2] - 1
    not_top = jnp.logical_not(top_z)

    def tell(sem):
        pl.semaphore_signal(sem, inc=1, device_id=partner, device_id_type=MESH)

    def learn_far():
        pl.semaphore_wait(barrier, far_count)
        tell(far_sem)

    first_up = lax.rem(me[0], 4) != 1
    sides = [jnp.where(first_up, 1, -1), jnp.where(first_up, -1, 1)]

    def send_x_signs(side):
        up = side > 0
        src = jnp.where(up, X, 2)
        dst = jnp.where(up, 0, X + 2)
        send("xS", S.at[:, pl.ds(src, 2), inner], S.at[:, pl.ds(dst, 2), inner],
             (side, 0, 0), 4 * YT)

    def send_x_bulk(side):
        up = side > 0
        n = jnp.where(up, 0, 1)
        to = (side, 0, 0)
        send("xB", V.at[:, jnp.where(up, X, 1), 0:Y], XB.at[n, 0:3], to, 3 * YT)
        for m, i in enumerate(X_UP):
            send("xB", pop.at[1, jnp.where(up, i, OPPOSITE[i]), jnp.where(up, X - 1, 0)],
                 XB.at[n, 3 + m], to, YT)

    def send_diagonal():
        for n, side in enumerate((1, -1)):
            for m, dz in enumerate((1, -1)):
                send("zD", XSND.at[n, 0], ZD.at[m, n, 0], (side, 0, dz), 1)
                for sy in y_sides:
                    send("zD", XSND.at[n, 0], ZD.at[m, n, 1 + y_slot[-sy]], (side, sy, dz), 1)

    ZS[5] = packs[0]

    def pack_faces():
        for x in range(X):
            for t in range(1, YT + 1):
                for g, i in enumerate(Z_UP):
                    put(*POP_PLACE[g], t, x, z_ends(i, x, t))
        merged = edges(packs[0], 0)
        for p in range(1, 4):
            merged = jnp.where(tile_t == p, edges(packs[p], p), merged)
        for m in range(2):
            one, two = packs[2 * m], packs[2 * m + 1]
            ZS[m] = jnp.where(even, one, roll(two, 1))
            ZS[2 + m] = jnp.where(even, roll(two, -1), one)
        ZS[4] = merged
        packs[2] = packs[3] = blank

    def send_faces():
        for m, dz in enumerate((1, -1)):
            send("zF", ZS.at[2 * m:2 * m + 2], ZF.at[m, 0:2], (0, 0, dz), 2)
            for sy in y_sides:
                send("zF", ZS.at[4], ZF.at[m, 2 + y_slot[-sy]], (0, sy, dz), 1)

    @pl.when(is_far & top_z)
    def _():
        learn_far()

    @pl.when(is_near & top_z)
    def _():
        pl.semaphore_wait(far_sem, 1)

    counted = sent[0]

    @pl.when(top_z)
    def _():
        send_diagonal()
        pack_faces()
        send_faces()

    sent[0] = counted

    @pl.when(is_near)
    def _():
        pl.semaphore_wait(barrier, near_count)
        tell(near_sem)

    @pl.when(is_far)
    def _():
        pl.semaphore_wait(near_sem, 1)

    send_x_signs(sides[0])
    send_x_signs(sides[1])
    for n, side in enumerate((1, -1)):
        for sy in y_sides:
            send("xE", XSND.at[n, 1], XE.at[n, y_slot[-sy]], (side, sy, 0), 1)
    for n, side in enumerate((1, -1)):
        tile = slice(Y - T, Y) if side > 0 else slice(0, T)
        wide = slice(Y, Y + T) if side > 0 else slice(T, 2 * T)
        to = (0, side, 0)
        send("y", S.at[:, 2:2 + X, wide], YR.at[n, 0:2], to, 2 * X)
        send("y", V.at[:, 1:1 + X, tile], YR.at[n, 2:5], to, 3 * X)
        for m, i in enumerate(Y_UP):
            i = i if side > 0 else OPPOSITE[i]
            send("y", pop.at[1, i, :, tile], YR.at[n, 5 + m], to, X)
    send_x_bulk(sides[0])

    @pl.when(not_top)
    def _():
        pack_faces()

    @pl.when(is_far & not_top)
    def _():
        learn_far()

    @pl.when(is_near & not_top)
    def _():
        pl.semaphore_wait(far_sem, 1)

    @pl.when(not_top)
    def _():
        send_diagonal()
        send_faces()

    send_x_bulk(sides[1])
    await_("y", YR)
    for x in range(X):
        for k in range(2):
            value = ends(YR[1, k, x], YR[0, k, x])
            S[k, 2 + x, low] = value
            S[k, 2 + x, high] = value
        for d in range(3):
            V[d, 1 + x, Y:Y + T] = ends(YR[1, 2 + d, x], YR[0, 2 + d, x])
        for m in range(5):
            WP[m, x] = ends(YR[1, 5 + m, x], YR[0, 5 + m, x])

    def window(w, dy):
        if w == 0:
            return slice(T + dy, T + dy + Y)
        return slice(Y + T - 1, Y + 2 * T - 1) if dy < 0 else slice(dy, T + dy)

    def rows_of(w):
        return slice(0, Y) if w == 0 else slice(Y, Y + T)

    def prepare(p):
        for k in range(2):
            for t in range(YT + 1):
                rows = slice(T * t, T * t + T)
                value = S[k, p, rows]
                SU[k, p, rows] = roll(value, -1)
                SD[k, p, rows] = roll(value, 1)

    def spread(tile, k, t, xx):
        return roll(tile, LANES - 1 - (k * HALF + t * stride_t + 2 * xx))

    def complete(p, columns, at):
        for k in range(2):
            for t in range(YT + 1):
                rows = slice(T * t, T * t + T)
                edge = spread(columns, k, t, at)
                above = jnp.where(last, edge, SU[k, p, rows])
                below = jnp.where(first, edge, SD[k, p, rows])
                size = jnp.abs(S[k, p, rows])
                a_above, a_below = jnp.abs(above), jnp.abs(below)
                for r in (rows,) if t else (low, high):
                    psi[k, p, r] = size
                    H[k, p, r] = 2.0 * size + (a_above + a_below)
                    O[k, p, r] = a_above - a_below
                    if k == 0:
                        signs[0, p, r] = S[k, p, rows]
                        signs[2, p, r] = above
                        signs[1, p, r] = below

    def sums(p):
        for k in range(2):
            for w in range(2):
                A[k, p, rows_of(w)] = (
                    H[k, p, window(w, 0)] + (psi[k, p, window(w, 1)] + psi[k, p, window(w, -1)])
                ) * (1.0 / 36.0)

    def gradient(k, p, w):
        gx = A[k, p + 1, rows_of(w)] - A[k, p - 1, rows_of(w)]
        sides_y = []
        for dy in (1, -1):
            r = window(w, dy)
            sides_y.append(H[k, p, r] + (psi[k, p + 1, r] + psi[k, p - 1, r]))
        gy = (sides_y[0] - sides_y[1]) * (1.0 / 36.0)
        r = window(w, 0)
        gz = 2.0 * O[k, p, r] + (O[k, p + 1, r] + O[k, p - 1, r])
        gz = (gz + (O[k, p, window(w, 1)] + O[k, p, window(w, -1)])) * (1.0 / 36.0)
        return gx, gy, gz

    def velocities(common, x, w):
        grads = [gradient(k, x + 2, w) for k in range(2)]
        return [
            [common[d] - (COUPLING * RELAX[k]) * grads[1 - k][d] for d in range(3)]
            for k in range(2)
        ]

    def common_of(x, w):
        return [V[d, 1 + x, rows_of(w)] for d in range(3)]

    def flat_of(u):
        return 1.0 - 1.5 * (u[0] * u[0] + u[1] * u[1] + u[2] * u[2])

    def one_way(w, flat, along, sign):
        even_part = w * (flat + 4.5 * (along * along))
        return even_part + w * ((3.0 * sign) * along)

    def collide_own(x):
        us = velocities(common_of(x, 0), x, 0)
        for k in range(2):
            u = us[k]
            rho = psi[k, 2 + x, inner] * INV[k]
            flat = flat_of(u)
            scaled = {w: rho * w for w in sorted(set(WEIGHTS))}
            values = {0: scaled[WEIGHTS[0]] * flat}
            for i in range(1, 19, 2):
                along = along_of(i, u)
                w = scaled[WEIGHTS[i]]
                even_part = w * (flat + 4.5 * (along * along))
                odd_part = w * (3.0 * along)
                values[i] = even_part + odd_part
                values[i + 1] = even_part - odd_part
            for i in range(19):
                if abs(KEEP[k]) > 1e-9:
                    values[i] = values[i] + KEEP[k] * pop[k, i, x]
                post[k, i, 1 + x, inner] = values[i]

    row_sign = jnp.where(upper, -1.0, 1.0)

    def collide_rows(x):
        us = velocities(common_of(x, 1), x, 1)
        for k in range(2):
            u = us[k]
            rho = psi[k, 2 + x, low] * INV[k]
            flat = flat_of(u)
            for m, i in enumerate(Y_UP):
                w = rho * WEIGHTS[i]
                value = one_way(w, flat, along_of(i, u), row_sign)
                if abs(KEEP[k]) > 1e-9:
                    value = value + KEEP[k] * WP[m, x]
                post[k, i, 1 + x, low] = value
                post[k, OPPOSITE[i], 1 + x, high] = value

    def collide_plane(n):
        x = -1 if n == 0 else X
        sign = 1.0 if n == 0 else -1.0
        us = velocities([XB[n, d] for d in range(3)], x, 0)
        for k in range(2):
            u = us[k]
            rho = psi[k, 2 + x, inner] * INV[k]
            flat = flat_of(u)
            for m, i in enumerate(X_UP):
                value = one_way(rho * WEIGHTS[i], flat, along_of(i, u), sign)
                if abs(KEEP[k]) > 1e-9:
                    value = value + KEEP[k] * XB[n, 3 + m]
                post[k, i if n == 0 else OPPOSITE[i], 1 + x, inner] = value

    def collide_corner(n):
        x = -1 if n == 0 else X
        sign = 1.0 if n == 0 else -1.0
        us = velocities(common_of(x, 1), x, 1)
        cx = 1 if n == 0 else -1
        up, down = INDEX[(cx, 1, 0)], INDEX[(cx, -1, 0)]
        for k in range(2):
            u = us[k]
            rho = psi[k, 2 + x, low] * INV[k]
            value = one_way(rho * WEIGHTS[up], flat_of(u), sign * u[0] + row_sign * u[1], 1.0)
            if abs(KEEP[k]) > 1e-9:
                value = value + KEEP[k] * XWP[n]
            post[k, up, 1 + x, low] = value
            post[k, down, 1 + x, high] = value

    def x_up(v):
        return roll(v, -2)

    def x_down(v):
        return roll(v, 2)

    def y_up(v, n=0):
        r = roll_rows(v, -1)
        return jnp.where(row == T - 1, roll(r, n - stride_t), roll(r, n))

    def y_down(v, n=0):
        r = roll_rows(v, 1)
        return jnp.where(row == 0, roll(r, n + stride_t), roll(r, n))

    def collide_z(s0, s1, s2, t1, t2, olds):
        other1, other2 = roll(t1, HALF), roll(t2, HALF)
        common = [
            jnp.where(lower, t1, other1),
            jnp.where(lower, t2, other2),
            jnp.where(lower, other1, t1),
        ]
        p0, p1, p2 = jnp.abs(s0), jnp.abs(s1), jnp.abs(s2)
        xs = [x_up(v) + x_down(v) for v in (p0, p1, p2)]
        ys = [y_up(v) + y_down(v) for v in (p0, p1, p2)]
        g = 2.0 * p1 + (p0 + p2)
        a = g + ys[1]
        b = g + xs[1]
        c0 = 2.0 * p0 + (xs[0] + ys[0])
        c2 = 2.0 * p2 + (xs[2] + ys[2])
        sign = jnp.where(even, 1.0, -1.0)
        grads = [
            roll(a, HALF - 2) - roll(a, HALF + 2),
            y_up(b, HALF) - y_down(b, HALF),
            roll((c0 - c2) * sign, HALF),
        ]
        factor = jnp.where(lower, COUPLING * RELAX[0] / 36.0, COUPLING * RELAX[1] / 36.0)
        u = [common[d] - factor * grads[d] for d in range(3)]
        rho = p1 * jnp.where(lower, INV[0], INV[1])
        keep = jnp.where(lower, KEEP[0], KEEP[1])
        flat = flat_of(u)
        beyond = (slot < 2) | (slot >= X + 2)
        for g, i in enumerate(Z_UP):
            c = VELOCITIES[i]
            old = jnp.where(beyond, t2, olds[g]) if c[0] else olds[g]
            value = one_way(rho * WEIGHTS[i], flat, along_of(i, u), sign)
            value = value + keep * jnp.where(lower, 0.0, old)
            if c[1]:
                a, b = (y_down, y_up) if c[1] > 0 else (y_up, y_down)
                value = jnp.where(even, b(value, -1), a(value, 1))
            else:
                value = jnp.where(even, roll(value, -1 - 2 * c[0]), roll(value, 1 + 2 * c[0]))
            for k in range(2):
                for x in range(X):
                    for t in range(1, YT + 1):
                        zpost[k, g, x, T * (t - 1):T * t] = spread(value, k, t, x + 2)

    for x in range(X):
        prepare(2 + x)

    await_("xS", S.at[:, 0:4, inner])
    for n, side in enumerate((1, -1)):
        wide = slice(Y, Y + T) if side > 0 else slice(T, 2 * T)
        for m, p in enumerate((0, X + 2)):
            send("yX", S.at[:, p:p + 2, wide], YX.at[n, m], (0, side, 0), 4)
    await_("xE", XE)
    for n in range(2):
        value = XE[n, y_slot[1]]
        if NY > 1:
            value = jnp.where(row % 2 == 0, value, XE[n, y_slot[-1]])
        plane = 0 if n == 0 else X + 1
        for d in range(3):
            V[d, plane, Y:Y + T] = roll_rows(value, -2 * d)
        XWP[n] = roll_rows(value, -6)
    await_("yX", YX)
    for m, base in enumerate((0, X + 2)):
        for q in range(2):
            for k in range(2):
                value = ends(YX[1, m, k, q], YX[0, m, k, q])
                S[k, base + q, low] = value
                S[k, base + q, high] = value
    outer = [0, 1, X + 2, X + 3]
    for p in outer:
        prepare(p)

    def with_rows(tile, w_low, w_high):
        return jnp.where(own_t, tile, jnp.where(tile_t == 0, w_low, w_high))

    def by_row(low_part, high_part):
        return low_part if NY == 1 else ends(low_part, high_part)

    top = stride_t * (YT + 1)

    def assemble(middle, left, right, shift_left, shift_right):
        return jnp.where(
            slot < 2,
            roll(left, 2 * shift_left),
            jnp.where(slot >= X + 2, roll(right, 2 * shift_right), middle),
        )

    s0 = roll(ZS[5], 4)
    for p in range(XX):
        for k in range(2):
            for t in ([0] if 2 <= p < X + 2 else range(YT + 1)):
                j = (k * HALF + t * stride_t) // 2 + p
                s0 = jnp.where(pair == j, roll(S[k, p, T * t:T * t + T], 2 * j + 1), s0)
    s0 = swap(jnp.where(tile_t == YT + 1, roll(s0, top), s0))

    await_("zF", ZF)
    one, two = ZF[0, 0], ZF[1, 0]
    rows_z = [jnp.where(even, ZF[0, 2 + m], ZF[1, 2 + m]) for m in range(NY)]
    z_rows = by_row(rows_z[y_slot[1]], rows_z[y_slot[-1]])
    near_signs = jnp.where(even, roll(two, -1), roll(one, 1))
    near_signs = jnp.where(tile_t == 0, swap(z_rows), near_signs)
    faces = []
    for m in range(2):
        one, two = ZF[0, m], ZF[1, m]
        faces.append(jnp.where(even, one, two))
        faces.append(jnp.where(even, roll(one, -1), roll(two, 1)))
    full = [
        with_rows(faces[p], roll(z_rows, -stride_t * p), roll(z_rows, top - stride_t * p))
        for p in range(4)
    ]
    center = [[roll(full[p], 2 * (2 - b * X)) for b in range(2)] for p in range(2)]
    olds = []
    for p, h, b in POP_PLACE:
        olds.append(roll(full[p], 2 * (2 - b * X) + HALF * (1 - h)))
    for x in range(X):
        complete(2 + x, near_signs, x)
    for x in range(X):
        sums(2 + x)
    for x in range(1, X - 1):
        collide_own(x)
        collide_rows(x)

    await_("zD", ZD)
    diags, far_signs = [], []
    for n in range(2):
        merged = [jnp.where(even, ZD[0, n, q], ZD[1, n, q]) for q in range(1 + NY)]
        w = by_row(merged[1 + y_slot[1]], merged[1 + y_slot[-1]])
        far_signs.append(swap(jnp.where(tile_t == 0, w, merged[0])))
        diags.append(with_rows(merged[0], w, roll(w, top)))
    for m in range(2):
        complete(m, far_signs[0], X - 2 + m)
        complete(X + 2 + m, far_signs[1], m)
    s1, s2 = [
        assemble(center[0][b], *diags, -(b * X + X - 2), X + 2 - b * X) for b in range(2)
    ]
    t1, t2 = [assemble(center[1][b], *diags, 1 - b * X, 3 - b * X) for b in range(2)]
    for p in outer:
        sums(p)
    for x in (0, X - 1):
        collide_own(x)
        collide_rows(x)
    collide_z(s0, s1, s2, t1, t2, olds)
    for n in range(2):
        collide_corner(n)
    for x in range(1, X - 1):
        stream(x, x - 1, (pop, solid, post, zpost, signs, inside))
    await_("xB", XB)
    for n in range(2):
        collide_plane(n)
    assert sent[0] == tally.shape[0]
    pltpu.make_async_copy(tally, tally, send_sem).wait()


def body(populations, solid):
    X, Y, Z = solid.shape
    f32 = jnp.float32
    dma = pltpu.SemaphoreType.DMA
    R = Y + 2 * T
    XX = X + 4
    NY = 1 if lax.axis_size("gy") == 2 else 2
    YT = Y // T
    tiles = 20 * X + 24 * YT + 24 + 8 * NY

    def vmem(*shape):
        return pltpu.VMEM(shape, f32)

    shapes = [
        populations.shape,
        solid.shape,
        (2, 19, X + 2, R, Z),
        (2, 5, X, Y, Z),
        (3, XX, R, Z),
        (2, 19, X - 2, Y, Z),
    ]
    types = [solid.dtype if n == 1 else f32 for n in range(6)]
    in_vmem = pl.BlockSpec(memory_space=pltpu.VMEM)
    state = pl.pallas_call(
        step_kernel,
        out_shape=[pltpu.VMEM(a, b) for a, b in zip(shapes, types)],
        in_specs=[pl.BlockSpec(memory_space=pltpu.HBM)] * 2,
        out_specs=[in_vmem] * 6,
        scratch_shapes=[
            vmem(2, XX, R, Z),
            vmem(2, XX, R, Z),
            vmem(2, XX, R, Z),
            vmem(2, XX, R, Z),
            vmem(2, XX, R, Z),
            vmem(2, XX, R, Z),
            vmem(2, XX, Y + T, Z),
            vmem(3, X + 2, Y + T, Z),
            vmem(2, 10, X, T, Z),
            vmem(5, X, T, Z),
            vmem(2, 8, Y, Z),
            vmem(2, T, Z),
            vmem(2, 2, T, LANES),
            vmem(2, NY, T, LANES),
            vmem(6, T, LANES),
            vmem(2, 2, 2, 2, T, LANES),
            vmem(2, 2 + NY, T, LANES),
            vmem(2, 2, 1 + NY, T, LANES),
            vmem(tiles, T, LANES),
            dma((3,)),
            dma,
            dma((7,)),
            pltpu.SemaphoreType.REGULAR,
            pltpu.SemaphoreType.REGULAR,
        ],
        compiler_params=pltpu.CompilerParams(
            collective_id=0, has_side_effects=True, vmem_limit_bytes=24 * 2**20
        ),
    )(*[pltpu.with_memory_space_constraint(v, pltpu.HBM) for v in (populations, solid)])
    return pl.pallas_call(
        finish_kernel,
        out_shape=jax.ShapeDtypeStruct(populations.shape, f32),
        in_specs=[in_vmem] * 6,
        out_specs=pl.BlockSpec(memory_space=pl.ANY),
        scratch_shapes=[vmem(2, 19, 2, Y, Z), dma((3,))],
        compiler_params=pltpu.CompilerParams(vmem_limit_bytes=16 * 2**20),
    )(*state)


def solution(mesh):
    in_specs = (P(None, None, "gx", "gy", "gz"), P("gx", "gy", "gz"))
    out_specs = P(None, None, "gx", "gy", "gz")
    return jax.shard_map(body, mesh=mesh, in_specs=in_specs, out_specs=out_specs, check_vma=False)
```

```python
import jax
import jax.numpy as jnp
from jax import lax
from jax.experimental import pallas as pl
from jax.experimental.pallas import tpu as pltpu
from jax.sharding import PartitionSpec as P

VELOCITIES = [
    (0, 0, 0),
    (1, 0, 0),
    (-1, 0, 0),
    (0, 1, 0),
    (0, -1, 0),
    (0, 0, 1),
    (0, 0, -1),
    (1, 1, 0),
    (-1, -1, 0),
    (1, -1, 0),
    (-1, 1, 0),
    (1, 0, 1),
    (-1, 0, -1),
    (1, 0, -1),
    (-1, 0, 1),
    (0, 1, 1),
    (0, -1, -1),
    (0, 1, -1),
    (0, -1, 1),
]
WEIGHTS = [1.0 / 3.0] + [1.0 / 18.0] * 6 + [1.0 / 36.0] * 12
OPPOSITE = [0, 2, 1, 4, 3, 6, 5, 8, 7, 10, 9, 12, 11, 14, 13, 16, 15, 18, 17]
INDEX = {v: i for i, v in enumerate(VELOCITIES)}
COUPLING = 0.9
RELAX = (1.0, 0.8)
WALL = (0.3, 1.5)
INV = [1.0 / t for t in RELAX]
KEEP = [1.0 - v for v in INV]
AXES = ("gx", "gy", "gz")
MESH = pl.DeviceIdType.MESH

X_UP = [i for i in range(19) if VELOCITIES[i][0] == 1]
Y_UP = [i for i in range(19) if VELOCITIES[i][1] == 1]
Z_UP = [(0, 0, 1), (1, 0, 1), (-1, 0, 1), (0, 1, 1), (0, -1, 1)]
Z_UP = [INDEX[v] for v in Z_UP]
Z_PAIR = {}
for _g, _i in enumerate(Z_UP):
    Z_PAIR[_i] = _g
    Z_PAIR[OPPOSITE[_i]] = _g
Z_FROM = [(dx, dz) for dz in (-1, 1) for dx in (0, -1, 1)]
T = 8
LANES = 128
HALF = LANES // 2


def along_of(i, u):
    total = None
    for d in range(3):
        c = VELOCITIES[i][d]
        if c:
            term = u[d] if c > 0 else -u[d]
            total = term if total is None else total + term
    return total


def reach(x, X):
    return [i for i, c in enumerate(VELOCITIES) if 1 <= x - c[0] <= X - 2 and c[2] == 0]


def stream(x, out_at, refs, dirs=range(19)):
    pop, solid, post, zpost, signs, out = refs
    X, Y, Z = solid.shape
    lane = lax.broadcasted_iota(jnp.int32, (Y, Z), 1)
    first, last = lane == 0, lane == Z - 1
    fluid = solid[x] == 0
    for k in range(2):
        for i in dirs:
            c = VELOCITIES[i]
            rows = slice(T - c[1], T - c[1] + Y)
            read = post[k, i, 1 + x - c[0], rows]
            if i:
                if c[2]:
                    shifted = pltpu.roll(read, c[2] % Z, 1)
                    read = jnp.where(first if c[2] > 0 else last, zpost[k, Z_PAIR[i], x], shifted)
                bounced = post[k, OPPOSITE[i], 1 + x, T:T + Y]
                read = jnp.where(signs[c[2] % 3, 2 + x - c[0], rows] > 0.0, read, bounced)
            out[k, i, out_at] = jnp.where(fluid, read, pop[k, i, x])


def finish_kernel(pop, solid, post, zpost, signs, inside, out, ends, sem):
    X, Y, Z = solid.shape
    copies = [pltpu.make_async_copy(inside, out.at[:, :, 1:X - 1], sem.at[0])]
    copies[0].start()
    for n, x in enumerate((0, X - 1)):
        stream(x, n, (pop, solid, post, zpost, signs, ends))
        copies.append(pltpu.make_async_copy(ends.at[:, :, n], out.at[:, :, x], sem.at[1 + n]))
        copies[-1].start()
    for copy in copies:
        copy.wait()


def step_kernel(pop_hbm, solid_hbm, pop, solid, post, zpost, signs, inside, S, SU, SD, psi, H, O, A, V,
                YR, WP, XB, XWP, XSND, XE, ZS, YX, ZF, ZD, tally, load_sem, send_sem, recv_sem,
                near_sem, far_sem):
    X, Y, Z = solid.shape
    YT = Y // T
    inner = slice(T, T + Y)
    low, high = slice(0, T), slice(Y + T, Y + 2 * T)
    XX = X + 4
    stride_t = HALF // (YT + 2)
    assert Z == LANES and YT == 2 and X >= 3
    assert stride_t >= 2 * XX and 2 * X <= XX

    me = [lax.axis_index(a) for a in AXES]
    count = [lax.axis_size(a) for a in AXES]
    assert count[1] % 2 == 0
    y_sides = (1,) if count[1] == 2 else (1, -1)
    NY = len(y_sides)
    y_slot = {1: 0, -1: NY - 1}

    loads = [pltpu.make_async_copy(solid_hbm, solid, load_sem.at[0])]
    for n in range(X):
        part = slice(X - 1 - n, X - n)
        loads.append(
            pltpu.make_async_copy(pop_hbm.at[:, :, part], pop.at[:, :, part], load_sem.at[1 + n])
        )
    for copy in loads:
        copy.start()

    parity = lax.rem(me[1], 2)
    is_near, is_far = parity == 0, parity == 1

    def device(offset):
        return tuple(lax.rem(me[d] + offset[d] + count[d], count[d]) for d in range(3))

    barrier = pltpu.get_barrier_semaphore()
    partner = (me[0], me[1] + 1 - 2 * parity, me[2])
    pairs = [me[1] - parity]
    if count[1] > 2:
        pairs.append(lax.rem(me[1] + 3 * parity - 2 + count[1], count[1]))

    def arrive(place):
        pl.semaphore_signal(barrier, inc=1, device_id=place, device_id_type=MESH)

    for dx in (1, -1, 0):
        for dz in (1, -1):
            place = device((dx, 0, dz))
            for base in pairs:
                arrive((place[0], base + 1, place[2]))
    for dx in (1, -1):
        place = device((dx, 0, 0))
        for base in pairs:
            arrive((place[0], base, place[2]))
    for base in pairs[1:]:
        arrive((me[0], base, me[2]))
    arrive(partner)
    near_count, far_count = 4 + 1, 12 + 1
    if count[1] > 2:
        near_count, far_count = near_count + 6, far_count + 12

    lane = lax.broadcasted_iota(jnp.int32, (T, LANES), 1)
    row = lax.broadcasted_iota(jnp.int32, (T, LANES), 0)
    pair = lane // 2
    even = lane % 2 == 0
    half = lane // HALF
    lower = half == 0
    slot = (lane % stride_t) // 2
    tile_t = (lane % HALF) // stride_t
    own_t = (tile_t > 0) & (tile_t <= YT)
    first, last = lane == 0, lane == Z - 1
    lane_y = lax.broadcasted_iota(jnp.int32, (Y, LANES), 1)
    first_y, last_y = lane_y == 0, lane_y == Z - 1
    upper = row < T // 2

    def roll(v, n):
        n = n % LANES
        return pltpu.roll(v, n, 1) if n else v

    def roll_rows(v, n):
        n = n % T
        return pltpu.roll(v, n, 0) if n else v

    def swap(v):
        return jnp.where(even, roll(v, -1), roll(v, 1))

    GROUPS = {"y": 0, "yX": 1, "xS": 2, "xE": 3, "zF": 4, "zD": 5, "xB": 6}
    sent = [0]

    def send(group, src, dst, offset, tiles):
        pltpu.make_async_remote_copy(
            src_ref=src,
            dst_ref=dst,
            send_sem=send_sem,
            recv_sem=recv_sem.at[GROUPS[group]],
            device_id=device(offset),
            device_id_type=MESH,
        ).start()
        sent[0] += tiles

    def await_(group, ref):
        pltpu.make_async_copy(ref, ref, recv_sem.at[GROUPS[group]]).wait()

    def moments(x):
        fluid = solid[x] == 0
        total, mom = [], []
        for k in range(2):
            f = [pop[k, i, x] for i in range(19)]
            rho = f[0]
            m = [None, None, None]
            for i in range(1, 19, 2):
                rho = rho + (f[i] + f[i + 1])
                diff = f[i] - f[i + 1]
                for d in range(3):
                    c = VELOCITIES[i][d]
                    if c:
                        m[d] = (
                            (diff if c > 0 else -diff)
                            if m[d] is None
                            else (m[d] + diff if c > 0 else m[d] - diff)
                        )
            total.append(rho)
            S[k, 2 + x, inner] = jnp.where(fluid, rho, -WALL[k])
            mom.append([v * INV[k] if INV[k] != 1.0 else v for v in m])
        scale = 1.0 / (total[0] * INV[0] + total[1] * INV[1])
        for d in range(3):
            V[d, 1 + x, 0:Y] = (mom[0][d] + mom[1][d]) * scale

    blank = jnp.zeros((T, LANES), jnp.float32)
    packs = [blank, blank, blank, blank]
    POP_PLACE = [(2, 0, 0), (2, 0, 1), (2, 1, 0), (2, 1, 1), (3, 1, 0)]
    V_PLACE = [(1, 0, 0), (1, 0, 1), (1, 1, 0)]

    def put(p, h, b, t, x, value, inside=False):
        j = (h * HALF + t * stride_t + (b * X + x) * 2) // 2
        if inside:
            value = jnp.where(even, roll(value, 2 * j + 2), roll(value, 2 * j))
        else:
            value = roll(value, 2 * j + 1)
        packs[p] = jnp.where(pair == j, value, packs[p])

    def z_ends(i, x, t):
        rows = slice(T * (t - 1), T * t)
        return jnp.where(lane < HALF, pop[1, OPPOSITE[i], x, rows], pop[1, i, x, rows])

    beside = [blank, blank]

    def put_beside(x, h, b, t, value):
        n, at = (1, X - 1) if x == 0 else (0, 0)
        j = (h * HALF + t * stride_t + (b * X + at) * 2) // 2
        beside[n] = jnp.where(pair == j, roll(value, 2 * j + 1), beside[n])

    def pack_signs(x):
        for t in range(1, YT + 1):
            rows = slice(T * (t - 1), T * t)
            for k in range(2):
                value = S[k, 2 + x, T * t:T * t + T]
                put(0, k, 0, t, x, value)
                put(0, k, 1, t, x, value, inside=True)
            if x in (0, X - 1):
                for d in range(3):
                    put_beside(x, *V_PLACE[d][1:], t, V[d, 1 + x, rows])
                out_i, in_i = (Z_UP[1], Z_UP[2]) if x else (Z_UP[2], Z_UP[1])
                value = jnp.where(lane < HALF, pop[1, OPPOSITE[in_i], x, rows], pop[1, out_i, x, rows])
                put_beside(x, 1, 1, t, value)

    top_z = me[2] == count[2] - 1
    not_top = jnp.logical_not(top_z)

    def tell(sem):
        pl.semaphore_signal(sem, inc=1, device_id=partner, device_id_type=MESH)

    def learn_far():
        pl.semaphore_wait(barrier, far_count)
        tell(far_sem)

    corner = top_z & (me[0] == count[0] - 1)
    place = slot % X

    def edges(v, q):
        return jnp.where(upper, roll(v, (q - 1) * stride_t), roll(v, (q - YT) * stride_t))

    def make_diagonal(n):
        tile = jnp.where((place >= X - 2) if n == 0 else (place < 2), packs[0], beside[n])
        XSND[n, 0] = jnp.where(tile_t == 0, edges(tile, 0), tile)

    def send_diagonal(n):
        side = 1 - 2 * n
        for m, dz in enumerate((1, -1)):
            send("zD", XSND.at[n, 0], ZD.at[m, n, 0], (side, 0, dz), 1)
            for sy in y_sides:
                send("zD", XSND.at[n, 0], ZD.at[m, n, 1 + y_slot[-sy]], (side, sy, dz), 1)

    @pl.when(is_far & corner)
    def _():
        learn_far()

    loads[0].wait()
    for n in range(X):
        loads[1 + n].wait()
        moments(X - 1 - n)
        pack_signs(X - 1 - n)
        if n == 1:
            make_diagonal(0)

            @pl.when(is_near & corner)
            def _():
                pl.semaphore_wait(far_sem, 1)

            @pl.when(corner)
            def _():
                send_diagonal(0)

    make_diagonal(1)

    def ends(a, b):
        return jnp.where(upper, a, b)

    t_first, t_last = slice(0, T), slice(Y - T, Y)
    for n, side in enumerate((1, -1)):
        x = X - 1 if side > 0 else 0
        up, down = INDEX[(side, 1, 0)], INDEX[(side, -1, 0)]
        fields = [ends(V[d, 1 + x, t_first], V[d, 1 + x, t_last]) for d in range(3)]
        fields.append(ends(pop[1, down, x, t_first], pop[1, up, x, t_last]))
        packed = fields[0]
        for f in range(1, 4):
            at = (row == 2 * f - 1) | (row == 2 * f)
            packed = jnp.where(at, roll_rows(fields[f], 2 * f), packed)
        XSND[n, 1] = packed

    first_up = lax.rem(me[0], 4) != 1
    sides = [jnp.where(first_up, 1, -1), jnp.where(first_up, -1, 1)]

    def send_x_signs(side):
        up = side > 0
        src = jnp.where(up, X, 2)
        dst = jnp.where(up, 0, X + 2)
        send("xS", S.at[:, pl.ds(src, 2), inner], S.at[:, pl.ds(dst, 2), inner],
             (side, 0, 0), 4 * YT)

    def send_x_bulk(side):
        up = side > 0
        n = jnp.where(up, 0, 1)
        to = (side, 0, 0)
        send("xB", V.at[:, jnp.where(up, X, 1), 0:Y], XB.at[n, 0:3], to, 3 * YT)
        for m, i in enumerate(X_UP):
            send("xB", pop.at[1, jnp.where(up, i, OPPOSITE[i]), jnp.where(up, X - 1, 0)],
                 XB.at[n, 3 + m], to, YT)

    ZS[5] = packs[0]

    def pack_faces():
        packs[1] = jnp.where(place == X - 1, roll(beside[0], 2 * (X - 1)), roll(beside[1], -2 * (X - 1)))
        for x in range(X):
            for t in range(1, YT + 1):
                for d in range(3) if 0 < x < X - 1 else ():
                    put(*V_PLACE[d], t, x, V[d, 1 + x, T * (t - 1):T * t])
                for g, i in enumerate(Z_UP):
                    put(*POP_PLACE[g], t, x, z_ends(i, x, t))
        merged = edges(packs[0], 0)
        for p in range(1, 4):
            merged = jnp.where(tile_t == p, edges(packs[p], p), merged)
        for m in range(2):
            one, two = packs[2 * m], packs[2 * m + 1]
            ZS[m] = jnp.where(even, one, roll(two, 1))
            ZS[2 + m] = jnp.where(even, roll(two, -1), one)
        ZS[4] = merged
        packs[1] = packs[2] = packs[3] = blank

    def send_faces():
        for m, dz in enumerate((1, -1)):
            send("zF", ZS.at[2 * m:2 * m + 2], ZF.at[m, 0:2], (0, 0, dz), 2)
            for sy in y_sides:
                send("zF", ZS.at[4], ZF.at[m, 2 + y_slot[-sy]], (0, sy, dz), 1)

    late = top_z & jnp.logical_not(corner)

    @pl.when(is_far & late)
    def _():
        learn_far()

    @pl.when(is_near & late)
    def _():
        pl.semaphore_wait(far_sem, 1)

    @pl.when(late)
    def _():
        send_diagonal(0)

    @pl.when(top_z)
    def _():
        send_diagonal(1)
        pack_faces()
        send_faces()

    sent[0] = 0

    @pl.when(is_near)
    def _():
        pl.semaphore_wait(barrier, near_count)
        tell(near_sem)

    @pl.when(is_far)
    def _():
        pl.semaphore_wait(near_sem, 1)

    send_x_signs(sides[0])
    send_x_signs(sides[1])
    for n, side in enumerate((1, -1)):
        for sy in y_sides:
            send("xE", XSND.at[n, 1], XE.at[n, y_slot[-sy]], (side, sy, 0), 1)
    for n, side in enumerate((1, -1)):
        tile = slice(Y - T, Y) if side > 0 else slice(0, T)
        wide = slice(Y, Y + T) if side > 0 else slice(T, 2 * T)
        to = (0, side, 0)
        send("y", S.at[:, 2:2 + X, wide], YR.at[n, 0:2], to, 2 * X)
        send("y", V.at[:, 1:1 + X, tile], YR.at[n, 2:5], to, 3 * X)
        for m, i in enumerate(Y_UP):
            i = i if side > 0 else OPPOSITE[i]
            send("y", pop.at[1, i, :, tile], YR.at[n, 5 + m], to, X)
    send_x_bulk(sides[0])

    @pl.when(not_top)
    def _():
        pack_faces()

    @pl.when(is_far & not_top)
    def _():
        learn_far()

    @pl.when(is_near & not_top)
    def _():
        pl.semaphore_wait(far_sem, 1)

    @pl.when(not_top)
    def _():
        send_diagonal(0)
        send_diagonal(1)
        send_faces()

    send_x_bulk(sides[1])
    await_("y", YR)
    for x in range(X):
        for k in range(2):
            value = ends(YR[1, k, x], YR[0, k, x])
            S[k, 2 + x, low] = value
            S[k, 2 + x, high] = value
        for d in range(3):
            V[d, 1 + x, Y:Y + T] = ends(YR[1, 2 + d, x], YR[0, 2 + d, x])
        for m in range(5):
            WP[m, x] = ends(YR[1, 5 + m, x], YR[0, 5 + m, x])

    def window(w, dy):
        if w == 0:
            return slice(T + dy, T + dy + Y)
        return slice(Y + T - 1, Y + 2 * T - 1) if dy < 0 else slice(dy, T + dy)

    def rows_of(w):
        return slice(0, Y) if w == 0 else slice(Y, Y + T)

    def prepare(p):
        for k in range(2):
            for t in range(YT + 1):
                rows = slice(T * t, T * t + T)
                value = S[k, p, rows]
                SU[k, p, rows] = roll(value, -1)
                SD[k, p, rows] = roll(value, 1)

    def spread(tile, k, t, xx):
        return roll(tile, LANES - 1 - (k * HALF + t * stride_t + 2 * xx))

    def complete(p, columns, at):
        for k in range(2):
            for t in range(YT + 1):
                rows = slice(T * t, T * t + T)
                edge = spread(columns, k, t, at)
                above = jnp.where(last, edge, SU[k, p, rows])
                below = jnp.where(first, edge, SD[k, p, rows])
                size = jnp.abs(S[k, p, rows])
                a_above, a_below = jnp.abs(above), jnp.abs(below)
                for r in (rows,) if t else (low, high):
                    psi[k, p, r] = size
                    H[k, p, r] = 2.0 * size + (a_above + a_below)
                    O[k, p, r] = a_above - a_below
                    if k == 0:
                        signs[0, p, r] = S[k, p, rows]
                        signs[2, p, r] = above
                        signs[1, p, r] = below

    def sums(p):
        for k in range(2):
            for w in range(2):
                A[k, p, rows_of(w)] = (
                    H[k, p, window(w, 0)] + (psi[k, p, window(w, 1)] + psi[k, p, window(w, -1)])
                ) * (1.0 / 36.0)

    def gradient(k, p, w):
        gx = A[k, p + 1, rows_of(w)] - A[k, p - 1, rows_of(w)]
        sides_y = []
        for dy in (1, -1):
            r = window(w, dy)
            sides_y.append(H[k, p, r] + (psi[k, p + 1, r] + psi[k, p - 1, r]))
        gy = (sides_y[0] - sides_y[1]) * (1.0 / 36.0)
        r = window(w, 0)
        gz = 2.0 * O[k, p, r] + (O[k, p + 1, r] + O[k, p - 1, r])
        gz = (gz + (O[k, p, window(w, 1)] + O[k, p, window(w, -1)])) * (1.0 / 36.0)
        return gx, gy, gz

    def velocities(common, x, w):
        grads = [gradient(k, x + 2, w) for k in range(2)]
        return [
            [common[d] - (COUPLING * RELAX[k]) * grads[1 - k][d] for d in range(3)]
            for k in range(2)
        ]

    def common_of(x, w):
        return [V[d, 1 + x, rows_of(w)] for d in range(3)]

    def flat_of(u):
        return 1.0 - 1.5 * (u[0] * u[0] + u[1] * u[1] + u[2] * u[2])

    def one_way(w, flat, along, sign):
        even_part = w * (flat + 4.5 * (along * along))
        return even_part + w * ((3.0 * sign) * along)

    def collide_own(x):
        us = velocities(common_of(x, 0), x, 0)
        for k in range(2):
            u = us[k]
            rho = psi[k, 2 + x, inner] * INV[k]
            flat = flat_of(u)
            scaled = {w: rho * w for w in sorted(set(WEIGHTS))}
            values = {0: scaled[WEIGHTS[0]] * flat}
            for i in range(1, 19, 2):
                along = along_of(i, u)
                w = scaled[WEIGHTS[i]]
                even_part = w * (flat + 4.5 * (along * along))
                odd_part = w * (3.0 * along)
                values[i] = even_part + odd_part
                values[i + 1] = even_part - odd_part
            for i in range(19):
                if abs(KEEP[k]) > 1e-9:
                    values[i] = values[i] + KEEP[k] * pop[k, i, x]
                post[k, i, 1 + x, inner] = values[i]

    row_sign = jnp.where(upper, -1.0, 1.0)

    def collide_rows(x):
        us = velocities(common_of(x, 1), x, 1)
        for k in range(2):
            u = us[k]
            rho = psi[k, 2 + x, low] * INV[k]
            flat = flat_of(u)
            for m, i in enumerate(Y_UP):
                w = rho * WEIGHTS[i]
                value = one_way(w, flat, along_of(i, u), row_sign)
                if abs(KEEP[k]) > 1e-9:
                    value = value + KEEP[k] * WP[m, x]
                post[k, i, 1 + x, low] = value
                post[k, OPPOSITE[i], 1 + x, high] = value

    def collide_plane(n):
        x = -1 if n == 0 else X
        sign = 1.0 if n == 0 else -1.0
        us = velocities([XB[n, d] for d in range(3)], x, 0)
        for k in range(2):
            u = us[k]
            rho = psi[k, 2 + x, inner] * INV[k]
            flat = flat_of(u)
            for m, i in enumerate(X_UP):
                value = one_way(rho * WEIGHTS[i], flat, along_of(i, u), sign)
                if abs(KEEP[k]) > 1e-9:
                    value = value + KEEP[k] * XB[n, 3 + m]
                post[k, i if n == 0 else OPPOSITE[i], 1 + x, inner] = value

    def collide_corner(n):
        x = -1 if n == 0 else X
        sign = 1.0 if n == 0 else -1.0
        us = velocities(common_of(x, 1), x, 1)
        cx = 1 if n == 0 else -1
        up, down = INDEX[(cx, 1, 0)], INDEX[(cx, -1, 0)]
        for k in range(2):
            u = us[k]
            rho = psi[k, 2 + x, low] * INV[k]
            value = one_way(rho * WEIGHTS[up], flat_of(u), sign * u[0] + row_sign * u[1], 1.0)
            if abs(KEEP[k]) > 1e-9:
                value = value + KEEP[k] * XWP[n]
            post[k, up, 1 + x, low] = value
            post[k, down, 1 + x, high] = value

    def x_up(v):
        return roll(v, -2)

    def x_down(v):
        return roll(v, 2)

    def y_up(v, n=0):
        r = roll_rows(v, -1)
        return jnp.where(row == T - 1, roll(r, n - stride_t), roll(r, n))

    def y_down(v, n=0):
        r = roll_rows(v, 1)
        return jnp.where(row == 0, roll(r, n + stride_t), roll(r, n))

    def collide_z(s0, s1, s2, t1, t2, olds):
        other1, other2 = roll(t1, HALF), roll(t2, HALF)
        common = [
            jnp.where(lower, t1, other1),
            jnp.where(lower, t2, other2),
            jnp.where(lower, other1, t1),
        ]
        p0, p1, p2 = jnp.abs(s0), jnp.abs(s1), jnp.abs(s2)
        xs = [x_up(v) + x_down(v) for v in (p0, p1, p2)]
        ys = [y_up(v) + y_down(v) for v in (p0, p1, p2)]
        g = 2.0 * p1 + (p0 + p2)
        a = g + ys[1]
        b = g + xs[1]
        c0 = 2.0 * p0 + (xs[0] + ys[0])
        c2 = 2.0 * p2 + (xs[2] + ys[2])
        sign = jnp.where(even, 1.0, -1.0)
        grads = [
            roll(a, HALF - 2) - roll(a, HALF + 2),
            y_up(b, HALF) - y_down(b, HALF),
            roll((c0 - c2) * sign, HALF),
        ]
        factor = jnp.where(lower, COUPLING * RELAX[0] / 36.0, COUPLING * RELAX[1] / 36.0)
        u = [common[d] - factor * grads[d] for d in range(3)]
        rho = p1 * jnp.where(lower, INV[0], INV[1])
        keep = jnp.where(lower, KEEP[0], KEEP[1])
        flat = flat_of(u)
        beyond = (slot < 2) | (slot >= X + 2)
        for g, i in enumerate(Z_UP):
            c = VELOCITIES[i]
            old = jnp.where(beyond, t2, olds[g]) if c[0] else olds[g]
            value = one_way(rho * WEIGHTS[i], flat, along_of(i, u), sign)
            value = value + keep * jnp.where(lower, 0.0, old)
            if c[1]:
                a, b = (y_down, y_up) if c[1] > 0 else (y_up, y_down)
                value = jnp.where(even, b(value, -1), a(value, 1))
            else:
                value = jnp.where(even, roll(value, -1 - 2 * c[0]), roll(value, 1 + 2 * c[0]))
            for k in range(2):
                for x in range(X):
                    for t in range(1, YT + 1):
                        zpost[k, g, x, T * (t - 1):T * t] = spread(value, k, t, x + 2)

    for x in range(X):
        prepare(2 + x)

    await_("xS", S.at[:, 0:4, inner])
    for n, side in enumerate((1, -1)):
        wide = slice(Y, Y + T) if side > 0 else slice(T, 2 * T)
        for m, p in enumerate((0, X + 2)):
            send("yX", S.at[:, p:p + 2, wide], YX.at[n, m], (0, side, 0), 4)
    await_("xE", XE)
    for n in range(2):
        value = XE[n, y_slot[1]]
        if NY > 1:
            value = jnp.where(row % 2 == 0, value, XE[n, y_slot[-1]])
        plane = 0 if n == 0 else X + 1
        for d in range(3):
            V[d, plane, Y:Y + T] = roll_rows(value, -2 * d)
        XWP[n] = roll_rows(value, -6)
    await_("yX", YX)
    for m, base in enumerate((0, X + 2)):
        for q in range(2):
            for k in range(2):
                value = ends(YX[1, m, k, q], YX[0, m, k, q])
                S[k, base + q, low] = value
                S[k, base + q, high] = value
    outer = [0, 1, X + 2, X + 3]
    for p in outer:
        prepare(p)

    def with_rows(tile, w_low, w_high):
        return jnp.where(own_t, tile, jnp.where(tile_t == 0, w_low, w_high))

    def by_row(low_part, high_part):
        return low_part if NY == 1 else ends(low_part, high_part)

    top = stride_t * (YT + 1)

    def assemble(middle, left, right, shift_left, shift_right):
        return jnp.where(
            slot < 2,
            roll(left, 2 * shift_left),
            jnp.where(slot >= X + 2, roll(right, 2 * shift_right), middle),
        )

    s0 = roll(ZS[5], 4)
    for p in range(XX):
        for k in range(2):
            for t in ([0] if 2 <= p < X + 2 else range(YT + 1)):
                j = (k * HALF + t * stride_t) // 2 + p
                s0 = jnp.where(pair == j, roll(S[k, p, T * t:T * t + T], 2 * j + 1), s0)
    s0 = swap(jnp.where(tile_t == YT + 1, roll(s0, top), s0))

    await_("zF", ZF)
    one, two = ZF[0, 0], ZF[1, 0]
    rows_z = [jnp.where(even, ZF[0, 2 + m], ZF[1, 2 + m]) for m in range(NY)]
    z_rows = by_row(rows_z[y_slot[1]], rows_z[y_slot[-1]])
    near_signs = jnp.where(even, roll(two, -1), roll(one, 1))
    near_signs = jnp.where(tile_t == 0, swap(z_rows), near_signs)
    faces = []
    for m in range(2):
        one, two = ZF[0, m], ZF[1, m]
        faces.append(jnp.where(even, one, two))
        faces.append(jnp.where(even, roll(one, -1), roll(two, 1)))
    full = [
        with_rows(faces[p], roll(z_rows, -stride_t * p), roll(z_rows, top - stride_t * p))
        for p in range(4)
    ]
    center = [[roll(full[p], 2 * (2 - b * X)) for b in range(2)] for p in range(2)]
    olds = []
    for p, h, b in POP_PLACE:
        olds.append(roll(full[p], 2 * (2 - b * X) + HALF * (1 - h)))
    for x in range(X):
        complete(2 + x, near_signs, x)
    for x in range(X):
        sums(2 + x)
    for x in range(1, X - 1):
        collide_own(x)
        collide_rows(x)
    state = (pop, solid, post, zpost, signs, inside)
    for x in range(1, X - 1):
        stream(x, x - 1, state, reach(x, X))

    await_("zD", ZD)
    diags, far_signs = [], []
    for n in range(2):
        merged = [jnp.where(even, ZD[0, n, q], ZD[1, n, q]) for q in range(1 + NY)]
        w = by_row(merged[1 + y_slot[1]], merged[1 + y_slot[-1]])
        far_signs.append(swap(jnp.where(tile_t == 0, w, merged[0])))
        diags.append(with_rows(merged[0], w, roll(w, top)))
    for m in range(2):
        complete(m, far_signs[0], X - 2 + m)
        complete(X + 2 + m, far_signs[1], m)
    s1, s2 = [
        assemble(center[0][b], *diags, -(b * X + X - 2), X + 2 - b * X) for b in range(2)
    ]
    t1, t2 = [assemble(center[1][b], *diags, 1 - b * X, 3 - b * X) for b in range(2)]
    for p in outer:
        sums(p)
    for x in (0, X - 1):
        collide_own(x)
        collide_rows(x)
    collide_z(s0, s1, s2, t1, t2, olds)
    for n in range(2):
        collide_corner(n)
    for x in range(1, X - 1):
        stream(x, x - 1, state, [i for i in range(19) if i not in reach(x, X)])
    await_("xB", XB)
    for n in range(2):
        collide_plane(n)
    assert sent[0] == tally.shape[0]
    pltpu.make_async_copy(tally, tally, send_sem).wait()


def body(populations, solid):
    X, Y, Z = solid.shape
    f32 = jnp.float32
    dma = pltpu.SemaphoreType.DMA
    R = Y + 2 * T
    XX = X + 4
    NY = 1 if lax.axis_size("gy") == 2 else 2
    YT = Y // T
    tiles = 20 * X + 24 * YT + 24 + 8 * NY

    def vmem(*shape):
        return pltpu.VMEM(shape, f32)

    shapes = [
        populations.shape,
        solid.shape,
        (2, 19, X + 2, R, Z),
        (2, 5, X, Y, Z),
        (3, XX, R, Z),
        (2, 19, X - 2, Y, Z),
    ]
    types = [solid.dtype if n == 1 else f32 for n in range(6)]
    in_vmem = pl.BlockSpec(memory_space=pltpu.VMEM)
    state = pl.pallas_call(
        step_kernel,
        out_shape=[pltpu.VMEM(a, b) for a, b in zip(shapes, types)],
        in_specs=[pl.BlockSpec(memory_space=pltpu.HBM)] * 2,
        out_specs=[in_vmem] * 6,
        scratch_shapes=[
            vmem(2, XX, R, Z),
            vmem(2, XX, R, Z),
            vmem(2, XX, R, Z),
            vmem(2, XX, R, Z),
            vmem(2, XX, R, Z),
            vmem(2, XX, R, Z),
            vmem(2, XX, Y + T, Z),
            vmem(3, X + 2, Y + T, Z),
            vmem(2, 10, X, T, Z),
            vmem(5, X, T, Z),
            vmem(2, 8, Y, Z),
            vmem(2, T, Z),
            vmem(2, 2, T, LANES),
            vmem(2, NY, T, LANES),
            vmem(6, T, LANES),
            vmem(2, 2, 2, 2, T, LANES),
            vmem(2, 2 + NY, T, LANES),
            vmem(2, 2, 1 + NY, T, LANES),
            vmem(tiles, T, LANES),
            dma((X + 1,)),
            dma,
            dma((7,)),
            pltpu.SemaphoreType.REGULAR,
            pltpu.SemaphoreType.REGULAR,
        ],
        compiler_params=pltpu.CompilerParams(
            collective_id=0, has_side_effects=True, vmem_limit_bytes=24 * 2**20
        ),
    )(*[pltpu.with_memory_space_constraint(v, pltpu.HBM) for v in (populations, solid)])
    return pl.pallas_call(
        finish_kernel,
        out_shape=jax.ShapeDtypeStruct(populations.shape, f32),
        in_specs=[in_vmem] * 6,
        out_specs=pl.BlockSpec(memory_space=pl.ANY),
        scratch_shapes=[vmem(2, 19, 2, Y, Z), dma((3,))],
        compiler_params=pltpu.CompilerParams(vmem_limit_bytes=16 * 2**20),
    )(*state)


def solution(mesh):
    in_specs = (P(None, None, "gx", "gy", "gz"), P("gx", "gy", "gz"))
    out_specs = P(None, None, "gx", "gy", "gz")
    return jax.shard_map(body, mesh=mesh, in_specs=in_specs, out_specs=out_specs, check_vma=False)
```

```python
import jax
import jax.numpy as jnp
from jax import lax
from jax.experimental import pallas as pl
from jax.experimental.pallas import tpu as pltpu
from jax.sharding import PartitionSpec as P

VELOCITIES = [
    (0, 0, 0),
    (1, 0, 0),
    (-1, 0, 0),
    (0, 1, 0),
    (0, -1, 0),
    (0, 0, 1),
    (0, 0, -1),
    (1, 1, 0),
    (-1, -1, 0),
    (1, -1, 0),
    (-1, 1, 0),
    (1, 0, 1),
    (-1, 0, -1),
    (1, 0, -1),
    (-1, 0, 1),
    (0, 1, 1),
    (0, -1, -1),
    (0, 1, -1),
    (0, -1, 1),
]
WEIGHTS = [1.0 / 3.0] + [1.0 / 18.0] * 6 + [1.0 / 36.0] * 12
OPPOSITE = [0, 2, 1, 4, 3, 6, 5, 8, 7, 10, 9, 12, 11, 14, 13, 16, 15, 18, 17]
INDEX = {v: i for i, v in enumerate(VELOCITIES)}
COUPLING = 0.9
RELAX = (1.0, 0.8)
WALL = (0.3, 1.5)
INV = [1.0 / t for t in RELAX]
KEEP = [1.0 - v for v in INV]
AXES = ("gx", "gy", "gz")
MESH = pl.DeviceIdType.MESH

X_UP = [i for i in range(19) if VELOCITIES[i][0] == 1]
Y_UP = [i for i in range(19) if VELOCITIES[i][1] == 1]
Z_UP = [(0, 0, 1), (1, 0, 1), (-1, 0, 1), (0, 1, 1), (0, -1, 1)]
Z_UP = [INDEX[v] for v in Z_UP]
Z_PAIR = {}
for _g, _i in enumerate(Z_UP):
    Z_PAIR[_i] = _g
    Z_PAIR[OPPOSITE[_i]] = _g
Z_FROM = [(dx, dz) for dz in (-1, 1) for dx in (0, -1, 1)]
T = 8
LANES = 128
HALF = LANES // 2


def along_of(i, u):
    total = None
    for d in range(3):
        c = VELOCITIES[i][d]
        if c:
            term = u[d] if c > 0 else -u[d]
            total = term if total is None else total + term
    return total


def reach(x, X):
    return [i for i, c in enumerate(VELOCITIES) if 1 <= x - c[0] <= X - 2 and c[2] == 0]


def stream(x, out_at, refs, dirs=range(19)):
    pop, solid, post, zpost, signs, out = refs
    X, Y, Z = solid.shape
    lane = lax.broadcasted_iota(jnp.int32, (Y, Z), 1)
    first, last = lane == 0, lane == Z - 1
    fluid = solid[x] == 0
    for k in range(2):
        for i in dirs:
            c = VELOCITIES[i]
            rows = slice(T - c[1], T - c[1] + Y)
            read = post[k, i, 1 + x - c[0], rows]
            if i:
                if c[2]:
                    shifted = pltpu.roll(read, c[2] % Z, 1)
                    read = jnp.where(first if c[2] > 0 else last, zpost[k, Z_PAIR[i], x], shifted)
                bounced = post[k, OPPOSITE[i], 1 + x, T:T + Y]
                read = jnp.where(signs[c[2] % 3, 2 + x - c[0], rows] > 0.0, read, bounced)
            out[k, i, out_at] = jnp.where(fluid, read, pop[k, i, x])


def finish_kernel(pop, solid, post, zpost, signs, inside, out, ends, sem):
    X, Y, Z = solid.shape
    copies = [pltpu.make_async_copy(inside, out.at[:, :, 1:X - 1], sem.at[0])]
    copies[0].start()
    for n, x in enumerate((0, X - 1)):
        stream(x, n, (pop, solid, post, zpost, signs, ends))
        copies.append(pltpu.make_async_copy(ends.at[:, :, n], out.at[:, :, x], sem.at[1 + n]))
        copies[-1].start()
    for copy in copies:
        copy.wait()


def step_kernel(pop_hbm, solid_hbm, pop, solid, post, zpost, signs, inside, S, SU, SD, psi, H, O, A, V,
                YR, WP, XB, XWP, XSND, XE, ZS, YX, ZF, ZD, tally, load_sem, send_sem, recv_sem,
                near_sem, far_sem):
    X, Y, Z = solid.shape
    YT = Y // T
    inner = slice(T, T + Y)
    low, high = slice(0, T), slice(Y + T, Y + 2 * T)
    XX = X + 4
    stride_t = HALF // (YT + 2)
    assert Z == LANES and YT == 2 and X >= 3
    assert stride_t >= 2 * XX and 2 * X <= XX

    me = [lax.axis_index(a) for a in AXES]
    count = [lax.axis_size(a) for a in AXES]
    assert count[1] % 2 == 0
    y_sides = (1,) if count[1] == 2 else (1, -1)
    NY = len(y_sides)
    y_slot = {1: 0, -1: NY - 1}

    loads = [pltpu.make_async_copy(solid_hbm, solid, load_sem.at[0])]
    for n in range(X):
        part = slice(X - 1 - n, X - n)
        loads.append(
            pltpu.make_async_copy(pop_hbm.at[:, :, part], pop.at[:, :, part], load_sem.at[1 + n])
        )
    for copy in loads:
        copy.start()

    parity = lax.rem(me[1], 2)
    is_near, is_far = parity == 0, parity == 1

    def device(offset):
        return tuple(lax.rem(me[d] + offset[d] + count[d], count[d]) for d in range(3))

    barrier = pltpu.get_barrier_semaphore()
    partner = (me[0], me[1] + 1 - 2 * parity, me[2])
    pairs = [me[1] - parity]
    if count[1] > 2:
        pairs.append(lax.rem(me[1] + 3 * parity - 2 + count[1], count[1]))

    def arrive(place):
        pl.semaphore_signal(barrier, inc=1, device_id=place, device_id_type=MESH)

    for dx in (1, -1, 0):
        for dz in (1, -1):
            place = device((dx, 0, dz))
            for base in pairs:
                arrive((place[0], base + 1, place[2]))
    for dx in (1, -1):
        place = device((dx, 0, 0))
        for base in pairs:
            arrive((place[0], base, place[2]))
    for base in pairs[1:]:
        arrive((me[0], base, me[2]))
    arrive(partner)
    near_count, far_count = 4 + 1, 12 + 1
    if count[1] > 2:
        near_count, far_count = near_count + 6, far_count + 12

    lane = lax.broadcasted_iota(jnp.int32, (T, LANES), 1)
    row = lax.broadcasted_iota(jnp.int32, (T, LANES), 0)
    pair = lane // 2
    even = lane % 2 == 0
    half = lane // HALF
    lower = half == 0
    slot = (lane % stride_t) // 2
    tile_t = (lane % HALF) // stride_t
    own_t = (tile_t > 0) & (tile_t <= YT)
    first, last = lane == 0, lane == Z - 1
    lane_y = lax.broadcasted_iota(jnp.int32, (Y, LANES), 1)
    first_y, last_y = lane_y == 0, lane_y == Z - 1
    upper = row < T // 2

    def roll(v, n):
        n = n % LANES
        return pltpu.roll(v, n, 1) if n else v

    def roll_rows(v, n):
        n = n % T
        return pltpu.roll(v, n, 0) if n else v

    def swap(v):
        return jnp.where(even, roll(v, -1), roll(v, 1))

    GROUPS = {"y": 0, "yX": 1, "xS": 2, "xE": 3, "zF": 4, "zD": 5, "xB": 6}
    sent = [0]

    def send(group, src, dst, offset, tiles, first=False):
        pltpu.make_async_remote_copy(
            src_ref=src,
            dst_ref=dst,
            send_sem=send_sem.at[1 if first else 0],
            recv_sem=recv_sem.at[GROUPS[group]],
            device_id=device(offset),
            device_id_type=MESH,
        ).start()
        sent[0] += 0 if first else tiles

    def await_(group, ref):
        pltpu.make_async_copy(ref, ref, recv_sem.at[GROUPS[group]]).wait()

    def moments(x):
        fluid = solid[x] == 0
        total, mom = [], []
        for k in range(2):
            f = [pop[k, i, x] for i in range(19)]
            rho = f[0]
            m = [None, None, None]
            for i in range(1, 19, 2):
                rho = rho + (f[i] + f[i + 1])
                diff = f[i] - f[i + 1]
                for d in range(3):
                    c = VELOCITIES[i][d]
                    if c:
                        m[d] = (
                            (diff if c > 0 else -diff)
                            if m[d] is None
                            else (m[d] + diff if c > 0 else m[d] - diff)
                        )
            total.append(rho)
            S[k, 2 + x, inner] = jnp.where(fluid, rho, -WALL[k])
            mom.append([v * INV[k] if INV[k] != 1.0 else v for v in m])
        scale = 1.0 / (total[0] * INV[0] + total[1] * INV[1])
        for d in range(3):
            V[d, 1 + x, 0:Y] = (mom[0][d] + mom[1][d]) * scale

    blank = jnp.zeros((T, LANES), jnp.float32)
    packs = [blank, blank, blank, blank]
    POP_PLACE = [(2, 0, 0), (2, 0, 1), (2, 1, 0), (2, 1, 1), (3, 1, 0)]
    V_PLACE = [(1, 0, 0), (1, 0, 1), (1, 1, 0)]

    def put(p, h, b, t, x, value, inside=False):
        j = (h * HALF + t * stride_t + (b * X + x) * 2) // 2
        if inside:
            value = jnp.where(even, roll(value, 2 * j + 2), roll(value, 2 * j))
        else:
            value = roll(value, 2 * j + 1)
        packs[p] = jnp.where(pair == j, value, packs[p])

    def z_ends(i, x, t):
        rows = slice(T * (t - 1), T * t)
        return jnp.where(lane < HALF, pop[1, OPPOSITE[i], x, rows], pop[1, i, x, rows])

    beside = [blank, blank]

    def put_beside(x, h, b, t, value):
        n, at = (1, X - 1) if x == 0 else (0, 0)
        j = (h * HALF + t * stride_t + (b * X + at) * 2) // 2
        beside[n] = jnp.where(pair == j, roll(value, 2 * j + 1), beside[n])

    def pack_signs(x):
        for t in range(1, YT + 1):
            rows = slice(T * (t - 1), T * t)
            for k in range(2):
                value = S[k, 2 + x, T * t:T * t + T]
                put(0, k, 0, t, x, value)
                put(0, k, 1, t, x, value, inside=True)
            if x in (0, X - 1):
                for d in range(3):
                    put_beside(x, *V_PLACE[d][1:], t, V[d, 1 + x, rows])
                out_i, in_i = (Z_UP[1], Z_UP[2]) if x else (Z_UP[2], Z_UP[1])
                value = jnp.where(lane < HALF, pop[1, OPPOSITE[in_i], x, rows], pop[1, out_i, x, rows])
                put_beside(x, 1, 1, t, value)

    top_z = me[2] == count[2] - 1
    not_top = jnp.logical_not(top_z)

    def tell(sem):
        pl.semaphore_signal(sem, inc=1, device_id=partner, device_id_type=MESH)

    def learn_far():
        pl.semaphore_wait(barrier, far_count)
        tell(far_sem)

    corner = top_z & (me[0] == count[0] - 1)
    place = slot % X

    def edges(v, q):
        return jnp.where(upper, roll(v, (q - 1) * stride_t), roll(v, (q - YT) * stride_t))

    def make_diagonal(n):
        tile = jnp.where((place >= X - 2) if n == 0 else (place < 2), packs[0], beside[n])
        XSND[n, 0] = jnp.where(tile_t == 0, edges(tile, 0), tile)

    def send_diagonal(n):
        side = 1 - 2 * n
        for m, dz in enumerate((1, -1)):
            send("zD", XSND.at[n, 0], ZD.at[m, n, 0], (side, 0, dz), 1)
            for sy in y_sides:
                send("zD", XSND.at[n, 0], ZD.at[m, n, 1 + y_slot[-sy]], (side, sy, dz), 1)

    @pl.when(is_far & corner)
    def _():
        learn_far()

    loads[0].wait()
    for n in range(X):
        loads[1 + n].wait()
        moments(X - 1 - n)
        pack_signs(X - 1 - n)
        if n == 1:
            make_diagonal(0)

            @pl.when(is_near & corner)
            def _():
                pl.semaphore_wait(far_sem, 1)

            @pl.when(corner)
            def _():
                send_diagonal(0)

    make_diagonal(1)

    def ends(a, b):
        return jnp.where(upper, a, b)

    t_first, t_last = slice(0, T), slice(Y - T, Y)
    for n, side in enumerate((1, -1)):
        x = X - 1 if side > 0 else 0
        up, down = INDEX[(side, 1, 0)], INDEX[(side, -1, 0)]
        fields = [ends(V[d, 1 + x, t_first], V[d, 1 + x, t_last]) for d in range(3)]
        fields.append(ends(pop[1, down, x, t_first], pop[1, up, x, t_last]))
        packed = fields[0]
        for f in range(1, 4):
            at = (row == 2 * f - 1) | (row == 2 * f)
            packed = jnp.where(at, roll_rows(fields[f], 2 * f), packed)
        XSND[n, 1] = packed

    first_up = lax.rem(me[0], 4) != 1
    sides = [jnp.where(first_up, 1, -1), jnp.where(first_up, -1, 1)]

    def send_x_signs(side):
        up = side > 0
        src = jnp.where(up, X, 2)
        dst = jnp.where(up, 0, X + 2)
        send("xS", S.at[:, pl.ds(src, 2), inner], S.at[:, pl.ds(dst, 2), inner],
             (side, 0, 0), 4 * YT)

    def send_x_bulk(side, first):
        up = side > 0
        n = jnp.where(up, 0, 1)
        to = (side, 0, 0)
        send("xB", V.at[:, jnp.where(up, X, 1), 0:Y], XB.at[n, 0:3], to, 3 * YT, first)
        for m, i in enumerate(X_UP):
            send("xB", pop.at[1, jnp.where(up, i, OPPOSITE[i]), jnp.where(up, X - 1, 0)],
                 XB.at[n, 3 + m], to, YT, first)

    ZS[5] = packs[0]

    def pack_faces():
        packs[1] = jnp.where(place == X - 1, roll(beside[0], 2 * (X - 1)), roll(beside[1], -2 * (X - 1)))
        for x in range(X):
            for t in range(1, YT + 1):
                for d in range(3) if 0 < x < X - 1 else ():
                    put(*V_PLACE[d], t, x, V[d, 1 + x, T * (t - 1):T * t])
                for g, i in enumerate(Z_UP):
                    put(*POP_PLACE[g], t, x, z_ends(i, x, t))
        merged = edges(packs[0], 0)
        for p in range(1, 4):
            merged = jnp.where(tile_t == p, edges(packs[p], p), merged)
        for m in range(2):
            one, two = packs[2 * m], packs[2 * m + 1]
            ZS[m] = jnp.where(even, one, roll(two, 1))
            ZS[2 + m] = jnp.where(even, roll(two, -1), one)
        ZS[4] = merged
        packs[1] = packs[2] = packs[3] = blank

    def send_faces():
        for m, dz in enumerate((1, -1)):
            send("zF", ZS.at[2 * m:2 * m + 2], ZF.at[m, 0:2], (0, 0, dz), 2)
            for sy in y_sides:
                send("zF", ZS.at[4], ZF.at[m, 2 + y_slot[-sy]], (0, sy, dz), 1)

    late = top_z & jnp.logical_not(corner)

    @pl.when(late)
    def _():
        pack_faces()

    @pl.when(is_far & late)
    def _():
        learn_far()

    @pl.when(is_near & late)
    def _():
        pl.semaphore_wait(far_sem, 1)

    @pl.when(late)
    def _():
        send_faces()
        send_diagonal(0)
        send_diagonal(1)

    @pl.when(corner)
    def _():
        send_diagonal(1)
        pack_faces()
        send_faces()

    sent[0] = 0

    @pl.when(is_near)
    def _():
        pl.semaphore_wait(barrier, near_count)
        tell(near_sem)

    @pl.when(is_far)
    def _():
        pl.semaphore_wait(near_sem, 1)

    send_x_signs(sides[0])
    send_x_signs(sides[1])
    for n, side in enumerate((1, -1)):
        for sy in y_sides:
            send("xE", XSND.at[n, 1], XE.at[n, y_slot[-sy]], (side, sy, 0), 1)
    for n, side in enumerate((1, -1)):
        tile = slice(Y - T, Y) if side > 0 else slice(0, T)
        wide = slice(Y, Y + T) if side > 0 else slice(T, 2 * T)
        to = (0, side, 0)
        send("y", S.at[:, 2:2 + X, wide], YR.at[n, 0:2], to, 2 * X)
        send("y", V.at[:, 1:1 + X, tile], YR.at[n, 2:5], to, 3 * X)
        for m, i in enumerate(Y_UP):
            i = i if side > 0 else OPPOSITE[i]
            send("y", pop.at[1, i, :, tile], YR.at[n, 5 + m], to, X)
    send_x_bulk(sides[0], True)

    @pl.when(not_top)
    def _():
        pack_faces()

    @pl.when(is_far & not_top)
    def _():
        learn_far()

    @pl.when(is_near & not_top)
    def _():
        pl.semaphore_wait(far_sem, 1)

    @pl.when(not_top)
    def _():
        send_diagonal(0)
        send_diagonal(1)
        send_faces()

    pltpu.make_async_copy(XB.at[0], XB.at[0], send_sem.at[1]).wait()
    send_x_bulk(sides[1], False)
    await_("y", YR)
    for x in range(X):
        for k in range(2):
            value = ends(YR[1, k, x], YR[0, k, x])
            S[k, 2 + x, low] = value
            S[k, 2 + x, high] = value
        for d in range(3):
            V[d, 1 + x, Y:Y + T] = ends(YR[1, 2 + d, x], YR[0, 2 + d, x])
        for m in range(5):
            WP[m, x] = ends(YR[1, 5 + m, x], YR[0, 5 + m, x])

    def window(w, dy):
        if w == 0:
            return slice(T + dy, T + dy + Y)
        return slice(Y + T - 1, Y + 2 * T - 1) if dy < 0 else slice(dy, T + dy)

    def rows_of(w):
        return slice(0, Y) if w == 0 else slice(Y, Y + T)

    def prepare(p):
        for k in range(2):
            for t in range(YT + 1):
                rows = slice(T * t, T * t + T)
                value = S[k, p, rows]
                SU[k, p, rows] = roll(value, -1)
                SD[k, p, rows] = roll(value, 1)

    def spread(tile, k, t, xx):
        return roll(tile, LANES - 1 - (k * HALF + t * stride_t + 2 * xx))

    def complete(p, columns, at):
        for k in range(2):
            for t in range(YT + 1):
                rows = slice(T * t, T * t + T)
                edge = spread(columns, k, t, at)
                above = jnp.where(last, edge, SU[k, p, rows])
                below = jnp.where(first, edge, SD[k, p, rows])
                size = jnp.abs(S[k, p, rows])
                a_above, a_below = jnp.abs(above), jnp.abs(below)
                for r in (rows,) if t else (low, high):
                    psi[k, p, r] = size
                    H[k, p, r] = 2.0 * size + (a_above + a_below)
                    O[k, p, r] = a_above - a_below
                    if k == 0:
                        signs[0, p, r] = S[k, p, rows]
                        signs[2, p, r] = above
                        signs[1, p, r] = below

    def sums(p):
        for k in range(2):
            for w in range(2):
                A[k, p, rows_of(w)] = (
                    H[k, p, window(w, 0)] + (psi[k, p, window(w, 1)] + psi[k, p, window(w, -1)])
                ) * (1.0 / 36.0)

    def gradient(k, p, w):
        gx = A[k, p + 1, rows_of(w)] - A[k, p - 1, rows_of(w)]
        sides_y = []
        for dy in (1, -1):
            r = window(w, dy)
            sides_y.append(H[k, p, r] + (psi[k, p + 1, r] + psi[k, p - 1, r]))
        gy = (sides_y[0] - sides_y[1]) * (1.0 / 36.0)
        r = window(w, 0)
        gz = 2.0 * O[k, p, r] + (O[k, p + 1, r] + O[k, p - 1, r])
        gz = (gz + (O[k, p, window(w, 1)] + O[k, p, window(w, -1)])) * (1.0 / 36.0)
        return gx, gy, gz

    def velocities(common, x, w):
        grads = [gradient(k, x + 2, w) for k in range(2)]
        return [
            [common[d] - (COUPLING * RELAX[k]) * grads[1 - k][d] for d in range(3)]
            for k in range(2)
        ]

    def common_of(x, w):
        return [V[d, 1 + x, rows_of(w)] for d in range(3)]

    def flat_of(u):
        return 1.0 - 1.5 * (u[0] * u[0] + u[1] * u[1] + u[2] * u[2])

    def one_way(w, flat, along, sign):
        even_part = w * (flat + 4.5 * (along * along))
        return even_part + w * ((3.0 * sign) * along)

    def collide_own(x):
        us = velocities(common_of(x, 0), x, 0)
        for k in range(2):
            u = us[k]
            rho = psi[k, 2 + x, inner] * INV[k]
            flat = flat_of(u)
            scaled = {w: rho * w for w in sorted(set(WEIGHTS))}
            values = {0: scaled[WEIGHTS[0]] * flat}
            for i in range(1, 19, 2):
                along = along_of(i, u)
                w = scaled[WEIGHTS[i]]
                even_part = w * (flat + 4.5 * (along * along))
                odd_part = w * (3.0 * along)
                values[i] = even_part + odd_part
                values[i + 1] = even_part - odd_part
            for i in range(19):
                if abs(KEEP[k]) > 1e-9:
                    values[i] = values[i] + KEEP[k] * pop[k, i, x]
                post[k, i, 1 + x, inner] = values[i]

    row_sign = jnp.where(upper, -1.0, 1.0)

    def collide_rows(x):
        us = velocities(common_of(x, 1), x, 1)
        for k in range(2):
            u = us[k]
            rho = psi[k, 2 + x, low] * INV[k]
            flat = flat_of(u)
            for m, i in enumerate(Y_UP):
                w = rho * WEIGHTS[i]
                value = one_way(w, flat, along_of(i, u), row_sign)
                if abs(KEEP[k]) > 1e-9:
                    value = value + KEEP[k] * WP[m, x]
                post[k, i, 1 + x, low] = value
                post[k, OPPOSITE[i], 1 + x, high] = value

    def collide_plane(n):
        x = -1 if n == 0 else X
        sign = 1.0 if n == 0 else -1.0
        us = velocities([XB[n, d] for d in range(3)], x, 0)
        for k in range(2):
            u = us[k]
            rho = psi[k, 2 + x, inner] * INV[k]
            flat = flat_of(u)
            for m, i in enumerate(X_UP):
                value = one_way(rho * WEIGHTS[i], flat, along_of(i, u), sign)
                if abs(KEEP[k]) > 1e-9:
                    value = value + KEEP[k] * XB[n, 3 + m]
                post[k, i if n == 0 else OPPOSITE[i], 1 + x, inner] = value

    def collide_corner(n):
        x = -1 if n == 0 else X
        sign = 1.0 if n == 0 else -1.0
        us = velocities(common_of(x, 1), x, 1)
        cx = 1 if n == 0 else -1
        up, down = INDEX[(cx, 1, 0)], INDEX[(cx, -1, 0)]
        for k in range(2):
            u = us[k]
            rho = psi[k, 2 + x, low] * INV[k]
            value = one_way(rho * WEIGHTS[up], flat_of(u), sign * u[0] + row_sign * u[1], 1.0)
            if abs(KEEP[k]) > 1e-9:
                value = value + KEEP[k] * XWP[n]
            post[k, up, 1 + x, low] = value
            post[k, down, 1 + x, high] = value

    def y_up(v, n=0):
        r = roll_rows(v, -1)
        return jnp.where(row == T - 1, roll(r, n - stride_t), roll(r, n))

    def y_down(v, n=0):
        r = roll_rows(v, 1)
        return jnp.where(row == 0, roll(r, n + stride_t), roll(r, n))

    def collide_z(s0, s1, s2, t1, t2, olds):
        other1, other2 = roll(t1, HALF), roll(t2, HALF)
        common = [
            jnp.where(lower, t1, other1),
            jnp.where(lower, t2, other2),
            jnp.where(lower, other1, t1),
        ]
        p0, p1, p2 = jnp.abs(s0), jnp.abs(s1), jnp.abs(s2)
        g = 2.0 * p1 + (p0 + p2)
        sign = jnp.where(even, 1.0, -1.0)
        d = (p0 - p2) * sign
        up_up, up_down = y_up(p1, HALF - 2), y_down(p1, HALF - 2)
        down_up, down_down = y_up(p1, HALF + 2), y_down(p1, HALF + 2)
        grads = [
            (roll(g, HALF - 2) - roll(g, HALF + 2)) + ((up_up + up_down) - (down_up + down_down)),
            (y_up(g, HALF) - y_down(g, HALF)) + ((up_up + down_up) - (up_down + down_down)),
            (2.0 * roll(d, HALF) + (roll(d, HALF - 2) + roll(d, HALF + 2)))
            + (y_up(d, HALF) + y_down(d, HALF)),
        ]
        factor = jnp.where(lower, COUPLING * RELAX[0] / 36.0, COUPLING * RELAX[1] / 36.0)
        u = [common[d] - factor * grads[d] for d in range(3)]
        rho = p1 * jnp.where(lower, INV[0], INV[1])
        keep = jnp.where(lower, KEEP[0], KEEP[1])
        flat = flat_of(u)
        beyond = (slot < 2) | (slot >= X + 2)
        for g, i in enumerate(Z_UP):
            c = VELOCITIES[i]
            old = jnp.where(beyond, t2, olds[g]) if c[0] else olds[g]
            value = one_way(rho * WEIGHTS[i], flat, along_of(i, u), sign)
            value = value + keep * jnp.where(lower, 0.0, old)
            if c[1]:
                a, b = (y_down, y_up) if c[1] > 0 else (y_up, y_down)
                value = jnp.where(even, b(value, -1), a(value, 1))
            else:
                value = jnp.where(even, roll(value, -1 - 2 * c[0]), roll(value, 1 + 2 * c[0]))
            for k in range(2):
                for x in range(X):
                    for t in range(1, YT + 1):
                        zpost[k, g, x, T * (t - 1):T * t] = spread(value, k, t, x + 2)

    for x in range(X):
        prepare(2 + x)

    await_("xS", S.at[:, 0:4, inner])
    for n, side in enumerate((1, -1)):
        wide = slice(Y, Y + T) if side > 0 else slice(T, 2 * T)
        for m, p in enumerate((0, X + 2)):
            send("yX", S.at[:, p:p + 2, wide], YX.at[n, m], (0, side, 0), 4)
    await_("xE", XE)
    for n in range(2):
        value = XE[n, y_slot[1]]
        if NY > 1:
            value = jnp.where(row % 2 == 0, value, XE[n, y_slot[-1]])
        plane = 0 if n == 0 else X + 1
        for d in range(3):
            V[d, plane, Y:Y + T] = roll_rows(value, -2 * d)
        XWP[n] = roll_rows(value, -6)
    await_("yX", YX)
    for m, base in enumerate((0, X + 2)):
        for q in range(2):
            for k in range(2):
                value = ends(YX[1, m, k, q], YX[0, m, k, q])
                S[k, base + q, low] = value
                S[k, base + q, high] = value
    outer = [0, 1, X + 2, X + 3]
    for p in outer:
        prepare(p)

    def with_rows(tile, w_low, w_high):
        return jnp.where(own_t, tile, jnp.where(tile_t == 0, w_low, w_high))

    def by_row(low_part, high_part):
        return low_part if NY == 1 else ends(low_part, high_part)

    top = stride_t * (YT + 1)

    s0 = roll(ZS[5], 4)
    for p in range(XX):
        for k in range(2):
            for t in ([0] if 2 <= p < X + 2 else range(YT + 1)):
                j = (k * HALF + t * stride_t) // 2 + p
                s0 = jnp.where(pair == j, roll(S[k, p, T * t:T * t + T], 2 * j + 1), s0)
    s0 = swap(jnp.where(tile_t == YT + 1, roll(s0, top), s0))

    await_("zF", ZF)
    one, two = ZF[0, 0], ZF[1, 0]
    rows_z = [jnp.where(even, ZF[0, 2 + m], ZF[1, 2 + m]) for m in range(NY)]
    z_rows = by_row(rows_z[y_slot[1]], rows_z[y_slot[-1]])
    near_signs = jnp.where(even, roll(two, -1), roll(one, 1))
    near_signs = jnp.where(tile_t == 0, swap(z_rows), near_signs)
    faces = []
    for m in range(2):
        one, two = ZF[0, m], ZF[1, m]
        faces.append(jnp.where(even, one, two))
        faces.append(jnp.where(even, roll(one, -1), roll(two, 1)))
    full = [
        with_rows(faces[p], roll(z_rows, -stride_t * p), roll(z_rows, top - stride_t * p))
        for p in range(4)
    ]
    center = [[roll(full[p], 2 * (2 - b * X)) for b in range(2)] for p in range(2)]
    olds = []
    for p, h, b in POP_PLACE:
        olds.append(roll(full[p], 2 * (2 - b * X) + HALF * (1 - h)))
    for x in range(X):
        complete(2 + x, near_signs, x)
    for x in range(X):
        sums(2 + x)
    for x in range(1, X - 1):
        collide_own(x)
        collide_rows(x)
    state = (pop, solid, post, zpost, signs, inside)
    for x in range(1, X - 1):
        stream(x, x - 1, state, reach(x, X))

    await_("zD", ZD)
    bases, row_parts, far_signs = [], [], []
    for n in range(2):
        merged = [jnp.where(even, ZD[0, n, q], ZD[1, n, q]) for q in range(1 + NY)]
        w = by_row(merged[1 + y_slot[1]], merged[1 + y_slot[-1]])
        bases.append(jnp.where(tile_t == 0, w, merged[0]))
        row_parts.append(w)
        far_signs.append(swap(bases[n]))

    def moved(n, shift):
        return jnp.where(
            tile_t == YT + 1, roll(row_parts[n], 2 * shift + top), roll(bases[n], 2 * shift)
        )

    def assemble(middle, shift_left, shift_right):
        outside = jnp.where(slot < 2, moved(0, shift_left), moved(1, shift_right))
        return jnp.where((slot < 2) | (slot >= X + 2), outside, middle)

    s1, s2 = [assemble(center[0][b], -(b * X + X - 2), X + 2 - b * X) for b in range(2)]
    t1, t2 = [assemble(center[1][b], 1 - b * X, 3 - b * X) for b in range(2)]
    for m in range(2):
        complete(m, far_signs[0], X - 2 + m)
        complete(X + 2 + m, far_signs[1], m)
    for p in outer:
        sums(p)
    collide_z(s0, s1, s2, t1, t2, olds)
    for x in (0, X - 1):
        collide_own(x)
        collide_rows(x)
    for n in range(2):
        collide_corner(n)
    for x in range(1, X - 1):
        stream(x, x - 1, state, [i for i in range(19) if i not in reach(x, X)])
    await_("xB", XB)
    for n in range(2):
        collide_plane(n)
    assert sent[0] == tally.shape[0]
    pltpu.make_async_copy(tally, tally, send_sem.at[0]).wait()


def body(populations, solid):
    X, Y, Z = solid.shape
    f32 = jnp.float32
    dma = pltpu.SemaphoreType.DMA
    R = Y + 2 * T
    XX = X + 4
    NY = 1 if lax.axis_size("gy") == 2 else 2
    YT = Y // T
    tiles = 20 * X + 16 * YT + 24 + 8 * NY

    def vmem(*shape):
        return pltpu.VMEM(shape, f32)

    shapes = [
        populations.shape,
        solid.shape,
        (2, 19, X + 2, R, Z),
        (2, 5, X, Y, Z),
        (3, XX, R, Z),
        (2, 19, X - 2, Y, Z),
    ]
    types = [solid.dtype if n == 1 else f32 for n in range(6)]
    in_vmem = pl.BlockSpec(memory_space=pltpu.VMEM)
    state = pl.pallas_call(
        step_kernel,
        out_shape=[pltpu.VMEM(a, b) for a, b in zip(shapes, types)],
        in_specs=[pl.BlockSpec(memory_space=pltpu.HBM)] * 2,
        out_specs=[in_vmem] * 6,
        scratch_shapes=[
            vmem(2, XX, R, Z),
            vmem(2, XX, R, Z),
            vmem(2, XX, R, Z),
            vmem(2, XX, R, Z),
            vmem(2, XX, R, Z),
            vmem(2, XX, R, Z),
            vmem(2, XX, Y + T, Z),
            vmem(3, X + 2, Y + T, Z),
            vmem(2, 10, X, T, Z),
            vmem(5, X, T, Z),
            vmem(2, 8, Y, Z),
            vmem(2, T, Z),
            vmem(2, 2, T, LANES),
            vmem(2, NY, T, LANES),
            vmem(6, T, LANES),
            vmem(2, 2, 2, 2, T, LANES),
            vmem(2, 2 + NY, T, LANES),
            vmem(2, 2, 1 + NY, T, LANES),
            vmem(tiles, T, LANES),
            dma((X + 1,)),
            dma((2,)),
            dma((7,)),
            pltpu.SemaphoreType.REGULAR,
            pltpu.SemaphoreType.REGULAR,
        ],
        compiler_params=pltpu.CompilerParams(
            collective_id=0, has_side_effects=True, vmem_limit_bytes=24 * 2**20
        ),
    )(*[pltpu.with_memory_space_constraint(v, pltpu.HBM) for v in (populations, solid)])
    return pl.pallas_call(
        finish_kernel,
        out_shape=jax.ShapeDtypeStruct(populations.shape, f32),
        in_specs=[in_vmem] * 6,
        out_specs=pl.BlockSpec(memory_space=pl.ANY),
        scratch_shapes=[vmem(2, 19, 2, Y, Z), dma((3,))],
        compiler_params=pltpu.CompilerParams(vmem_limit_bytes=16 * 2**20),
    )(*state)


def solution(mesh):
    in_specs = (P(None, None, "gx", "gy", "gz"), P("gx", "gy", "gz"))
    out_specs = P(None, None, "gx", "gy", "gz")
    return jax.shard_map(body, mesh=mesh, in_specs=in_specs, out_specs=out_specs, check_vma=False)
```

```python
import jax
import jax.numpy as jnp
from jax import lax
from jax.experimental import pallas as pl
from jax.experimental.pallas import tpu as pltpu
from jax.sharding import PartitionSpec as P

VELOCITIES = [
    (0, 0, 0),
    (1, 0, 0),
    (-1, 0, 0),
    (0, 1, 0),
    (0, -1, 0),
    (0, 0, 1),
    (0, 0, -1),
    (1, 1, 0),
    (-1, -1, 0),
    (1, -1, 0),
    (-1, 1, 0),
    (1, 0, 1),
    (-1, 0, -1),
    (1, 0, -1),
    (-1, 0, 1),
    (0, 1, 1),
    (0, -1, -1),
    (0, 1, -1),
    (0, -1, 1),
]
WEIGHTS = [1.0 / 3.0] + [1.0 / 18.0] * 6 + [1.0 / 36.0] * 12
OPPOSITE = [0, 2, 1, 4, 3, 6, 5, 8, 7, 10, 9, 12, 11, 14, 13, 16, 15, 18, 17]
INDEX = {v: i for i, v in enumerate(VELOCITIES)}
COUPLING = 0.9
RELAX = (1.0, 0.8)
WALL = (0.3, 1.5)
INV = [1.0 / t for t in RELAX]
KEEP = [1.0 - v for v in INV]
AXES = ("gx", "gy", "gz")
MESH = pl.DeviceIdType.MESH

X_UP = [i for i in range(19) if VELOCITIES[i][0] == 1]
Y_UP = [i for i in range(19) if VELOCITIES[i][1] == 1]
Z_UP = [(0, 0, 1), (1, 0, 1), (-1, 0, 1), (0, 1, 1), (0, -1, 1)]
Z_UP = [INDEX[v] for v in Z_UP]
Z_PAIR = {}
for _g, _i in enumerate(Z_UP):
    Z_PAIR[_i] = _g
    Z_PAIR[OPPOSITE[_i]] = _g
Z_FROM = [(dx, dz) for dz in (-1, 1) for dx in (0, -1, 1)]
T = 8
LANES = 128
HALF = LANES // 2


def along_of(i, u):
    total = None
    for d in range(3):
        c = VELOCITIES[i][d]
        if c:
            term = u[d] if c > 0 else -u[d]
            total = term if total is None else total + term
    return total


def reach(x, X):
    return [i for i, c in enumerate(VELOCITIES) if 1 <= x - c[0] <= X - 2 and c[2] == 0]


def stream(x, out_at, refs, dirs=range(19)):
    pop, solid, post, zpost, signs, out = refs
    X, Y, Z = solid.shape
    lane = lax.broadcasted_iota(jnp.int32, (Y, Z), 1)
    first, last = lane == 0, lane == Z - 1
    fluid = solid[x] == 0
    for k in range(2):
        for i in dirs:
            c = VELOCITIES[i]
            rows = slice(T - c[1], T - c[1] + Y)
            read = post[k, i, 1 + x - c[0], rows]
            if i:
                if c[2]:
                    shifted = pltpu.roll(read, c[2] % Z, 1)
                    read = jnp.where(first if c[2] > 0 else last, zpost[k, Z_PAIR[i], x], shifted)
                bounced = post[k, OPPOSITE[i], 1 + x, T:T + Y]
                read = jnp.where(signs[c[2] % 3, 2 + x - c[0], rows] > 0.0, read, bounced)
            out[k, i, out_at] = jnp.where(fluid, read, pop[k, i, x])


def finish_kernel(pop, solid, post, zpost, signs, inside, out, ends, sem):
    X, Y, Z = solid.shape
    copies = [pltpu.make_async_copy(inside, out.at[:, :, 1:X - 1], sem.at[0])]
    copies[0].start()
    for n, x in enumerate((0, X - 1)):
        stream(x, n, (pop, solid, post, zpost, signs, ends))
        copies.append(pltpu.make_async_copy(ends.at[:, :, n], out.at[:, :, x], sem.at[1 + n]))
        copies[-1].start()
    for copy in copies:
        copy.wait()


def step_kernel(pop_hbm, solid_hbm, pop, solid, post, zpost, signs, inside, S, SU, SD, psi, H, O, A, V,
                YR, WP, XB, XWP, XSND, XE, ZS, YX, ZF, ZD, tally, load_sem, send_sem, recv_sem,
                told_sem):
    X, Y, Z = solid.shape
    YT = Y // T
    inner = slice(T, T + Y)
    low, high = slice(0, T), slice(Y + T, Y + 2 * T)
    XX = X + 4
    stride_t = HALF // (YT + 2)
    assert Z == LANES and YT == 2 and X >= 3
    assert stride_t >= 2 * XX and 2 * X <= XX

    me = [lax.axis_index(a) for a in AXES]
    count = [lax.axis_size(a) for a in AXES]
    assert count[1] % 2 == 0
    y_sides = (1,) if count[1] == 2 else (1, -1)
    NY = len(y_sides)
    y_slot = {1: 0, -1: NY - 1}

    loads = [pltpu.make_async_copy(solid_hbm, solid, load_sem.at[0])]
    for n in range(X):
        part = slice(X - 1 - n, X - n)
        loads.append(
            pltpu.make_async_copy(pop_hbm.at[:, :, part], pop.at[:, :, part], load_sem.at[1 + n])
        )
    for copy in loads:
        copy.start()

    parity = lax.rem(me[1], 2)
    is_near, is_far = parity == 0, parity == 1

    def device(offset):
        return tuple(lax.rem(me[d] + offset[d] + count[d], count[d]) for d in range(3))

    barrier = pltpu.get_barrier_semaphore()
    partner = (me[0], me[1] + 1 - 2 * parity, me[2])
    pairs = [me[1] - parity]
    if count[1] > 2:
        pairs.append(lax.rem(me[1] + 3 * parity - 2 + count[1], count[1]))

    def arrive(place):
        pl.semaphore_signal(barrier, inc=1, device_id=place, device_id_type=MESH)

    for dx in (1, -1, 0):
        for dz in (1, -1):
            place = device((dx, 0, dz))
            for base in pairs:
                arrive((place[0], base + 1, place[2]))
    for dx in (1, -1):
        place = device((dx, 0, 0))
        for base in pairs:
            arrive((place[0], base, place[2]))
    for base in pairs[1:]:
        arrive((me[0], base, me[2]))
    arrive(partner)
    near_count, far_count = 4 + 1, 12 + 1
    if count[1] > 2:
        near_count, far_count = near_count + 6, far_count + 12

    lane = lax.broadcasted_iota(jnp.int32, (T, LANES), 1)
    row = lax.broadcasted_iota(jnp.int32, (T, LANES), 0)
    pair = lane // 2
    even = lane % 2 == 0
    half = lane // HALF
    lower = half == 0
    slot = (lane % stride_t) // 2
    tile_t = (lane % HALF) // stride_t
    own_t = (tile_t > 0) & (tile_t <= YT)
    first, last = lane == 0, lane == Z - 1
    lane_y = lax.broadcasted_iota(jnp.int32, (Y, LANES), 1)
    first_y, last_y = lane_y == 0, lane_y == Z - 1
    upper = row < T // 2

    def roll(v, n):
        n = n % LANES
        return pltpu.roll(v, n, 1) if n else v

    def roll_rows(v, n):
        n = n % T
        return pltpu.roll(v, n, 0) if n else v

    def swap(v):
        return jnp.where(even, roll(v, -1), roll(v, 1))

    GROUPS = {"y": 0, "yX": 1, "xS": 2, "xE": 3, "zF": 4, "zD": 5, "xB": 6}
    sent = [0]

    def send(group, src, dst, offset, tiles, first=False):
        pltpu.make_async_remote_copy(
            src_ref=src,
            dst_ref=dst,
            send_sem=send_sem.at[1 if first else 0],
            recv_sem=recv_sem.at[GROUPS[group]],
            device_id=device(offset),
            device_id_type=MESH,
        ).start()
        sent[0] += 0 if first else tiles

    def await_(group, ref):
        pltpu.make_async_copy(ref, ref, recv_sem.at[GROUPS[group]]).wait()

    def moments(x):
        fluid = solid[x] == 0
        total, mom = [], []
        for k in range(2):
            f = [pop[k, i, x] for i in range(19)]
            rho = f[0]
            m = [None, None, None]
            for i in range(1, 19, 2):
                rho = rho + (f[i] + f[i + 1])
                diff = f[i] - f[i + 1]
                for d in range(3):
                    c = VELOCITIES[i][d]
                    if c:
                        m[d] = (
                            (diff if c > 0 else -diff)
                            if m[d] is None
                            else (m[d] + diff if c > 0 else m[d] - diff)
                        )
            total.append(rho)
            S[k, 2 + x, inner] = jnp.where(fluid, rho, -WALL[k])
            mom.append([v * INV[k] if INV[k] != 1.0 else v for v in m])
        scale = 1.0 / (total[0] * INV[0] + total[1] * INV[1])
        for d in range(3):
            V[d, 1 + x, 0:Y] = (mom[0][d] + mom[1][d]) * scale

    blank = jnp.zeros((T, LANES), jnp.float32)
    packs = [blank, blank, blank, blank]
    POP_PLACE = [(2, 0, 0), (2, 0, 1), (2, 1, 0), (2, 1, 1), (3, 1, 0)]
    V_PLACE = [(1, 0, 0), (1, 0, 1), (1, 1, 0)]

    def put(p, h, b, t, x, value, inside=False):
        j = (h * HALF + t * stride_t + (b * X + x) * 2) // 2
        if inside:
            value = jnp.where(even, roll(value, 2 * j + 2), roll(value, 2 * j))
        else:
            value = roll(value, 2 * j + 1)
        packs[p] = jnp.where(pair == j, value, packs[p])

    def z_ends(i, x, t):
        rows = slice(T * (t - 1), T * t)
        return jnp.where(lane < HALF, pop[1, OPPOSITE[i], x, rows], pop[1, i, x, rows])

    beside = [blank, blank]

    def put_beside(x, h, b, t, value):
        n, at = (1, X - 1) if x == 0 else (0, 0)
        j = (h * HALF + t * stride_t + (b * X + at) * 2) // 2
        beside[n] = jnp.where(pair == j, roll(value, 2 * j + 1), beside[n])

    def pack_signs(x):
        for t in range(1, YT + 1):
            rows = slice(T * (t - 1), T * t)
            for k in range(2):
                value = S[k, 2 + x, T * t:T * t + T]
                put(0, k, 0, t, x, value)
                put(0, k, 1, t, x, value, inside=True)
            if x in (0, X - 1):
                for d in range(3):
                    put_beside(x, *V_PLACE[d][1:], t, V[d, 1 + x, rows])
                out_i, in_i = (Z_UP[1], Z_UP[2]) if x else (Z_UP[2], Z_UP[1])
                value = jnp.where(lane < HALF, pop[1, OPPOSITE[in_i], x, rows], pop[1, out_i, x, rows])
                put_beside(x, 1, 1, t, value)

    top_z = me[2] == count[2] - 1
    not_top = jnp.logical_not(top_z)

    def tell(sem):
        pl.semaphore_signal(sem, inc=1, device_id=partner, device_id_type=MESH)

    def learn_far():
        pl.semaphore_wait(barrier, far_count)
        tell(told_sem)

    corner = top_z & (me[0] == count[0] - 1)
    place = slot % X

    def edges(v, q):
        return jnp.where(upper, roll(v, (q - 1) * stride_t), roll(v, (q - YT) * stride_t))

    def make_diagonal(n):
        tile = jnp.where((place >= X - 2) if n == 0 else (place < 2), packs[0], beside[n])
        XSND[n, 0] = jnp.where(tile_t == 0, edges(tile, 0), tile)

    def send_diagonal(n):
        side = 1 - 2 * n
        for m, dz in enumerate((1, -1)):
            send("zD", XSND.at[n, 0], ZD.at[m, n, 0], (side, 0, dz), 1)
            for sy in y_sides:
                send("zD", XSND.at[n, 0], ZD.at[m, n, 1 + y_slot[-sy]], (side, sy, dz), 1)

    @pl.when(is_far & corner)
    def _():
        learn_far()

    loads[0].wait()
    for n in range(X):
        loads[1 + n].wait()
        moments(X - 1 - n)
        pack_signs(X - 1 - n)
        if n == 1:
            make_diagonal(0)

            @pl.when(is_near & corner)
            def _():
                pl.semaphore_wait(told_sem, 1)

            @pl.when(corner)
            def _():
                send_diagonal(0)

    make_diagonal(1)

    def ends(a, b):
        return jnp.where(upper, a, b)

    t_first, t_last = slice(0, T), slice(Y - T, Y)
    for n, side in enumerate((1, -1)):
        x = X - 1 if side > 0 else 0
        up, down = INDEX[(side, 1, 0)], INDEX[(side, -1, 0)]
        fields = [ends(V[d, 1 + x, t_first], V[d, 1 + x, t_last]) for d in range(3)]
        fields.append(ends(pop[1, down, x, t_first], pop[1, up, x, t_last]))
        packed = fields[0]
        for f in range(1, 4):
            at = (row == 2 * f - 1) | (row == 2 * f)
            packed = jnp.where(at, roll_rows(fields[f], 2 * f), packed)
        XSND[n, 1] = packed

    first_up = lax.rem(me[0], 4) != 1
    sides = [jnp.where(first_up, 1, -1), jnp.where(first_up, -1, 1)]

    def send_x_signs(side):
        up = side > 0
        src = jnp.where(up, X, 2)
        dst = jnp.where(up, 0, X + 2)
        send("xS", S.at[:, pl.ds(src, 2), inner], S.at[:, pl.ds(dst, 2), inner],
             (side, 0, 0), 4 * YT)

    def send_x_bulk(side, first):
        up = side > 0
        n = jnp.where(up, 0, 1)
        to = (side, 0, 0)
        send("xB", V.at[:, jnp.where(up, X, 1), 0:Y], XB.at[n, 0:3], to, 3 * YT, first)
        for m, i in enumerate(X_UP):
            send("xB", pop.at[1, jnp.where(up, i, OPPOSITE[i]), jnp.where(up, X - 1, 0)],
                 XB.at[n, 3 + m], to, YT, first)

    ZS[5] = packs[0]

    def pack_faces():
        packs[1] = jnp.where(place == X - 1, roll(beside[0], 2 * (X - 1)), roll(beside[1], -2 * (X - 1)))
        for x in range(X):
            for t in range(1, YT + 1):
                for d in range(3) if 0 < x < X - 1 else ():
                    put(*V_PLACE[d], t, x, V[d, 1 + x, T * (t - 1):T * t])
                for g, i in enumerate(Z_UP):
                    put(*POP_PLACE[g], t, x, z_ends(i, x, t))
        merged = edges(packs[0], 0)
        for p in range(1, 4):
            merged = jnp.where(tile_t == p, edges(packs[p], p), merged)
        for m in range(2):
            one, two = packs[2 * m], packs[2 * m + 1]
            ZS[m] = jnp.where(even, one, roll(two, 1))
            ZS[2 + m] = jnp.where(even, roll(two, -1), one)
        ZS[4] = merged
        packs[1] = packs[2] = packs[3] = blank

    def send_faces():
        for m, dz in enumerate((1, -1)):
            send("zF", ZS.at[2 * m:2 * m + 2], ZF.at[m, 0:2], (0, 0, dz), 2)
            for sy in y_sides:
                send("zF", ZS.at[4], ZF.at[m, 2 + y_slot[-sy]], (0, sy, dz), 1)

    late = top_z & jnp.logical_not(corner)

    @pl.when(late)
    def _():
        pack_faces()

    @pl.when(is_far & late)
    def _():
        learn_far()

    @pl.when(is_near & late)
    def _():
        pl.semaphore_wait(told_sem, 1)

    @pl.when(late)
    def _():
        send_faces()
        send_diagonal(0)
        send_diagonal(1)

    @pl.when(corner)
    def _():
        send_diagonal(1)
        pack_faces()
        send_faces()

    sent[0] = 0

    @pl.when(is_near)
    def _():
        pl.semaphore_wait(barrier, near_count)
        tell(told_sem)

    @pl.when(is_far)
    def _():
        pl.semaphore_wait(told_sem, 1)

    send_x_signs(sides[0])
    send_x_signs(sides[1])
    for n, side in enumerate((1, -1)):
        for sy in y_sides:
            send("xE", XSND.at[n, 1], XE.at[n, y_slot[-sy]], (side, sy, 0), 1)
    for n, side in enumerate((1, -1)):
        tile = slice(Y - T, Y) if side > 0 else slice(0, T)
        wide = slice(Y, Y + T) if side > 0 else slice(T, 2 * T)
        to = (0, side, 0)
        send("y", S.at[:, 2:2 + X, wide], YR.at[n, 0:2], to, 2 * X)
        send("y", V.at[:, 1:1 + X, tile], YR.at[n, 2:5], to, 3 * X)
        for m, i in enumerate(Y_UP):
            i = i if side > 0 else OPPOSITE[i]
            send("y", pop.at[1, i, :, tile], YR.at[n, 5 + m], to, X)
    send_x_bulk(sides[0], True)

    @pl.when(not_top)
    def _():
        pack_faces()

    @pl.when(is_far & not_top)
    def _():
        learn_far()

    @pl.when(is_near & not_top)
    def _():
        pl.semaphore_wait(told_sem, 1)

    @pl.when(not_top)
    def _():
        send_diagonal(0)
        send_diagonal(1)
        send_faces()

    await_("y", YR)
    for x in range(X):
        for k in range(2):
            value = ends(YR[1, k, x], YR[0, k, x])
            S[k, 2 + x, low] = value
            S[k, 2 + x, high] = value
        for d in range(3):
            V[d, 1 + x, Y:Y + T] = ends(YR[1, 2 + d, x], YR[0, 2 + d, x])
        for m in range(5):
            WP[m, x] = ends(YR[1, 5 + m, x], YR[0, 5 + m, x])

    def window(w, dy):
        if w == 0:
            return slice(T + dy, T + dy + Y)
        return slice(Y + T - 1, Y + 2 * T - 1) if dy < 0 else slice(dy, T + dy)

    def rows_of(w):
        return slice(0, Y) if w == 0 else slice(Y, Y + T)

    def prepare(p):
        for k in range(2):
            for t in range(YT + 1):
                rows = slice(T * t, T * t + T)
                value = S[k, p, rows]
                SU[k, p, rows] = roll(value, -1)
                SD[k, p, rows] = roll(value, 1)

    def spread(tile, k, t, xx):
        return roll(tile, LANES - 1 - (k * HALF + t * stride_t + 2 * xx))

    def complete(p, columns, at):
        for k in range(2):
            for t in range(YT + 1):
                rows = slice(T * t, T * t + T)
                edge = spread(columns, k, t, at)
                above = jnp.where(last, edge, SU[k, p, rows])
                below = jnp.where(first, edge, SD[k, p, rows])
                size = jnp.abs(S[k, p, rows])
                a_above, a_below = jnp.abs(above), jnp.abs(below)
                for r in (rows,) if t else (low, high):
                    psi[k, p, r] = size
                    H[k, p, r] = 2.0 * size + (a_above + a_below)
                    O[k, p, r] = a_above - a_below
                    if k == 0:
                        signs[0, p, r] = S[k, p, rows]
                        signs[2, p, r] = above
                        signs[1, p, r] = below

    def sums(p):
        for k in range(2):
            for w in range(2):
                A[k, p, rows_of(w)] = (
                    H[k, p, window(w, 0)] + (psi[k, p, window(w, 1)] + psi[k, p, window(w, -1)])
                ) * (1.0 / 36.0)

    def gradient(k, p, w):
        gx = A[k, p + 1, rows_of(w)] - A[k, p - 1, rows_of(w)]
        sides_y = []
        for dy in (1, -1):
            r = window(w, dy)
            sides_y.append(H[k, p, r] + (psi[k, p + 1, r] + psi[k, p - 1, r]))
        gy = (sides_y[0] - sides_y[1]) * (1.0 / 36.0)
        r = window(w, 0)
        gz = 2.0 * O[k, p, r] + (O[k, p + 1, r] + O[k, p - 1, r])
        gz = (gz + (O[k, p, window(w, 1)] + O[k, p, window(w, -1)])) * (1.0 / 36.0)
        return gx, gy, gz

    def velocities(common, x, w):
        grads = [gradient(k, x + 2, w) for k in range(2)]
        return [
            [common[d] - (COUPLING * RELAX[k]) * grads[1 - k][d] for d in range(3)]
            for k in range(2)
        ]

    def common_of(x, w):
        return [V[d, 1 + x, rows_of(w)] for d in range(3)]

    def flat_of(u):
        return 1.0 - 1.5 * (u[0] * u[0] + u[1] * u[1] + u[2] * u[2])

    def one_way(w, flat, along, sign):
        even_part = w * (flat + 4.5 * (along * along))
        return even_part + w * ((3.0 * sign) * along)

    def collide_own(x):
        us = velocities(common_of(x, 0), x, 0)
        for k in range(2):
            u = us[k]
            rho = psi[k, 2 + x, inner] * INV[k]
            flat = flat_of(u)
            scaled = {w: rho * w for w in sorted(set(WEIGHTS))}
            values = {0: scaled[WEIGHTS[0]] * flat}
            for i in range(1, 19, 2):
                along = along_of(i, u)
                w = scaled[WEIGHTS[i]]
                even_part = w * (flat + 4.5 * (along * along))
                odd_part = w * (3.0 * along)
                values[i] = even_part + odd_part
                values[i + 1] = even_part - odd_part
            for i in range(19):
                if abs(KEEP[k]) > 1e-9:
                    values[i] = values[i] + KEEP[k] * pop[k, i, x]
                post[k, i, 1 + x, inner] = values[i]

    row_sign = jnp.where(upper, -1.0, 1.0)

    def collide_rows(x):
        us = velocities(common_of(x, 1), x, 1)
        for k in range(2):
            u = us[k]
            rho = psi[k, 2 + x, low] * INV[k]
            flat = flat_of(u)
            for m, i in enumerate(Y_UP):
                w = rho * WEIGHTS[i]
                value = one_way(w, flat, along_of(i, u), row_sign)
                if abs(KEEP[k]) > 1e-9:
                    value = value + KEEP[k] * WP[m, x]
                post[k, i, 1 + x, low] = value
                post[k, OPPOSITE[i], 1 + x, high] = value

    def collide_plane(n):
        x = -1 if n == 0 else X
        sign = 1.0 if n == 0 else -1.0
        us = velocities([XB[n, d] for d in range(3)], x, 0)
        for k in range(2):
            u = us[k]
            rho = psi[k, 2 + x, inner] * INV[k]
            flat = flat_of(u)
            for m, i in enumerate(X_UP):
                value = one_way(rho * WEIGHTS[i], flat, along_of(i, u), sign)
                if abs(KEEP[k]) > 1e-9:
                    value = value + KEEP[k] * XB[n, 3 + m]
                post[k, i if n == 0 else OPPOSITE[i], 1 + x, inner] = value

    def collide_corner(n):
        x = -1 if n == 0 else X
        sign = 1.0 if n == 0 else -1.0
        us = velocities(common_of(x, 1), x, 1)
        cx = 1 if n == 0 else -1
        up, down = INDEX[(cx, 1, 0)], INDEX[(cx, -1, 0)]
        for k in range(2):
            u = us[k]
            rho = psi[k, 2 + x, low] * INV[k]
            value = one_way(rho * WEIGHTS[up], flat_of(u), sign * u[0] + row_sign * u[1], 1.0)
            if abs(KEEP[k]) > 1e-9:
                value = value + KEEP[k] * XWP[n]
            post[k, up, 1 + x, low] = value
            post[k, down, 1 + x, high] = value

    def y_up(v, n=0):
        r = roll_rows(v, -1)
        return jnp.where(row == T - 1, roll(r, n - stride_t), roll(r, n))

    def y_down(v, n=0):
        r = roll_rows(v, 1)
        return jnp.where(row == 0, roll(r, n + stride_t), roll(r, n))

    def collide_z(s0, s1, s2, t1, t2, olds):
        other1, other2 = roll(t1, HALF), roll(t2, HALF)
        common = [
            jnp.where(lower, t1, other1),
            jnp.where(lower, t2, other2),
            jnp.where(lower, other1, t1),
        ]
        p0, p1, p2 = jnp.abs(s0), jnp.abs(s1), jnp.abs(s2)
        g = 2.0 * p1 + (p0 + p2)
        sign = jnp.where(even, 1.0, -1.0)
        d = (p0 - p2) * sign
        up_up, up_down = y_up(p1, HALF - 2), y_down(p1, HALF - 2)
        down_up, down_down = y_up(p1, HALF + 2), y_down(p1, HALF + 2)
        grads = [
            (roll(g, HALF - 2) - roll(g, HALF + 2)) + ((up_up + up_down) - (down_up + down_down)),
            (y_up(g, HALF) - y_down(g, HALF)) + ((up_up + down_up) - (up_down + down_down)),
            (2.0 * roll(d, HALF) + (roll(d, HALF - 2) + roll(d, HALF + 2)))
            + (y_up(d, HALF) + y_down(d, HALF)),
        ]
        factor = jnp.where(lower, COUPLING * RELAX[0] / 36.0, COUPLING * RELAX[1] / 36.0)
        u = [common[d] - factor * grads[d] for d in range(3)]
        rho = p1 * jnp.where(lower, INV[0], INV[1])
        keep = jnp.where(lower, KEEP[0], KEEP[1])
        flat = flat_of(u)
        beyond = (slot < 2) | (slot >= X + 2)
        for g, i in enumerate(Z_UP):
            c = VELOCITIES[i]
            old = jnp.where(beyond, t2, olds[g]) if c[0] else olds[g]
            value = one_way(rho * WEIGHTS[i], flat, along_of(i, u), sign)
            value = value + keep * jnp.where(lower, 0.0, old)
            if c[1]:
                a, b = (y_down, y_up) if c[1] > 0 else (y_up, y_down)
                value = jnp.where(even, b(value, -1), a(value, 1))
            else:
                value = jnp.where(even, roll(value, -1 - 2 * c[0]), roll(value, 1 + 2 * c[0]))
            for k in range(2):
                for x in range(X):
                    for t in range(1, YT + 1):
                        zpost[k, g, x, T * (t - 1):T * t] = spread(value, k, t, x + 2)

    for x in range(X):
        prepare(2 + x)

    pltpu.make_async_copy(XB.at[0], XB.at[0], send_sem.at[1]).wait()
    send_x_bulk(sides[1], False)
    await_("xS", S.at[:, 0:4, inner])
    for n, side in enumerate((1, -1)):
        wide = slice(Y, Y + T) if side > 0 else slice(T, 2 * T)
        for m, p in enumerate((0, X + 2)):
            send("yX", S.at[:, p:p + 2, wide], YX.at[n, m], (0, side, 0), 4)
    await_("xE", XE)
    for n in range(2):
        value = XE[n, y_slot[1]]
        if NY > 1:
            value = jnp.where(row % 2 == 0, value, XE[n, y_slot[-1]])
        plane = 0 if n == 0 else X + 1
        for d in range(3):
            V[d, plane, Y:Y + T] = roll_rows(value, -2 * d)
        XWP[n] = roll_rows(value, -6)
    await_("yX", YX)
    for m, base in enumerate((0, X + 2)):
        for q in range(2):
            for k in range(2):
                value = ends(YX[1, m, k, q], YX[0, m, k, q])
                S[k, base + q, low] = value
                S[k, base + q, high] = value
    outer = [0, 1, X + 2, X + 3]
    for p in outer:
        prepare(p)

    def with_rows(tile, w_low, w_high):
        return jnp.where(own_t, tile, jnp.where(tile_t == 0, w_low, w_high))

    def by_row(low_part, high_part):
        return low_part if NY == 1 else ends(low_part, high_part)

    top = stride_t * (YT + 1)

    s0 = roll(ZS[5], 4)
    for p in range(XX):
        for k in range(2):
            for t in ([0] if 2 <= p < X + 2 else range(YT + 1)):
                j = (k * HALF + t * stride_t) // 2 + p
                s0 = jnp.where(pair == j, roll(S[k, p, T * t:T * t + T], 2 * j + 1), s0)
    s0 = swap(jnp.where(tile_t == YT + 1, roll(s0, top), s0))

    await_("zF", ZF)
    one, two = ZF[0, 0], ZF[1, 0]
    rows_z = [jnp.where(even, ZF[0, 2 + m], ZF[1, 2 + m]) for m in range(NY)]
    z_rows = by_row(rows_z[y_slot[1]], rows_z[y_slot[-1]])
    near_signs = jnp.where(even, roll(two, -1), roll(one, 1))
    near_signs = jnp.where(tile_t == 0, swap(z_rows), near_signs)
    faces = []
    for m in range(2):
        one, two = ZF[0, m], ZF[1, m]
        faces.append(jnp.where(even, one, two))
        faces.append(jnp.where(even, roll(one, -1), roll(two, 1)))
    full = [
        with_rows(faces[p], roll(z_rows, -stride_t * p), roll(z_rows, top - stride_t * p))
        for p in range(4)
    ]
    center = [[roll(full[p], 2 * (2 - b * X)) for b in range(2)] for p in range(2)]
    olds = []
    for p, h, b in POP_PLACE:
        olds.append(roll(full[p], 2 * (2 - b * X) + HALF * (1 - h)))
    for x in range(X):
        complete(2 + x, near_signs, x)
    for x in range(X):
        sums(2 + x)
    for x in range(1, X - 1):
        collide_own(x)
        collide_rows(x)
    state = (pop, solid, post, zpost, signs, inside)
    for x in range(1, X - 1):
        stream(x, x - 1, state, reach(x, X))

    await_("zD", ZD)
    bases, row_parts, far_signs = [], [], []
    for n in range(2):
        merged = [jnp.where(even, ZD[0, n, q], ZD[1, n, q]) for q in range(1 + NY)]
        w = by_row(merged[1 + y_slot[1]], merged[1 + y_slot[-1]])
        bases.append(jnp.where(tile_t == 0, w, merged[0]))
        row_parts.append(w)
        far_signs.append(swap(bases[n]))

    def moved(n, shift):
        return jnp.where(
            tile_t == YT + 1, roll(row_parts[n], 2 * shift + top), roll(bases[n], 2 * shift)
        )

    def assemble(middle, shift_left, shift_right):
        outside = jnp.where(slot < 2, moved(0, shift_left), moved(1, shift_right))
        return jnp.where((slot < 2) | (slot >= X + 2), outside, middle)

    s1, s2 = [assemble(center[0][b], -(b * X + X - 2), X + 2 - b * X) for b in range(2)]
    t1, t2 = [assemble(center[1][b], 1 - b * X, 3 - b * X) for b in range(2)]
    for m in range(2):
        complete(m, far_signs[0], X - 2 + m)
        complete(X + 2 + m, far_signs[1], m)
    for p in outer:
        sums(p)
    collide_z(s0, s1, s2, t1, t2, olds)
    for x in (0, X - 1):
        collide_own(x)
        collide_rows(x)
    for n in range(2):
        collide_corner(n)
    for x in range(1, X - 1):
        stream(x, x - 1, state, [i for i in range(19) if i not in reach(x, X)])
    await_("xB", XB)
    for n in range(2):
        collide_plane(n)
    assert sent[0] == tally.shape[0]
    pltpu.make_async_copy(tally, tally, send_sem.at[0]).wait()


def body(populations, solid):
    X, Y, Z = solid.shape
    f32 = jnp.float32
    dma = pltpu.SemaphoreType.DMA
    R = Y + 2 * T
    XX = X + 4
    NY = 1 if lax.axis_size("gy") == 2 else 2
    YT = Y // T
    tiles = 20 * X + 16 * YT + 24 + 8 * NY

    def vmem(*shape):
        return pltpu.VMEM(shape, f32)

    shapes = [
        populations.shape,
        solid.shape,
        (2, 19, X + 2, R, Z),
        (2, 5, X, Y, Z),
        (3, XX, R, Z),
        (2, 19, X - 2, Y, Z),
    ]
    types = [solid.dtype if n == 1 else f32 for n in range(6)]
    in_vmem = pl.BlockSpec(memory_space=pltpu.VMEM)
    state = pl.pallas_call(
        step_kernel,
        out_shape=[pltpu.VMEM(a, b) for a, b in zip(shapes, types)],
        in_specs=[pl.BlockSpec(memory_space=pltpu.HBM)] * 2,
        out_specs=[in_vmem] * 6,
        scratch_shapes=[
            vmem(2, XX, R, Z),
            vmem(2, XX, R, Z),
            vmem(2, XX, R, Z),
            vmem(2, XX, R, Z),
            vmem(2, XX, R, Z),
            vmem(2, XX, R, Z),
            vmem(2, XX, Y + T, Z),
            vmem(3, X + 2, Y + T, Z),
            vmem(2, 10, X, T, Z),
            vmem(5, X, T, Z),
            vmem(2, 8, Y, Z),
            vmem(2, T, Z),
            vmem(2, 2, T, LANES),
            vmem(2, NY, T, LANES),
            vmem(6, T, LANES),
            vmem(2, 2, 2, 2, T, LANES),
            vmem(2, 2 + NY, T, LANES),
            vmem(2, 2, 1 + NY, T, LANES),
            vmem(tiles, T, LANES),
            dma((X + 1,)),
            dma((2,)),
            dma((7,)),
            pltpu.SemaphoreType.REGULAR,
        ],
        compiler_params=pltpu.CompilerParams(
            collective_id=0, has_side_effects=True, vmem_limit_bytes=24 * 2**20
        ),
    )(*[pltpu.with_memory_space_constraint(v, pltpu.HBM) for v in (populations, solid)])
    return pl.pallas_call(
        finish_kernel,
        out_shape=jax.ShapeDtypeStruct(populations.shape, f32),
        in_specs=[in_vmem] * 6,
        out_specs=pl.BlockSpec(memory_space=pl.ANY),
        scratch_shapes=[vmem(2, 19, 2, Y, Z), dma((3,))],
        compiler_params=pltpu.CompilerParams(vmem_limit_bytes=16 * 2**20),
    )(*state)


def solution(mesh):
    in_specs = (P(None, None, "gx", "gy", "gz"), P("gx", "gy", "gz"))
    out_specs = P(None, None, "gx", "gy", "gz")
    return jax.shard_map(body, mesh=mesh, in_specs=in_specs, out_specs=out_specs, check_vma=False)
```
